8 devices in a mesh: dp: 2 (over z, y), tp: 4 (over x, core).
Axes of the slice: x: 2, y: 2, z: 1, core: 2. Of those that a mesh axis runs over, the one named last changes fastest.
Arguments:
- start_hidden: bfloat16 [64, 2304], P('dp'), parts along dimension 0
- embedding: bfloat16 [256000, 2304], P('tp')
- pre_norm: bfloat16 [2304], replicated
- w_gate: bfloat16 [2304, 9216], P(None, 'tp')
- w_up: bfloat16 [2304, 9216], P(None, 'tp')
- w_down: bfloat16 [9216, 2304], P('tp')
- post_norm: bfloat16 [2304], replicated
- final_norm: bfloat16 [2304], replicated
- temperature: float32 [], replicated
- step_noise: float32 [4, 64, 256000], P(None, 'dp', 'tp'), parts along dimension 1
Outputs:
- output 1: int32 [4, 64], P(None, 'dp'), parts along dimension 1
- output 2: bfloat16 [64, 2304], P('dp'), parts along dimension 0
There are 2 independent parts. The reference program is written for one: setup_inputs(seed, part) draws one part's arguments, and reference() takes and returns one part's arrays. A program takes and returns all parts, laid end to end along the dimension named above; an argument that names none is the same for every part.
All inputs are finite; a program needn't handle non-finite values.
Results may differ from the reference program's by a relative error of at most 0.001.
Values are sent between devices in bfloat16 or wider.
A program may use at most 1.5 GiB of HBM per device.

```python
import math
import jax
import jax.numpy as jnp
from jax import lax

VOCAB = 256000
D = 2304
FF = 9216
BATCH = 32
STEPS = 4

SOFT_CAP = 30.0
EPSILON = 1e-6
GAP = 1.0


def rms_scale(values, gain_vec):
    x_f32 = values.astype(jnp.float32)
    mean_sq = jnp.mean(x_f32 * x_f32, axis=-1, keepdims=True)
    return x_f32 * lax.rsqrt(mean_sq + EPSILON) * (1.0 + gain_vec.astype(jnp.float32))


def head_scores(hidden, embedding, pre_norm, w_gate, w_up, w_down, post_norm, final_norm, temperature):
    normed = rms_scale(hidden, pre_norm).astype(jnp.bfloat16)
    gate_proj = jnp.dot(normed, w_gate, preferred_element_type=jnp.float32)
    up_proj = jnp.dot(normed, w_up, preferred_element_type=jnp.float32)
    gated_act = (jax.nn.gelu(gate_proj, approximate=True) * up_proj).astype(jnp.bfloat16)
    down_sum = jnp.dot(gated_act, w_down, preferred_element_type=jnp.float32)
    post_out = rms_scale(down_sum, post_norm).astype(jnp.bfloat16)
    resid_sum = (hidden.astype(jnp.float32) + post_out.astype(jnp.float32)).astype(jnp.bfloat16)
    final_in = rms_scale(resid_sum, final_norm).astype(jnp.bfloat16)
    logits = lax.dot_general(final_in, embedding, (((1,), (1,)), ((), ())), preferred_element_type=jnp.float32)
    return SOFT_CAP * jnp.tanh(logits / SOFT_CAP) / temperature


def lookup_rows(embedding, next_token):
    embed_scale = jnp.asarray(math.sqrt(embedding.shape[1]), jnp.bfloat16).astype(jnp.float32)
    return (jnp.take(embedding, next_token, axis=0).astype(jnp.float32) * embed_scale).astype(jnp.bfloat16)


def noise_rows(step_key, scores):
    batch_rows = scores.shape[0]
    key_a, key_b, key_c, key_d, key_e = jax.random.split(step_key, 5)
    hot_span = VOCAB // 16
    wide_half = (VOCAB - hot_span) // 2
    wide_a = jax.random.randint(key_a, (batch_rows, 1), hot_span, hot_span + wide_half)
    wide_b = jax.random.randint(key_b, (batch_rows, 1), hot_span + wide_half, VOCAB)
    hot_ids = jax.random.randint(key_c, (batch_rows, 2), 0, hot_span // 2) + jnp.array([0, hot_span // 2])
    cand_ids = jnp.concatenate([wide_a, wide_b, hot_ids], axis=1).astype(jnp.int32)
    cand_bonus = jax.random.uniform(key_d, (batch_rows, 4), jnp.float32, 0.0, 4.0) + jnp.array([0.0, 0.0, 2.0, 2.0], jnp.float32)
    coin_flip = jax.random.bernoulli(key_e, 0.5, (batch_rows,))
    best_two = lax.top_k(scores, 2)[0]
    top_score = best_two[:, 0]
    cand_scores = jnp.take_along_axis(scores, cand_ids, axis=1)
    cand_totals = cand_scores + cand_bonus
    cand_pair = lax.top_k(cand_totals, 2)[0]
    win_bump = jnp.where(cand_pair[:, 0] - cand_pair[:, 1] < GAP, GAP, 0.0)
    win_hot = jax.nn.one_hot(jnp.argmax(cand_totals, axis=1), 4, dtype=jnp.float32)
    over_base = top_score - jnp.min(cand_scores, axis=1) + GAP
    over_vals = over_base[:, None] + cand_bonus + win_bump[:, None] * win_hot
    under_vals = jnp.maximum(top_score[:, None] - GAP - cand_scores - cand_bonus, 0.0)
    keep_under = coin_flip & (top_score - best_two[:, 1] >= GAP)
    cand_vals = jnp.where(keep_under[:, None], under_vals, over_vals)
    row_ids = jnp.arange(batch_rows)[:, None]
    return jnp.zeros((batch_rows, VOCAB), jnp.float32).at[row_ids, cand_ids].set(cand_vals)


def setup_inputs(seed: int = 0, part: int = 0) -> dict:
    shared = jax.random.split(jax.random.key(seed), 8)
    part_keys = jax.random.split(jax.random.fold_in(jax.random.key(seed + 1), part), 2)
    embedding = (jax.random.normal(shared[0], (VOCAB, D), jnp.float32) * D ** -0.5).astype(jnp.bfloat16)
    w_gate = (jax.random.normal(shared[1], (D, FF), jnp.float32) * D ** -0.5).astype(jnp.bfloat16)
    w_up = (jax.random.normal(shared[2], (D, FF), jnp.float32) * D ** -0.5).astype(jnp.bfloat16)
    w_down = (jax.random.normal(shared[3], (FF, D), jnp.float32) * FF ** -0.5).astype(jnp.bfloat16)
    pre_norm = (0.5 * jax.random.normal(shared[4], (D,), jnp.float32)).astype(jnp.bfloat16)
    post_norm = (0.5 * jax.random.normal(shared[5], (D,), jnp.float32)).astype(jnp.bfloat16)
    final_norm = (5.0 + 1.5 * jax.random.normal(shared[6], (D,), jnp.float32)).astype(jnp.bfloat16)
    temperature = jax.random.uniform(shared[7], (), jnp.float32, 0.6, 1.2)
    start_hidden = jax.random.normal(part_keys[0], (BATCH, D), jnp.float32).astype(jnp.bfloat16)

    def body(hidden, step_key):
        scores = head_scores(hidden, embedding, pre_norm, w_gate, w_up, w_down, post_norm, final_norm, temperature)
        noise_step = noise_rows(step_key, scores)
        next_token = jnp.argmax(scores + noise_step, axis=1).astype(jnp.int32)
        return lookup_rows(embedding, next_token), noise_step

    final_hidden, step_noise = lax.scan(body, start_hidden, jax.random.split(part_keys[1], STEPS))
    return {'start_hidden': start_hidden, 'embedding': embedding, 'pre_norm': pre_norm, 'w_gate': w_gate, 'w_up': w_up, 'w_down': w_down, 'post_norm': post_norm, 'final_norm': final_norm, 'temperature': temperature, 'step_noise': step_noise}


def reference(start_hidden, embedding, pre_norm, w_gate, w_up, w_down, post_norm, final_norm, temperature, step_noise):
    def body(hidden, noise_step):
        scores = head_scores(hidden, embedding, pre_norm, w_gate, w_up, w_down, post_norm, final_norm, temperature) + noise_step
        next_token = jnp.argmax(scores, axis=1).astype(jnp.int32)
        return lookup_rows(embedding, next_token), next_token

    last_hidden, tokens = lax.scan(body, start_hidden, step_noise)
    return tokens, last_hidden
```

```python
import functools
import math

import jax
import jax.numpy as jnp
import numpy as np
from jax import lax
from jax.experimental import pallas as pl
from jax.experimental.pallas import tpu as pltpu
from jax.sharding import PartitionSpec as P

SOFT_CAP = 30.0
EPSILON = 1e-6
MESH = pl.DeviceIdType.MESH

SUB = 512
NSUB = 5
GROUP = SUB * NSUB
RING_GROUPS = 4
OWN = 5
NEG = -3.0e38


def rms_scale(x_f32, gain_row):
    mean_sq = jnp.mean(x_f32 * x_f32, axis=-1, keepdims=True)
    return x_f32 * lax.rsqrt(mean_sq + EPSILON) * (1.0 + gain_row.astype(jnp.float32))


def remote(src, dst, sem, peer):
    return pltpu.make_async_remote_copy(
        src_ref=src, dst_ref=dst, send_sem=sem.at[0], recv_sem=sem.at[1], device_id=peer, device_id_type=MESH
    )


def step_kernel(cfg, *refs):
    step, first, last, n_group, embed_scale = cfg
    refs = list(refs)
    take = lambda n: [refs.pop(0) for _ in range(n)]
    if first:
        (hid_ref,) = take(1)
    else:
        rows_ref, meta_ref = take(2)
    if not last:
        pre_ref, post_ref, fin_ref, temp_ref, wg_ref, wu_ref, wd_ref, emb_ref, noise_ref = take(9)
    if not first:
        tok_ref, hout_ref = take(2)
    if not last:
        best_ref = take(1)[0]
    if not first:
        rows_a, meta_a, rows_m, meta_m, rows_b, meta_b, rows_f, meta_f, rows_c, meta_c, sem_rows, sem_meta = take(12)
    if not last:
        (ring, nz_own, nz_oth, part_s, part_a, half_s, part_b, f_send, f_all, f_own, f_oth, f_two,
         hid32, gate_s, bv, bi, best_oth, best_in,
         sem_w, sem_e, sem_no, sem_ns, sem_nr, sem_ra, sem_rb, sem_f, sem_fo, sem_by) = take(28)

    dp, tp = lax.axis_index("dp"), lax.axis_index("tp")
    core, chip = lax.rem(tp, 2), lax.div(tp, 2)
    tp_sib = chip * 2 + (1 - core)
    tp_x = (1 - chip) * 2 + core
    tp_diag = (1 - chip) * 2 + (1 - core)
    sib, over, diag, pair = (dp, tp_sib), (dp, tp_x), (dp, tp_diag), (1 - dp, tp)

    if not last:
        half = (n_group - OWN) // 2
        n_iter = OWN + half
        width = ring.shape[1]
        inner = wg_ref.shape[1]
        w_copies = [
            pltpu.make_async_copy(wg_ref, ring.at[pl.ds(0, width)], sem_w.at[0]),
            pltpu.make_async_copy(wu_ref, ring.at[pl.ds(width, width)], sem_w.at[1]),
            pltpu.make_async_copy(wd_ref, ring.at[pl.ds(2 * width, inner)], sem_w.at[2]),
        ]

        def e_copy(i, j):
            group = i + jnp.where(i < OWN, 0, dp * half)
            slot = lax.rem(i + 3, RING_GROUPS)
            return pltpu.make_async_copy(
                emb_ref.at[pl.ds(group * GROUP + j * SUB, SUB)],
                ring.at[pl.ds(slot * GROUP + j * SUB, SUB)],
                sem_e.at[slot, j],
            )

        def e_start(i):
            for j in range(NSUB):
                e_copy(i, j).start()

        def no_copy(i):
            group = i + jnp.where(i < OWN, 0, dp * half)
            return pltpu.make_async_copy(
                noise_ref.at[step, :, pl.ds(group * GROUP, GROUP)], nz_own.at[i], sem_no.at[i]
            )

        def nr_copy(j):
            group = OWN + (1 - dp) * half + j
            return pltpu.make_async_remote_copy(
                src_ref=noise_ref.at[step, :, pl.ds(group * GROUP, GROUP)],
                dst_ref=nz_oth.at[j],
                send_sem=sem_ns.at[j],
                recv_sem=sem_nr.at[j],
                device_id=pair,
                device_id_type=MESH,
            )

        for copy in w_copies:
            copy.start()
        e_start(0)
        pl.loop(0, n_iter)(lambda i: no_copy(i).start())

    barrier = pltpu.get_barrier_semaphore()
    peers = (sib, over) if last else (sib, over, diag, pair)
    for peer in peers:
        pl.semaphore_signal(barrier, inc=1, device_id=peer, device_id_type=MESH)
    pl.semaphore_wait(barrier, len(peers))

    if not last:
        early = 3
        pl.loop(0, early)(lambda j: nr_copy(j).start())

    if first:
        hid = hid_ref[...].astype(jnp.float32)
    else:
        a_rows = remote(rows_ref.at[1 - core], rows_a, sem_rows.at[0], sib)
        a_meta = remote(meta_ref.at[1 - core], meta_a, sem_meta.at[0], sib)
        a_rows.start()
        a_meta.start()
        a_rows.wait()
        a_meta.wait()
        mine = meta_ref[core]
        seen = meta_a[...]
        keep = mine[0] >= seen[0]
        meta_m[...] = jnp.where(keep[None], mine, seen)
        rows_m[...] = jnp.where(
            keep[:, :1], rows_ref[core].astype(jnp.float32), rows_a[...].astype(jnp.float32)
        ).astype(jnp.bfloat16)
        b_rows = remote(rows_m, rows_b, sem_rows.at[1], over)
        b_meta = remote(meta_m, meta_b, sem_meta.at[1], over)
        b_rows.start()
        b_meta.start()
        b_rows.wait()
        b_meta.wait()
        mine = meta_m[...]
        seen = meta_b[...]
        keep = mine[0] >= seen[0]
        meta_f[...] = jnp.where(keep[None], mine, seen)
        rows_f[...] = jnp.where(
            keep[:, :1], rows_m[...].astype(jnp.float32), rows_b[...].astype(jnp.float32)
        ).astype(jnp.bfloat16)
        c_rows = remote(rows_f, rows_c, sem_rows.at[2], sib)
        c_meta = remote(meta_f, meta_c, sem_meta.at[2], sib)
        c_rows.start()
        c_meta.start()
        c_rows.wait()
        c_meta.wait()
        low = core == 0
        r_f, r_c = rows_f[...].astype(jnp.float32), rows_c[...].astype(jnp.float32)
        t_f, t_c = meta_f[1], meta_c[1]
        picked = jnp.concatenate([jnp.where(low, r_f, r_c), jnp.where(low, r_c, r_f)], axis=0)
        tok_ref[...] = jnp.concatenate([jnp.where(low, t_f, t_c), jnp.where(low, t_c, t_f)], axis=0).astype(jnp.int32)
        hid_bf = (picked * embed_scale).astype(jnp.bfloat16)
        hout_ref[...] = hid_bf
        hid = hid_bf.astype(jnp.float32)

    if last:
        return

    batch = hid.shape[0]
    quarter = batch // 4
    hid32[...] = hid.reshape(4, quarter, width)
    normed = rms_scale(hid, pre_ref[...]).astype(jnp.bfloat16)
    f_two[pl.ds(0, batch)] = normed
    w_copies[0].wait()
    w_copies[1].wait()
    col = 768

    @pl.loop(0, inner // col)
    def _(n):
        cols = pl.ds(pl.multiple_of(n * col, col), col)
        lhs = f_two[pl.ds(0, batch)]
        gate = jnp.dot(lhs, ring[pl.ds(0, width), cols], preferred_element_type=jnp.float32)
        up = jnp.dot(lhs, ring[pl.ds(width, width), cols], preferred_element_type=jnp.float32)
        gate_s[:, cols] = (jax.nn.gelu(gate, approximate=True) * up).astype(jnp.bfloat16)

    e_start(1)
    w_copies[2].wait()

    @pl.loop(0, width // col)
    def _(n):
        cols = pl.ds(pl.multiple_of(n * col, col), col)
        part_s[:, :, cols] = jnp.dot(
            gate_s[...], ring[pl.ds(2 * width, inner), cols], preferred_element_type=jnp.float32
        ).reshape(4, quarter, col)

    e_start(2)
    e_start(3)

    ra = remote(part_s.at[pl.ds(2 * (1 - core), 2)], part_a, sem_ra, sib)
    ra.start()
    ra.wait()
    half_s[...] = part_s[pl.ds(2 * core, 2)] + part_a[...]
    rb = remote(half_s.at[1 - chip], part_b, sem_rb, over)
    rb.start()
    rb.wait()
    down_sum = half_s[chip] + part_b[...]
    place = 2 * core + chip
    post_out = rms_scale(down_sum, post_ref[...]).astype(jnp.bfloat16)
    resid = (hid32[place] + post_out.astype(jnp.float32)).astype(jnp.bfloat16)
    final_in = rms_scale(resid.astype(jnp.float32), fin_ref[...]).astype(jnp.bfloat16)
    f_send[...] = final_in
    f_copies = [remote(f_send, f_all.at[k], sem_f.at[k], peer) for k, peer in enumerate((sib, over, diag))]
    for copy in f_copies:
        copy.start()
    for copy in f_copies:
        copy.wait()
    me_f, sib_f, over_f, diag_f = (v.astype(jnp.float32) for v in (f_send[...], f_all[0], f_all[1], f_all[2]))
    low_core, low_chip = core == 0, chip == 0
    core0 = [jnp.where(low_core, a, b) for a, b in ((me_f, sib_f), (over_f, diag_f))]
    core1 = [jnp.where(low_core, b, a) for a, b in ((me_f, sib_f), (over_f, diag_f))]
    order = [
        jnp.where(low_chip, core0[0], core0[1]),
        jnp.where(low_chip, core0[1], core0[0]),
        jnp.where(low_chip, core1[0], core1[1]),
        jnp.where(low_chip, core1[1], core1[0]),
    ]
    f_bf = jnp.concatenate(order, axis=0).astype(jnp.bfloat16)
    f_own[...] = f_bf
    f_two[pl.ds(0, batch)] = f_bf
    fo = remote(f_own, f_oth, sem_fo, pair)
    fo.start()
    pl.loop(early, half)(lambda j: nr_copy(j).start())

    bv[...] = jnp.full_like(bv, NEG)
    bi[...] = jnp.zeros_like(bi)
    c1 = temp_ref[0:1, 0:1]
    c2 = temp_ref[1:2, 0:1]

    def score(i, rows, nz_refs):
        slot = lax.rem(i + 3, RING_GROUPS)
        group = i + jnp.where(i < OWN, 0, dp * half)
        for j in range(NSUB):
            e_copy(i, j).wait()
        lhs = f_two[pl.ds(0, rows)]
        for j in range(NSUB):
            block = ring[pl.ds(pl.multiple_of(slot * GROUP + j * SUB, SUB), SUB), :]
            z = lax.dot_general(lhs, block, (((1,), (1,)), ((), ())), preferred_element_type=jnp.float32)
            s = jnp.tanh(z * (1.0 / SOFT_CAP)) * c1 * c2
            for part, nz in enumerate(nz_refs):
                take_rows = pl.ds(part * batch, batch)
                for q in range(SUB // 256):
                    v = s[part * batch : (part + 1) * batch, q * 256 : (q + 1) * 256]
                    v = v + nz[:, j * SUB + q * 256 : j * SUB + (q + 1) * 256]
                    old = bv[take_rows]
                    better = v > old
                    bv[take_rows] = jnp.where(better, v, old)
                    bi[take_rows] = jnp.where(better, group * (GROUP // 256) + (j * (SUB // 256) + q), bi[take_rows])

        @pl.when(i + RING_GROUPS < n_iter)
        def _():
            e_start(i + RING_GROUPS)

    @pl.loop(0, OWN)
    def _(i):
        no_copy(i).wait()
        score(i, batch, [nz_own.at[i]])

    fo.wait()
    f_two[pl.ds(batch, batch)] = f_oth[...]

    @pl.loop(OWN, n_iter)
    def _(i):
        no_copy(i).wait()
        nr_copy(i - OWN).wait_recv()
        score(i, 2 * batch, [nz_own.at[i], nz_oth.at[i - OWN]])

    pl.loop(0, half)(lambda j: nr_copy(j).wait_send())

    def settle(part):
        val = bv[pl.ds(part * batch, batch)]
        tile = bi[pl.ds(part * batch, batch)]
        top = jnp.max(val, axis=1, keepdims=True)
        ids = (tile * 256 + lax.broadcasted_iota(jnp.int32, tile.shape, 1)).astype(jnp.float32)
        row = jnp.min(jnp.where(val == top, ids, 3.0e7), axis=1, keepdims=True)
        return jnp.broadcast_to(top, (batch, 128)), jnp.broadcast_to(row, (batch, 128))

    o_val, o_row = settle(1)
    best_oth[0] = o_val
    best_oth[1] = o_row
    by = remote(best_oth, best_in, sem_by, pair)
    by.start()
    m_val, m_row = settle(0)
    by.wait()
    keep = m_val >= best_in[0]
    best_ref[0] = jnp.where(keep, m_val, best_in[0])
    best_ref[1] = jnp.where(keep, m_row, best_in[1])


def call_step(step, steps, batch, width, inner, vocab_local, embed_scale, operands):
    first, last = step == 0, step == steps
    f32, bf16, i32 = jnp.float32, jnp.bfloat16, jnp.int32
    vmem, hbm = pl.BlockSpec(memory_space=pltpu.VMEM), pl.BlockSpec(memory_space=pl.ANY)
    dma = pltpu.SemaphoreType.DMA
    n_group = vocab_local // GROUP
    half = (n_group - OWN) // 2
    n_iter = OWN + half
    hb, quarter = batch // 2, batch // 4
    in_specs = [vmem] * (1 if first else 2)
    if not last:
        in_specs += [vmem] * 4 + [hbm] * 5
    outs, scratch = [], []
    if not first:
        outs += [jax.ShapeDtypeStruct((batch, 128), i32), jax.ShapeDtypeStruct((batch, width), bf16)]
        rows, meta = pltpu.VMEM((hb, width), bf16), pltpu.VMEM((2, hb, 128), f32)
        scratch += [rows, meta] * 5 + [dma((3, 2)), dma((3, 2))]
    if not last:
        outs += [jax.ShapeDtypeStruct((2, batch, 128), f32)]
        scratch += [
            pltpu.VMEM((RING_GROUPS * GROUP, width), bf16),
            pltpu.VMEM((n_iter, batch, GROUP), f32),
            pltpu.VMEM((half, batch, GROUP), f32),
            pltpu.VMEM((4, quarter, width), f32),
            pltpu.VMEM((2, quarter, width), f32),
            pltpu.VMEM((2, quarter, width), f32),
            pltpu.VMEM((quarter, width), f32),
            pltpu.VMEM((quarter, width), bf16),
            pltpu.VMEM((3, quarter, width), bf16),
            pltpu.VMEM((batch, width), bf16),
            pltpu.VMEM((batch, width), bf16),
            pltpu.VMEM((2 * batch, width), bf16),
            pltpu.VMEM((4, quarter, width), f32),
            pltpu.VMEM((batch, inner), bf16),
            pltpu.VMEM((2 * batch, 256), f32),
            pltpu.VMEM((2 * batch, 256), i32),
            pltpu.VMEM((2, batch, 128), f32),
            pltpu.VMEM((2, batch, 128), f32),
            dma((3,)),
            dma((RING_GROUPS, NSUB)),
            dma((n_iter,)),
            dma((half,)),
            dma((half,)),
            dma((2,)),
            dma((2,)),
            dma((3, 2)),
            dma((2,)),
            dma((2,)),
        ]
    return pl.pallas_call(
        functools.partial(step_kernel, (step, first, last, n_group, embed_scale)),
        out_shape=outs,
        in_specs=in_specs,
        out_specs=[vmem] * len(outs),
        scratch_shapes=scratch,
        compiler_params=pltpu.CompilerParams(
            collective_id=step, has_side_effects=True, vmem_limit_bytes=66_000_000 if not last else 16_000_000
        ),
        name=f"step{step}",
    )(*operands)


def solution(mesh):
    def local_steps(start_hidden, embedding, pre_norm, w_gate, w_up, w_down, post_norm, final_norm, temperature, step_noise):
        vocab_local, width = embedding.shape
        batch, steps = start_hidden.shape[0], step_noise.shape[0]
        inner = w_gate.shape[1]
        row_offset = (lax.axis_index("tp") * vocab_local).astype(jnp.float32)
        embed_scale = float(np.float64(math.sqrt(width)).astype(jnp.bfloat16))
        a = jnp.where(temperature > 2.0**64, 2.0**-64, 1.0).astype(jnp.float32)
        temp = jnp.broadcast_to(jnp.stack([SOFT_CAP * a, 1.0 / (temperature * a)])[:, None], (2, 128))
        norms = [v[None] for v in (pre_norm, post_norm, final_norm)]
        common = [*norms, temp, w_gate, w_up, w_down, embedding, step_noise]
        sizes = (steps, batch, width, inner, vocab_local, embed_scale)
        (best,) = call_step(0, *sizes, [start_hidden, *common])
        token_list = []
        for step in range(1, steps + 1):
            local_row = best[1, :, 0].astype(jnp.int32)
            rows = jnp.take(embedding, local_row, axis=0, mode="clip").reshape(2, batch // 2, width)
            meta = jnp.stack([best[0], best[1] + row_offset]).reshape(2, 2, batch // 2, 128).transpose(1, 0, 2, 3)
            outs = call_step(step, *sizes, [rows, meta, *(common if step < steps else [])])
            token_list.append(outs[0][:, 0])
            hidden = outs[1]
            if step < steps:
                best = outs[2]
        return jnp.stack(token_list), hidden

    return jax.shard_map(
        local_steps,
        mesh=mesh,
        in_specs=(P("dp", None), P("tp", None), P(), P(None, "tp"), P(None, "tp"), P("tp", None), P(), P(), P(), P(None, "dp", "tp")),
        out_specs=(P(None, "dp"), P("dp", None)),
        check_vma=False,
    )
```

```python
import functools
import math

import jax
import jax.numpy as jnp
import numpy as np
from jax import lax
from jax.experimental import pallas as pl
from jax.experimental.pallas import tpu as pltpu
from jax.sharding import PartitionSpec as P

SOFT_CAP = 30.0
EPSILON = 1e-6
MESH = pl.DeviceIdType.MESH

SUB = 512
NSUB = 5
GROUP = SUB * NSUB
RING_GROUPS = 4
HEAD = 8
TAIL = 1
OWN = HEAD + TAIL
NEG = -3.0e38


def gain(ref):
    return ref[...].astype(jnp.float32).reshape(1, ref.shape[0])


def rms_scale(x_f32, gain_row):
    mean_sq = jnp.mean(x_f32 * x_f32, axis=-1, keepdims=True)
    return x_f32 * lax.rsqrt(mean_sq + EPSILON) * (1.0 + gain_row)


def remote(src, dst, sem, peer):
    return pltpu.make_async_remote_copy(
        src_ref=src, dst_ref=dst, send_sem=sem.at[0], recv_sem=sem.at[1], device_id=peer, device_id_type=MESH
    )


def as_line(wide):
    eye = lax.broadcasted_iota(jnp.int32, wide.shape, 0) == lax.broadcasted_iota(jnp.int32, wide.shape, 1)
    return jnp.sum(jnp.where(eye, wide, 0), axis=0, keepdims=True)


def step_kernel(cfg, *refs):
    step, first, last, n_group, embed_scale = cfg
    refs = list(refs)
    take = lambda n: [refs.pop(0) for _ in range(n)]
    if first:
        (hid_ref,) = take(1)
    else:
        rows_ref, meta_ref = take(2)
        if last:
            old_refs = take(step - 1)
    if not last:
        pre_ref, post_ref, fin_ref, temp_ref, wg_ref, wu_ref, wd_ref, emb_ref, noise_ref = take(9)
    if not first:
        tok_ref, hout_ref = take(2)
    if not last:
        best_ref, line_ref = take(2)
    if not first:
        rows_a, meta_a, rows_m, meta_m, rows_b, meta_b, rows_f, meta_f, rows_c, meta_c, sem_rows, sem_meta = take(12)
    if not last:
        (ring, nz_own, nz_oth, part_s, part_a, half_s, part_b, f_send, f_all, f_own, f_oth, f_two,
         hid32, gate_s, bv, bi, best_oth, best_in,
         sem_w, sem_e, sem_no, sem_ns, sem_nr, sem_ra, sem_rb, sem_f, sem_fo, sem_by) = take(28)

    dp, tp = lax.axis_index("dp"), lax.axis_index("tp")
    core, chip = lax.rem(tp, 2), lax.div(tp, 2)
    tp_sib = chip * 2 + (1 - core)
    tp_x = (1 - chip) * 2 + core
    tp_diag = (1 - chip) * 2 + (1 - core)
    sib, over, diag, pair = (dp, tp_sib), (dp, tp_x), (dp, tp_diag), (1 - dp, tp)

    if not last:
        half = (n_group - OWN) // 2
        n_iter = OWN + half
        width = ring.shape[1]
        inner = wg_ref.shape[1]
        w_copies = [
            pltpu.make_async_copy(wg_ref, ring.at[pl.ds(0, width)], sem_w.at[0]),
            pltpu.make_async_copy(wu_ref, ring.at[pl.ds(width, width)], sem_w.at[1]),
            pltpu.make_async_copy(wd_ref, ring.at[pl.ds(2 * width, inner)], sem_w.at[2]),
        ]

        def group_of(i):
            moved = jnp.where(i < HEAD + half, dp * half, half)
            return i + jnp.where(i < HEAD, 0, moved)

        def e_copy(i, j):
            group = group_of(i)
            slot = lax.rem(i + 3, RING_GROUPS)
            return pltpu.make_async_copy(
                emb_ref.at[pl.ds(group * GROUP + j * SUB, SUB)],
                ring.at[pl.ds(slot * GROUP + j * SUB, SUB)],
                sem_e.at[slot, j],
            )

        def e_start(i):
            for j in range(NSUB):
                e_copy(i, j).start()

        def no_copy(i):
            group = group_of(i)
            return pltpu.make_async_copy(
                noise_ref.at[step, :, pl.ds(group * GROUP, GROUP)], nz_own.at[i], sem_no.at[i]
            )

        def nr_copy(j):
            group = HEAD + (1 - dp) * half + j
            return pltpu.make_async_remote_copy(
                src_ref=noise_ref.at[step, :, pl.ds(group * GROUP, GROUP)],
                dst_ref=nz_oth.at[j],
                send_sem=sem_ns.at[j],
                recv_sem=sem_nr.at[j],
                device_id=pair,
                device_id_type=MESH,
            )

        for copy in w_copies:
            copy.start()
        e_start(0)
        pl.loop(0, n_iter)(lambda i: no_copy(i).start())

    barrier = pltpu.get_barrier_semaphore()
    peers = (sib, over) if last else (sib, over, diag, pair)
    for peer in peers:
        pl.semaphore_signal(barrier, inc=1, device_id=peer, device_id_type=MESH)
    pl.semaphore_wait(barrier, len(peers))

    if not last:
        early = 3
        pl.loop(0, early)(lambda j: nr_copy(j).start())

    if first:
        hid = hid_ref[...].astype(jnp.float32)
    else:
        a_rows = remote(rows_ref.at[1 - core], rows_a, sem_rows.at[0], sib)
        a_meta = remote(meta_ref.at[1 - core], meta_a, sem_meta.at[0], sib)
        a_rows.start()
        a_meta.start()
        a_rows.wait()
        a_meta.wait()
        mine = meta_ref[core]
        seen = meta_a[...]
        keep = mine[0] >= seen[0]
        meta_m[...] = jnp.where(keep[None], mine, seen)
        rows_m[...] = jnp.where(
            keep[:, :1], rows_ref[core].astype(jnp.float32), rows_a[...].astype(jnp.float32)
        ).astype(jnp.bfloat16)
        b_rows = remote(rows_m, rows_b, sem_rows.at[1], over)
        b_meta = remote(meta_m, meta_b, sem_meta.at[1], over)
        b_rows.start()
        b_meta.start()
        b_rows.wait()
        b_meta.wait()
        mine = meta_m[...]
        seen = meta_b[...]
        keep = mine[0] >= seen[0]
        meta_f[...] = jnp.where(keep[None], mine, seen)
        rows_f[...] = jnp.where(
            keep[:, :1], rows_m[...].astype(jnp.float32), rows_b[...].astype(jnp.float32)
        ).astype(jnp.bfloat16)
        c_rows = remote(rows_f, rows_c, sem_rows.at[2], sib)
        c_meta = remote(meta_f, meta_c, sem_meta.at[2], sib)
        c_rows.start()
        c_meta.start()
        c_rows.wait()
        c_meta.wait()
        low = core == 0
        r_f, r_c = rows_f[...].astype(jnp.float32), rows_c[...].astype(jnp.float32)
        t_f, t_c = meta_f[1], meta_c[1]
        picked = jnp.concatenate([jnp.where(low, r_f, r_c), jnp.where(low, r_c, r_f)], axis=0)
        token = jnp.concatenate([jnp.where(low, t_f, t_c), jnp.where(low, t_c, t_f)], axis=0).astype(jnp.int32)
        if last:
            for k, line in enumerate([ref[...] for ref in old_refs] + [as_line(token)]):
                tok_ref[k : k + 1] = line[:, : token.shape[0]]
        else:
            tok_ref[...] = as_line(token)
        hid_bf = (picked * embed_scale).astype(jnp.bfloat16)
        hout_ref[...] = hid_bf
        hid = hid_bf.astype(jnp.float32)

    if last:
        return

    batch = hid.shape[0]
    quarter = batch // 4
    hid32[...] = hid.reshape(4, quarter, width)
    normed = rms_scale(hid, gain(pre_ref)).astype(jnp.bfloat16)
    f_two[pl.ds(0, batch)] = normed
    w_copies[0].wait()
    w_copies[1].wait()
    col = 768

    @pl.loop(0, inner // col)
    def _(n):
        cols = pl.ds(pl.multiple_of(n * col, col), col)
        lhs = f_two[pl.ds(0, batch)]
        gate = jnp.dot(lhs, ring[pl.ds(0, width), cols], preferred_element_type=jnp.float32)
        up = jnp.dot(lhs, ring[pl.ds(width, width), cols], preferred_element_type=jnp.float32)
        gate_s[:, cols] = (jax.nn.gelu(gate, approximate=True) * up).astype(jnp.bfloat16)

    e_start(1)
    w_copies[2].wait()

    @pl.loop(0, width // col)
    def _(n):
        cols = pl.ds(pl.multiple_of(n * col, col), col)
        part_s[:, :, cols] = jnp.dot(
            gate_s[...], ring[pl.ds(2 * width, inner), cols], preferred_element_type=jnp.float32
        ).reshape(4, quarter, col)

    e_start(2)
    e_start(3)

    ra = remote(part_s.at[pl.ds(2 * (1 - core), 2)], part_a, sem_ra, sib)
    ra.start()
    ra.wait()
    half_s[...] = part_s[pl.ds(2 * core, 2)] + part_a[...]
    rb = remote(half_s.at[1 - chip], part_b, sem_rb, over)
    rb.start()
    rb.wait()
    down_sum = half_s[chip] + part_b[...]
    place = 2 * core + chip
    post_out = rms_scale(down_sum, gain(post_ref)).astype(jnp.bfloat16)
    resid = (hid32[place] + post_out.astype(jnp.float32)).astype(jnp.bfloat16)
    final_in = rms_scale(resid.astype(jnp.float32), gain(fin_ref)).astype(jnp.bfloat16)
    f_send[...] = final_in
    f_copies = [remote(f_send, f_all.at[k], sem_f.at[k], peer) for k, peer in enumerate((sib, over, diag))]
    for copy in f_copies:
        copy.start()
    for copy in f_copies:
        copy.wait()
    me_f, sib_f, over_f, diag_f = (v.astype(jnp.float32) for v in (f_send[...], f_all[0], f_all[1], f_all[2]))
    low_core, low_chip = core == 0, chip == 0
    core0 = [jnp.where(low_core, a, b) for a, b in ((me_f, sib_f), (over_f, diag_f))]
    core1 = [jnp.where(low_core, b, a) for a, b in ((me_f, sib_f), (over_f, diag_f))]
    order = [
        jnp.where(low_chip, core0[0], core0[1]),
        jnp.where(low_chip, core0[1], core0[0]),
        jnp.where(low_chip, core1[0], core1[1]),
        jnp.where(low_chip, core1[1], core1[0]),
    ]
    f_bf = jnp.concatenate(order, axis=0).astype(jnp.bfloat16)
    f_own[...] = f_bf
    f_two[pl.ds(0, batch)] = f_bf
    fo = remote(f_own, f_oth, sem_fo, pair)
    fo.start()
    pl.loop(early, half)(lambda j: nr_copy(j).start())

    bv[...] = jnp.full_like(bv, NEG)
    bi[...] = jnp.zeros_like(bi)
    heat = jnp.full((1, 128), temp_ref[0, 0], jnp.float32)
    fold = jnp.where(heat > 2.0**64, 2.0**-64, 1.0)
    c1 = (SOFT_CAP * fold)[:, :1]
    c2 = (1.0 / (heat * fold))[:, :1]

    def score(i, rows, nz_refs):
        slot = lax.rem(i + 3, RING_GROUPS)
        group = group_of(i)
        for j in range(NSUB):
            e_copy(i, j).wait()
        lhs = f_two[pl.ds(0, rows)]
        for j in range(NSUB):
            block = ring[pl.ds(pl.multiple_of(slot * GROUP + j * SUB, SUB), SUB), :]
            z = lax.dot_general(lhs, block, (((1,), (1,)), ((), ())), preferred_element_type=jnp.float32)
            s = jnp.tanh(z * (1.0 / SOFT_CAP)) * c1 * c2
            for part, nz in enumerate(nz_refs):
                take_rows = pl.ds(part * batch, batch)
                for q in range(SUB // 256):
                    v = s[part * batch : (part + 1) * batch, q * 256 : (q + 1) * 256]
                    v = v + nz[:, j * SUB + q * 256 : j * SUB + (q + 1) * 256]
                    old = bv[take_rows]
                    better = v > old
                    bv[take_rows] = jnp.where(better, v, old)
                    bi[take_rows] = jnp.where(better, group * (GROUP // 256) + (j * (SUB // 256) + q), bi[take_rows])

        @pl.when(i + RING_GROUPS < n_iter)
        def _():
            e_start(i + RING_GROUPS)

    def own(i):
        no_copy(i).wait()
        score(i, batch, [nz_own.at[i]])

    pl.loop(0, HEAD)(own)
    fo.wait()
    f_two[pl.ds(batch, batch)] = f_oth[...]

    @pl.loop(HEAD, HEAD + half)
    def _(i):
        no_copy(i).wait()
        nr_copy(i - HEAD).wait_recv()
        score(i, 2 * batch, [nz_own.at[i], nz_oth.at[i - HEAD]])

    def settle(part):
        val = bv[pl.ds(part * batch, batch)]
        tile = bi[pl.ds(part * batch, batch)]
        top = jnp.max(val, axis=1, keepdims=True)
        ids = (tile * 256 + lax.broadcasted_iota(jnp.int32, tile.shape, 1)).astype(jnp.float32)
        row = jnp.min(jnp.where(val == top, ids, 3.0e7), axis=1, keepdims=True)
        return jnp.broadcast_to(top, (batch, 128)), jnp.broadcast_to(row, (batch, 128))

    o_val, o_row = settle(1)
    best_oth[0] = o_val
    best_oth[1] = o_row
    by = remote(best_oth, best_in, sem_by, pair)
    by.start()
    pl.loop(HEAD + half, n_iter)(own)
    pl.loop(0, half)(lambda j: nr_copy(j).wait_send())
    m_val, m_row = settle(0)
    by.wait()
    keep = m_val >= best_in[0]
    top = jnp.where(keep, m_val, best_in[0])
    row = jnp.where(keep, m_row, best_in[1])
    offset = (tp * (n_group * GROUP)).astype(jnp.float32)
    hb = batch // 2
    for part in range(2):
        best_ref[part, 0] = top[part * hb : (part + 1) * hb]
        best_ref[part, 1] = row[part * hb : (part + 1) * hb] + offset
    line_ref[...] = as_line(row.astype(jnp.int32))


def lookup_kernel(line_ref, emb_ref, out_ref, tiles, sem):
    half, batch = out_ref.shape[1], 2 * out_ref.shape[1]
    for r in range(batch):
        base = pl.multiple_of(lax.div(line_ref[0, r], 8) * 8, 8)
        pltpu.make_async_copy(emb_ref.at[pl.ds(base, 8)], tiles.at[pl.ds(8 * r, 8)], sem).start()
    shape = (batch, 8 * batch)
    place = lax.broadcasted_iota(jnp.int32, (batch, 1), 0)
    want = 8 * place
    for r in range(batch):
        want = want + jnp.where(place == r, lax.rem(line_ref[0, r], 8), 0)
    pick = (lax.broadcasted_iota(jnp.int32, shape, 1) == want).astype(jnp.bfloat16)
    pltpu.make_async_copy(emb_ref.at[pl.ds(0, 8 * batch)], tiles, sem).wait()
    rows = jnp.dot(pick, tiles[...], preferred_element_type=jnp.float32).astype(jnp.bfloat16)
    out_ref[0] = rows[:half]
    out_ref[1] = rows[half:]


def lookup(line, batch, embedding):
    width = embedding.shape[1]
    return pl.pallas_call(
        lookup_kernel,
        out_shape=jax.ShapeDtypeStruct((2, batch // 2, width), jnp.bfloat16),
        in_specs=[pl.BlockSpec(memory_space=pltpu.SMEM), pl.BlockSpec(memory_space=pl.ANY)],
        out_specs=pl.BlockSpec(memory_space=pltpu.VMEM),
        scratch_shapes=[pltpu.VMEM((8 * batch, width), jnp.bfloat16), pltpu.SemaphoreType.DMA(())],
        compiler_params=pltpu.CompilerParams(vmem_limit_bytes=66_000_000),
        name="lookup",
    )(line, embedding)


def call_step(step, steps, batch, width, inner, vocab_local, embed_scale, operands):
    first, last = step == 0, step == steps
    f32, bf16, i32 = jnp.float32, jnp.bfloat16, jnp.int32
    vmem, hbm = pl.BlockSpec(memory_space=pltpu.VMEM), pl.BlockSpec(memory_space=pl.ANY)
    dma = pltpu.SemaphoreType.DMA
    n_group = vocab_local // GROUP
    half = (n_group - OWN) // 2
    n_iter = OWN + half
    hb, quarter = batch // 2, batch // 4
    in_specs = [vmem] * (1 if first else 2 + (step - 1) * last)
    if not last:
        in_specs += [vmem] * 3 + [pl.BlockSpec(memory_space=pltpu.SMEM)] + [hbm] * 5
    outs, scratch = [], []
    if not first:
        outs += [jax.ShapeDtypeStruct((steps, batch) if last else (1, 128), i32), jax.ShapeDtypeStruct((batch, width), bf16)]
        rows, meta = pltpu.VMEM((hb, width), bf16), pltpu.VMEM((2, hb, 128), f32)
        scratch += [rows, meta] * 5 + [dma((3, 2)), dma((3, 2))]
    if not last:
        outs += [
            jax.ShapeDtypeStruct((2, 2, hb, 128), f32),
            jax.ShapeDtypeStruct((1, 128), i32),
        ]
        scratch += [
            pltpu.VMEM((RING_GROUPS * GROUP, width), bf16),
            pltpu.VMEM((n_iter, batch, GROUP), f32),
            pltpu.VMEM((half, batch, GROUP), f32),
            pltpu.VMEM((4, quarter, width), f32),
            pltpu.VMEM((2, quarter, width), f32),
            pltpu.VMEM((2, quarter, width), f32),
            pltpu.VMEM((quarter, width), f32),
            pltpu.VMEM((quarter, width), bf16),
            pltpu.VMEM((3, quarter, width), bf16),
            pltpu.VMEM((batch, width), bf16),
            pltpu.VMEM((batch, width), bf16),
            pltpu.VMEM((2 * batch, width), bf16),
            pltpu.VMEM((4, quarter, width), f32),
            pltpu.VMEM((batch, inner), bf16),
            pltpu.VMEM((2 * batch, 256), f32),
            pltpu.VMEM((2 * batch, 256), i32),
            pltpu.VMEM((2, batch, 128), f32),
            pltpu.VMEM((2, batch, 128), f32),
            dma((3,)),
            dma((RING_GROUPS, NSUB)),
            dma((n_iter,)),
            dma((half,)),
            dma((half,)),
            dma((2,)),
            dma((2,)),
            dma((3, 2)),
            dma((2,)),
            dma((2,)),
        ]
    return pl.pallas_call(
        functools.partial(step_kernel, (step, first, last, n_group, embed_scale)),
        out_shape=outs,
        in_specs=in_specs,
        out_specs=[vmem] * len(outs),
        scratch_shapes=scratch,
        compiler_params=pltpu.CompilerParams(
            collective_id=step, has_side_effects=True, vmem_limit_bytes=66_000_000
        ),
        name=f"step{step}",
    )(*operands)


def solution(mesh):
    def local_steps(start_hidden, embedding, pre_norm, w_gate, w_up, w_down, post_norm, final_norm, temperature, step_noise):
        vocab_local, width = embedding.shape
        batch, steps = start_hidden.shape[0], step_noise.shape[0]
        inner = w_gate.shape[1]
        embed_scale = float(np.float64(math.sqrt(width)).astype(jnp.bfloat16))
        common = [pre_norm, post_norm, final_norm, temperature.reshape(1, 1), w_gate, w_up, w_down, embedding, step_noise]
        sizes = (steps, batch, width, inner, vocab_local, embed_scale)
        best, line = call_step(0, *sizes, [start_hidden, *common])
        lines = []
        for step in range(1, steps):
            outs = call_step(step, *sizes, [lookup(line, batch, embedding), best, *common])
            lines.append(outs[0])
            best, line = outs[2:]
        tokens, hidden = call_step(steps, *sizes, [lookup(line, batch, embedding), best, *lines])
        return tokens, hidden

    return jax.shard_map(
        local_steps,
        mesh=mesh,
        in_specs=(P("dp", None), P("tp", None), P(), P(None, "tp"), P(None, "tp"), P("tp", None), P(), P(), P(), P(None, "dp", "tp")),
        out_specs=(P(None, "dp"), P("dp", None)),
        check_vma=False,
    )
```

```python
import functools
import math

import jax
import jax.numpy as jnp
import numpy as np
from jax import lax
from jax.experimental import pallas as pl
from jax.experimental.pallas import tpu as pltpu
from jax.sharding import PartitionSpec as P

SOFT_CAP = 30.0
EPSILON = 1e-6
MESH = pl.DeviceIdType.MESH

SUB = 512
NSUB = 5
GROUP = SUB * NSUB
RING_GROUPS = 4
TURNED = (1, 2, 4)
HEAD = 6
TAIL = 1
OWN = HEAD + TAIL
NEG = -3.0e38


def gain(ref):
    return ref[...].astype(jnp.float32).reshape(1, ref.shape[0])


def rms_scale(x_f32, gain_row):
    mean_sq = jnp.mean(x_f32 * x_f32, axis=-1, keepdims=True)
    return x_f32 * lax.rsqrt(mean_sq + EPSILON) * (1.0 + gain_row)


def remote(src, dst, sem, peer):
    return pltpu.make_async_remote_copy(
        src_ref=src, dst_ref=dst, send_sem=sem.at[0], recv_sem=sem.at[1], device_id=peer, device_id_type=MESH
    )


def as_line(wide):
    eye = lax.broadcasted_iota(jnp.int32, wide.shape, 0) == lax.broadcasted_iota(jnp.int32, wide.shape, 1)
    return jnp.sum(jnp.where(eye, wide, 0), axis=0, keepdims=True)


def step_kernel(cfg, *refs):
    step, first, last, n_group, embed_scale = cfg
    refs = list(refs)
    take = lambda n: [refs.pop(0) for _ in range(n)]
    if first:
        (hid_ref,) = take(1)
    else:
        rows_ref, meta_ref = take(2)
        if last:
            old_refs = take(step - 1)
    if not last:
        pre_ref, post_ref, fin_ref, temp_ref, wg_ref, wu_ref, wd_ref, emb_ref, noise_ref = take(9)
    if not first:
        tok_ref, hout_ref = take(2)
    if not last:
        best_ref, line_ref = take(2)
    if not first:
        rows_a, meta_a, rows_m, meta_m, rows_b, meta_b, rows_f, meta_f, rows_c, meta_c, sem_rows, sem_meta = take(12)
    if not last:
        (ring, nz_own, nz_oth, part_s, part_a, half_s, part_b, f_send, f_all, f_own, f_oth, f_two,
         hid32, gate_s, turned, bv, bi, best_oth, best_in,
         sem_w, sem_e, sem_no, sem_ns, sem_nr, sem_ra, sem_rb, sem_f, sem_fo, sem_by) = take(29)

    dp, tp = lax.axis_index("dp"), lax.axis_index("tp")
    core, chip = lax.rem(tp, 2), lax.div(tp, 2)
    tp_sib = chip * 2 + (1 - core)
    tp_x = (1 - chip) * 2 + core
    tp_diag = (1 - chip) * 2 + (1 - core)
    sib, over, diag, pair = (dp, tp_sib), (dp, tp_x), (dp, tp_diag), (1 - dp, tp)

    if not last:
        half = (n_group - OWN) // 2
        n_iter = OWN + half
        width = ring.shape[1]
        inner = wg_ref.shape[1]
        w_copies = [
            pltpu.make_async_copy(wg_ref, ring.at[pl.ds(0, width)], sem_w.at[0]),
            pltpu.make_async_copy(wu_ref, ring.at[pl.ds(width, width)], sem_w.at[1]),
            pltpu.make_async_copy(wd_ref, ring.at[pl.ds(2 * width, inner)], sem_w.at[2]),
        ]

        def group_of(i):
            moved = jnp.where(i < HEAD + half, dp * half, half)
            return i + jnp.where(i < HEAD, 0, moved)

        def e_copy(i, j):
            group = group_of(i)
            slot = lax.rem(i + 3, RING_GROUPS)
            return pltpu.make_async_copy(
                emb_ref.at[pl.ds(group * GROUP + j * SUB, SUB)],
                ring.at[pl.ds(slot * GROUP + j * SUB, SUB)],
                sem_e.at[slot, j],
            )

        def e_start(i):
            for j in range(NSUB):
                e_copy(i, j).start()

        def no_copy(i):
            group = group_of(i)
            return pltpu.make_async_copy(
                noise_ref.at[step, :, pl.ds(group * GROUP, GROUP)], nz_own.at[i], sem_no.at[i]
            )

        def nr_copy(j):
            group = HEAD + (1 - dp) * half + j
            return pltpu.make_async_remote_copy(
                src_ref=noise_ref.at[step, :, pl.ds(group * GROUP, GROUP)],
                dst_ref=nz_oth.at[j],
                send_sem=sem_ns.at[j],
                recv_sem=sem_nr.at[j],
                device_id=pair,
                device_id_type=MESH,
            )

        w_copies[0].start()
        w_copies[1].start()

    barrier = pltpu.get_barrier_semaphore()
    peers = (sib, over) if last else (sib, over, diag, pair)
    for peer in peers:
        pl.semaphore_signal(barrier, inc=1, device_id=peer, device_id_type=MESH)
    pl.semaphore_wait(barrier, len(peers))

    def fetch_head():
        e_start(0)
        pl.loop(0, n_iter)(lambda i: no_copy(i).start())

    if not last:
        early = 3
        pl.loop(0, early)(lambda j: nr_copy(j).start())

    if first:
        hid = hid_ref[...].astype(jnp.float32)
        w_copies[2].start()
        w_copies[0].wait()
        fetch_head()
    else:
        a_rows = remote(rows_ref.at[1 - core], rows_a, sem_rows.at[0], sib)
        a_meta = remote(meta_ref.at[1 - core], meta_a, sem_meta.at[0], sib)
        a_rows.start()
        a_meta.start()
        a_rows.wait()
        a_meta.wait()
        if not last:
            w_copies[2].start()
        mine = meta_ref[core]
        seen = meta_a[...]
        keep = mine[0] >= seen[0]
        meta_m[...] = jnp.where(keep[None], mine, seen)
        rows_m[...] = jnp.where(
            keep[:, :1], rows_ref[core].astype(jnp.float32), rows_a[...].astype(jnp.float32)
        ).astype(jnp.bfloat16)
        b_rows = remote(rows_m, rows_b, sem_rows.at[1], over)
        b_meta = remote(meta_m, meta_b, sem_meta.at[1], over)
        b_rows.start()
        b_meta.start()
        b_rows.wait()
        b_meta.wait()
        mine = meta_m[...]
        seen = meta_b[...]
        keep = mine[0] >= seen[0]
        meta_f[...] = jnp.where(keep[None], mine, seen)
        rows_f[...] = jnp.where(
            keep[:, :1], rows_m[...].astype(jnp.float32), rows_b[...].astype(jnp.float32)
        ).astype(jnp.bfloat16)
        c_rows = remote(rows_f, rows_c, sem_rows.at[2], sib)
        c_meta = remote(meta_f, meta_c, sem_meta.at[2], sib)
        c_rows.start()
        c_meta.start()
        c_rows.wait()
        c_meta.wait()
        if not last:
            w_copies[0].wait()
            fetch_head()
        low = core == 0
        r_f, r_c = rows_f[...].astype(jnp.float32), rows_c[...].astype(jnp.float32)
        t_f, t_c = meta_f[1], meta_c[1]
        picked = jnp.concatenate([jnp.where(low, r_f, r_c), jnp.where(low, r_c, r_f)], axis=0)
        token = jnp.concatenate([jnp.where(low, t_f, t_c), jnp.where(low, t_c, t_f)], axis=0).astype(jnp.int32)
        if last:
            for k, line in enumerate([ref[...] for ref in old_refs] + [as_line(token)]):
                tok_ref[k : k + 1] = line[:, : token.shape[0]]
        else:
            tok_ref[...] = as_line(token)
        hid_bf = (picked * embed_scale).astype(jnp.bfloat16)
        hout_ref[...] = hid_bf
        hid = hid_bf.astype(jnp.float32)

    if last:
        return

    batch = hid.shape[0]
    quarter = batch // 4
    hid32[...] = hid.reshape(4, quarter, width)
    normed = rms_scale(hid, gain(pre_ref)).astype(jnp.bfloat16)
    f_two[pl.ds(0, batch)] = normed
    w_copies[1].wait()
    col = 768

    @pl.loop(0, inner // col)
    def _(n):
        cols = pl.ds(pl.multiple_of(n * col, col), col)
        lhs = f_two[pl.ds(0, batch)]
        gate = jnp.dot(lhs, ring[pl.ds(0, width), cols], preferred_element_type=jnp.float32)
        up = jnp.dot(lhs, ring[pl.ds(width, width), cols], preferred_element_type=jnp.float32)
        gate_s[:, cols] = (jax.nn.gelu(gate, approximate=True) * up).astype(jnp.bfloat16)

    e_start(1)
    w_copies[2].wait()

    @pl.loop(0, width // col)
    def _(n):
        cols = pl.ds(pl.multiple_of(n * col, col), col)
        part_s[:, :, cols] = jnp.dot(
            gate_s[...], ring[pl.ds(2 * width, inner), cols], preferred_element_type=jnp.float32
        ).reshape(4, quarter, col)

    e_start(2)
    e_start(3)

    ra = remote(part_s.at[pl.ds(2 * (1 - core), 2)], part_a, sem_ra, sib)
    ra.start()
    ra.wait()
    half_s[...] = part_s[pl.ds(2 * core, 2)] + part_a[...]
    rb = remote(half_s.at[1 - chip], part_b, sem_rb, over)
    rb.start()
    rb.wait()
    down_sum = half_s[chip] + part_b[...]
    place = 2 * core + chip
    post_out = rms_scale(down_sum, gain(post_ref)).astype(jnp.bfloat16)
    resid = (hid32[place] + post_out.astype(jnp.float32)).astype(jnp.bfloat16)
    final_in = rms_scale(resid.astype(jnp.float32), gain(fin_ref)).astype(jnp.bfloat16)
    f_send[...] = final_in
    f_copies = [remote(f_send, f_all.at[k], sem_f.at[k], peer) for k, peer in enumerate((sib, over, diag))]
    for copy in f_copies:
        copy.start()
    for copy in f_copies:
        copy.wait()
    me_f, sib_f, over_f, diag_f = (v.astype(jnp.float32) for v in (f_send[...], f_all[0], f_all[1], f_all[2]))
    low_core, low_chip = core == 0, chip == 0
    core0 = [jnp.where(low_core, a, b) for a, b in ((me_f, sib_f), (over_f, diag_f))]
    core1 = [jnp.where(low_core, b, a) for a, b in ((me_f, sib_f), (over_f, diag_f))]
    order = [
        jnp.where(low_chip, core0[0], core0[1]),
        jnp.where(low_chip, core0[1], core0[0]),
        jnp.where(low_chip, core1[0], core1[1]),
        jnp.where(low_chip, core1[1], core1[0]),
    ]
    f_bf = jnp.concatenate(order, axis=0).astype(jnp.bfloat16)
    f_own[...] = f_bf
    f_two[pl.ds(0, batch)] = f_bf
    fo = remote(f_own, f_oth, sem_fo, pair)
    fo.start()
    pl.loop(early, half)(lambda j: nr_copy(j).start())

    bv[...] = jnp.full_like(bv, NEG)
    bi[...] = jnp.zeros_like(bi)
    heat = jnp.full((1, 128), temp_ref[0, 0], jnp.float32)
    fold = jnp.where(heat > 2.0**64, 2.0**-64, 1.0)
    c1 = (SOFT_CAP * fold)[:, :1]
    c2 = (1.0 / (heat * fold))[:, :1]

    def score(i, rows, nz_refs):
        slot = lax.rem(i + 3, RING_GROUPS)
        group = group_of(i)
        for j in range(NSUB):
            e_copy(i, j).wait()
        lhs = f_two[pl.ds(0, rows)]
        for j in range(NSUB):
            block = ring[pl.ds(pl.multiple_of(slot * GROUP + j * SUB, SUB), SUB), :]
            if j in TURNED:
                spare = TURNED.index(j) % turned.shape[0]
                for k in range(0, width, 256):
                    turned[spare, pl.ds(k, 256)] = block[:, k : k + 256].T
                z = jnp.dot(lhs, turned[spare], preferred_element_type=jnp.float32)
            else:
                z = lax.dot_general(lhs, block, (((1,), (1,)), ((), ())), preferred_element_type=jnp.float32)
            s = jnp.tanh(z * (1.0 / SOFT_CAP)) * c1 * c2
            for part, nz in enumerate(nz_refs):
                take_rows = pl.ds(part * batch, batch)
                for q in range(SUB // 256):
                    v = s[part * batch : (part + 1) * batch, q * 256 : (q + 1) * 256]
                    v = v + nz[:, j * SUB + q * 256 : j * SUB + (q + 1) * 256]
                    old = bv[take_rows]
                    better = v > old
                    bv[take_rows] = jnp.where(better, v, old)
                    bi[take_rows] = jnp.where(better, group * (GROUP // 256) + (j * (SUB // 256) + q), bi[take_rows])

        @pl.when(i + RING_GROUPS < n_iter)
        def _():
            e_start(i + RING_GROUPS)

    def own(i):
        no_copy(i).wait()
        score(i, batch, [nz_own.at[i]])

    def shared(i):
        no_copy(i).wait()
        nr_copy(i - HEAD).wait_recv()
        score(i, 2 * batch, [nz_own.at[i], nz_oth.at[i - HEAD]])

    def settle(part):
        val = bv[pl.ds(part * batch, batch)]
        tile = bi[pl.ds(part * batch, batch)]
        top = jnp.max(val, axis=1, keepdims=True)
        ids = (tile * 256 + lax.broadcasted_iota(jnp.int32, tile.shape, 1)).astype(jnp.float32)
        row = jnp.min(jnp.where(val == top, ids, 3.0e7), axis=1, keepdims=True)
        return jnp.broadcast_to(top, (batch, 128)), jnp.broadcast_to(row, (batch, 128))

    by = remote(best_oth, best_in, sem_by, pair)

    @pl.loop(0, 2)
    def _(phase):
        pl.loop(jnp.where(phase == 0, 0, HEAD + half), jnp.where(phase == 0, HEAD, n_iter))(own)

        @pl.when(phase == 0)
        def _():
            fo.wait()
            f_two[pl.ds(batch, batch)] = f_oth[...]
            pl.loop(HEAD, HEAD + half)(shared)
            o_val, o_row = settle(1)
            best_oth[0] = o_val
            best_oth[1] = o_row
            by.start()

    pl.loop(0, half)(lambda j: nr_copy(j).wait_send())
    m_val, m_row = settle(0)
    by.wait()
    keep = m_val >= best_in[0]
    top = jnp.where(keep, m_val, best_in[0])
    row = jnp.where(keep, m_row, best_in[1])
    offset = (tp * (n_group * GROUP)).astype(jnp.float32)
    hb = batch // 2
    for part in range(2):
        best_ref[part, 0] = top[part * hb : (part + 1) * hb]
        best_ref[part, 1] = row[part * hb : (part + 1) * hb] + offset
    line_ref[...] = as_line(row.astype(jnp.int32))


def lookup_kernel(line_ref, emb_ref, out_ref, tiles, sem):
    half, batch = out_ref.shape[1], 2 * out_ref.shape[1]
    for r in range(batch):
        base = pl.multiple_of(lax.div(line_ref[0, r], 8) * 8, 8)
        pltpu.make_async_copy(emb_ref.at[pl.ds(base, 8)], tiles.at[pl.ds(8 * r, 8)], sem).start()
    shape = (batch, 8 * batch)
    place = lax.broadcasted_iota(jnp.int32, (batch, 1), 0)
    want = 8 * place
    for r in range(batch):
        want = want + jnp.where(place == r, lax.rem(line_ref[0, r], 8), 0)
    pick = (lax.broadcasted_iota(jnp.int32, shape, 1) == want).astype(jnp.bfloat16)
    pltpu.make_async_copy(emb_ref.at[pl.ds(0, 8 * batch)], tiles, sem).wait()
    rows = jnp.dot(pick, tiles[...], preferred_element_type=jnp.float32).astype(jnp.bfloat16)
    out_ref[0] = rows[:half]
    out_ref[1] = rows[half:]


def lookup(line, batch, embedding):
    width = embedding.shape[1]
    return pl.pallas_call(
        lookup_kernel,
        out_shape=jax.ShapeDtypeStruct((2, batch // 2, width), jnp.bfloat16),
        in_specs=[pl.BlockSpec(memory_space=pltpu.SMEM), pl.BlockSpec(memory_space=pl.ANY)],
        out_specs=pl.BlockSpec(memory_space=pltpu.VMEM),
        scratch_shapes=[pltpu.VMEM((8 * batch, width), jnp.bfloat16), pltpu.SemaphoreType.DMA(())],
        compiler_params=pltpu.CompilerParams(vmem_limit_bytes=66_000_000),
        name="lookup",
    )(line, embedding)


def call_step(step, steps, batch, width, inner, vocab_local, embed_scale, operands):
    first, last = step == 0, step == steps
    f32, bf16, i32 = jnp.float32, jnp.bfloat16, jnp.int32
    vmem, hbm = pl.BlockSpec(memory_space=pltpu.VMEM), pl.BlockSpec(memory_space=pl.ANY)
    dma = pltpu.SemaphoreType.DMA
    n_group = vocab_local // GROUP
    half = (n_group - OWN) // 2
    n_iter = OWN + half
    hb, quarter = batch // 2, batch // 4
    in_specs = [vmem] * (1 if first else 2 + (step - 1) * last)
    if not last:
        in_specs += [vmem] * 3 + [pl.BlockSpec(memory_space=pltpu.SMEM)] + [hbm] * 5
    outs, scratch = [], []
    if not first:
        outs += [jax.ShapeDtypeStruct((steps, batch) if last else (1, 128), i32), jax.ShapeDtypeStruct((batch, width), bf16)]
        rows, meta = pltpu.VMEM((hb, width), bf16), pltpu.VMEM((2, hb, 128), f32)
        scratch += [rows, meta] * 5 + [dma((3, 2)), dma((3, 2))]
    if not last:
        outs += [
            jax.ShapeDtypeStruct((2, 2, hb, 128), f32),
            jax.ShapeDtypeStruct((1, 128), i32),
        ]
        scratch += [
            pltpu.VMEM((RING_GROUPS * GROUP, width), bf16),
            pltpu.VMEM((n_iter, batch, GROUP), f32),
            pltpu.VMEM((half, batch, GROUP), f32),
            pltpu.VMEM((4, quarter, width), f32),
            pltpu.VMEM((2, quarter, width), f32),
            pltpu.VMEM((2, quarter, width), f32),
            pltpu.VMEM((quarter, width), f32),
            pltpu.VMEM((quarter, width), bf16),
            pltpu.VMEM((3, quarter, width), bf16),
            pltpu.VMEM((batch, width), bf16),
            pltpu.VMEM((batch, width), bf16),
            pltpu.VMEM((2 * batch, width), bf16),
            pltpu.VMEM((4, quarter, width), f32),
            pltpu.VMEM((batch, inner), bf16),
            pltpu.VMEM((2, width, SUB), bf16),
            pltpu.VMEM((2 * batch, 256), f32),
            pltpu.VMEM((2 * batch, 256), i32),
            pltpu.VMEM((2, batch, 128), f32),
            pltpu.VMEM((2, batch, 128), f32),
            dma((3,)),
            dma((RING_GROUPS, NSUB)),
            dma((n_iter,)),
            dma((half,)),
            dma((half,)),
            dma((2,)),
            dma((2,)),
            dma((3, 2)),
            dma((2,)),
            dma((2,)),
        ]
    return pl.pallas_call(
        functools.partial(step_kernel, (step, first, last, n_group, embed_scale)),
        out_shape=outs,
        in_specs=in_specs,
        out_specs=[vmem] * len(outs),
        scratch_shapes=scratch,
        compiler_params=pltpu.CompilerParams(
            collective_id=step, has_side_effects=True, vmem_limit_bytes=66_000_000
        ),
        name=f"step{step}",
    )(*operands)


def solution(mesh):
    def local_steps(start_hidden, embedding, pre_norm, w_gate, w_up, w_down, post_norm, final_norm, temperature, step_noise):
        vocab_local, width = embedding.shape
        batch, steps = start_hidden.shape[0], step_noise.shape[0]
        inner = w_gate.shape[1]
        embed_scale = float(np.float64(math.sqrt(width)).astype(jnp.bfloat16))
        common = [pre_norm, post_norm, final_norm, temperature.reshape(1, 1), w_gate, w_up, w_down, embedding, step_noise]
        sizes = (steps, batch, width, inner, vocab_local, embed_scale)
        best, line = call_step(0, *sizes, [start_hidden, *common])
        lines = []
        for step in range(1, steps):
            outs = call_step(step, *sizes, [lookup(line, batch, embedding), best, *common])
            lines.append(outs[0])
            best, line = outs[2:]
        tokens, hidden = call_step(steps, *sizes, [lookup(line, batch, embedding), best, *lines])
        return tokens, hidden

    return jax.shard_map(
        local_steps,
        mesh=mesh,
        in_specs=(P("dp", None), P("tp", None), P(), P(None, "tp"), P(None, "tp"), P("tp", None), P(), P(), P(), P(None, "dp", "tp")),
        out_specs=(P(None, "dp"), P("dp", None)),
        check_vma=False,
    )
```

```python
import functools
import math

import jax
import jax.numpy as jnp
import numpy as np
from jax import lax
from jax.experimental import pallas as pl
from jax.experimental.pallas import tpu as pltpu
from jax.sharding import PartitionSpec as P

SOFT_CAP = 30.0
EPSILON = 1e-6
MESH = pl.DeviceIdType.MESH

SUB = 640
NSUB = 2
GROUP = SUB * NSUB
RING_GROUPS = 8
WEIGHT_GROUPS = 6
CUTS = ((0, 512, False), (512, 768, True))
HEAD = 14
TAIL = 2
OWN = HEAD + TAIL
NEG = -3.0e38


def gain(ref):
    return ref[...].astype(jnp.float32).reshape(1, ref.shape[0])


def rms_scale(x_f32, gain_row):
    mean_sq = jnp.mean(x_f32 * x_f32, axis=-1, keepdims=True)
    return x_f32 * lax.rsqrt(mean_sq + EPSILON) * (1.0 + gain_row)


def remote(src, dst, sem, peer):
    return pltpu.make_async_remote_copy(
        src_ref=src, dst_ref=dst, send_sem=sem.at[0], recv_sem=sem.at[1], device_id=peer, device_id_type=MESH
    )


def as_line(wide):
    eye = lax.broadcasted_iota(jnp.int32, wide.shape, 0) == lax.broadcasted_iota(jnp.int32, wide.shape, 1)
    return jnp.sum(jnp.where(eye, wide, 0), axis=0, keepdims=True)


def step_kernel(cfg, *refs):
    step, first, last, n_group, embed_scale = cfg
    refs = list(refs)
    take = lambda n: [refs.pop(0) for _ in range(n)]
    if first:
        (hid_ref,) = take(1)
    else:
        rows_ref, meta_ref = take(2)
        if last:
            old_refs = take(step - 1)
    if not last:
        pre_ref, post_ref, fin_ref, temp_ref, wg_ref, wu_ref, wd_ref, emb_ref, noise_ref = take(9)
    if not first:
        tok_ref, hout_ref = take(2)
    if not last:
        best_ref, line_ref = take(2)
    if not first:
        rows_a, meta_a, rows_m, meta_m, rows_b, meta_b, rows_f, meta_f, rows_c, meta_c, sem_rows, sem_meta = take(12)
    if not last:
        (ring, nz_own, nz_oth, part_s, part_a, half_s, part_b, f_send, f_all, f_pair, g_all, f_two,
         hid32, gate_s, turned, bv, bi, best_oth, best_in,
         sem_w, sem_e, sem_no, sem_ns, sem_nr, sem_ra, sem_rb, sem_f, sem_fo, sem_g, sem_by) = take(30)

    dp, tp = lax.axis_index("dp"), lax.axis_index("tp")
    core, chip = lax.rem(tp, 2), lax.div(tp, 2)
    tp_sib = chip * 2 + (1 - core)
    tp_x = (1 - chip) * 2 + core
    tp_diag = (1 - chip) * 2 + (1 - core)
    sib, over, diag, pair = (dp, tp_sib), (dp, tp_x), (dp, tp_diag), (1 - dp, tp)

    if not last:
        half = (n_group - OWN) // 2
        n_iter = OWN + half
        width = ring.shape[1]
        inner = wg_ref.shape[1]
        w_copies = [
            pltpu.make_async_copy(wg_ref, ring.at[pl.ds(0, width)], sem_w.at[0]),
            pltpu.make_async_copy(wu_ref, ring.at[pl.ds(width, width)], sem_w.at[1]),
            pltpu.make_async_copy(wd_ref, ring.at[pl.ds(2 * width, inner)], sem_w.at[2]),
        ]

        def group_of(i):
            moved = jnp.where(i < HEAD + half, dp * half, half)
            return i + jnp.where(i < HEAD, 0, moved)

        def e_copy(i, j):
            group = group_of(i)
            slot = lax.rem(i + WEIGHT_GROUPS, RING_GROUPS)
            return pltpu.make_async_copy(
                emb_ref.at[pl.ds(group * GROUP + j * SUB, SUB)],
                ring.at[pl.ds(slot * GROUP + j * SUB, SUB)],
                sem_e.at[slot, j],
            )

        def e_start(i):
            for j in range(NSUB):
                e_copy(i, j).start()

        def no_copy(i):
            group = group_of(i)
            return pltpu.make_async_copy(
                noise_ref.at[step, :, pl.ds(group * GROUP, GROUP)], nz_own.at[i], sem_no.at[i]
            )

        def nr_copy(j):
            group = HEAD + (1 - dp) * half + j
            return pltpu.make_async_remote_copy(
                src_ref=noise_ref.at[step, :, pl.ds(group * GROUP, GROUP)],
                dst_ref=nz_oth.at[j],
                send_sem=sem_ns.at[j],
                recv_sem=sem_nr.at[j],
                device_id=pair,
                device_id_type=MESH,
            )

        w_copies[0].start()
        w_copies[1].start()

    barrier = pltpu.get_barrier_semaphore()
    peers = (sib, over) if last else (sib, over, diag, pair)
    for peer in peers:
        pl.semaphore_signal(barrier, inc=1, device_id=peer, device_id_type=MESH)
    pl.semaphore_wait(barrier, len(peers))

    def fetch_head():
        e_start(0)
        e_start(1)
        pl.loop(0, n_iter)(lambda i: no_copy(i).start())

    if not last:
        early = 6
        pl.loop(0, early)(lambda j: nr_copy(j).start())

    if first:
        hid = hid_ref[...].astype(jnp.float32)
        w_copies[2].start()
        w_copies[0].wait()
        fetch_head()
    else:
        a_rows = remote(rows_ref.at[1 - core], rows_a, sem_rows.at[0], sib)
        a_meta = remote(meta_ref.at[1 - core], meta_a, sem_meta.at[0], sib)
        a_rows.start()
        a_meta.start()
        a_rows.wait()
        a_meta.wait()
        if not last:
            w_copies[2].start()
        mine = meta_ref[core]
        seen = meta_a[...]
        keep = mine[0] >= seen[0]
        meta_m[...] = jnp.where(keep[None], mine, seen)
        rows_m[...] = jnp.where(
            keep[:, :1], rows_ref[core].astype(jnp.float32), rows_a[...].astype(jnp.float32)
        ).astype(jnp.bfloat16)
        b_rows = remote(rows_m, rows_b, sem_rows.at[1], over)
        b_meta = remote(meta_m, meta_b, sem_meta.at[1], over)
        b_rows.start()
        b_meta.start()
        b_rows.wait()
        b_meta.wait()
        mine = meta_m[...]
        seen = meta_b[...]
        keep = mine[0] >= seen[0]
        meta_f[...] = jnp.where(keep[None], mine, seen)
        rows_f[...] = jnp.where(
            keep[:, :1], rows_m[...].astype(jnp.float32), rows_b[...].astype(jnp.float32)
        ).astype(jnp.bfloat16)
        c_rows = remote(rows_f, rows_c, sem_rows.at[2], sib)
        c_meta = remote(meta_f, meta_c, sem_meta.at[2], sib)
        c_rows.start()
        c_meta.start()
        c_rows.wait()
        c_meta.wait()
        if not last:
            w_copies[0].wait()
            fetch_head()
        low = core == 0
        r_f, r_c = rows_f[...].astype(jnp.float32), rows_c[...].astype(jnp.float32)
        t_f, t_c = meta_f[1], meta_c[1]
        picked = jnp.concatenate([jnp.where(low, r_f, r_c), jnp.where(low, r_c, r_f)], axis=0)
        token = jnp.concatenate([jnp.where(low, t_f, t_c), jnp.where(low, t_c, t_f)], axis=0).astype(jnp.int32)
        if last:
            for k, line in enumerate([ref[...] for ref in old_refs] + [as_line(token)]):
                tok_ref[k : k + 1] = line[:, : token.shape[0]]
        else:
            tok_ref[...] = as_line(token)
        hid_bf = (picked * embed_scale).astype(jnp.bfloat16)
        hout_ref[...] = hid_bf
        hid = hid_bf.astype(jnp.float32)

    if last:
        return

    batch = hid.shape[0]
    quarter = batch // 4
    hid32[...] = hid.reshape(4, quarter, width)
    normed = rms_scale(hid, gain(pre_ref)).astype(jnp.bfloat16)
    f_two[pl.ds(0, batch)] = normed
    w_copies[1].wait()
    col = 768

    @pl.loop(0, inner // col)
    def _(n):
        cols = pl.ds(pl.multiple_of(n * col, col), col)
        lhs = f_two[pl.ds(0, batch)]
        gate = jnp.dot(lhs, ring[pl.ds(0, width), cols], preferred_element_type=jnp.float32)
        up = jnp.dot(lhs, ring[pl.ds(width, width), cols], preferred_element_type=jnp.float32)
        gate_s[:, cols] = (jax.nn.gelu(gate, approximate=True) * up).astype(jnp.bfloat16)

    for i in range(2, 2 + (2 * width) // GROUP):
        e_start(i)
    w_copies[2].wait()

    @pl.loop(0, width // col)
    def _(n):
        cols = pl.ds(pl.multiple_of(n * col, col), col)
        part_s[:, :, cols] = jnp.dot(
            gate_s[...], ring[pl.ds(2 * width, inner), cols], preferred_element_type=jnp.float32
        ).reshape(4, quarter, col)

    for i in range(2 + (2 * width) // GROUP, RING_GROUPS):
        e_start(i)

    ra = remote(part_s.at[pl.ds(2 * (1 - core), 2)], part_a, sem_ra, sib)
    ra.start()
    ra.wait()
    half_s[...] = part_s[pl.ds(2 * core, 2)] + part_a[...]
    rb = remote(half_s.at[1 - chip], part_b, sem_rb, over)
    rb.start()
    rb.wait()
    down_sum = half_s[chip] + part_b[...]
    place = 2 * core + chip
    post_out = rms_scale(down_sum, gain(post_ref)).astype(jnp.bfloat16)
    resid = (hid32[place] + post_out.astype(jnp.float32)).astype(jnp.bfloat16)
    final_in = rms_scale(resid.astype(jnp.float32), gain(fin_ref)).astype(jnp.bfloat16)
    f_send[...] = final_in
    f_copies = [remote(f_send, f_all.at[k], sem_f.at[k], peer) for k, peer in enumerate((sib, over, diag))]
    f_pair_copy = remote(f_send, f_pair, sem_fo, pair)
    for copy in [*f_copies, f_pair_copy]:
        copy.start()
    pl.loop(early, half)(lambda j: nr_copy(j).start())
    for copy in f_copies:
        copy.wait()
    low_core, low_chip = core == 0, chip == 0

    def in_order(mine_ref, others_ref):
        me_f, sib_f, over_f, diag_f = (v.astype(jnp.float32) for v in (mine_ref[...], *(others_ref[k] for k in range(3))))
        core0 = [jnp.where(low_core, a, b) for a, b in ((me_f, sib_f), (over_f, diag_f))]
        core1 = [jnp.where(low_core, b, a) for a, b in ((me_f, sib_f), (over_f, diag_f))]
        order = [
            jnp.where(low_chip, core0[0], core0[1]),
            jnp.where(low_chip, core0[1], core0[0]),
            jnp.where(low_chip, core1[0], core1[1]),
            jnp.where(low_chip, core1[1], core1[0]),
        ]
        return jnp.concatenate(order, axis=0).astype(jnp.bfloat16)

    f_two[pl.ds(0, batch)] = in_order(f_send, f_all)
    f_pair_copy.wait()
    g_copies = [remote(f_pair, g_all.at[k], sem_g.at[k], peer) for k, peer in enumerate((sib, over, diag))]
    for copy in g_copies:
        copy.start()

    bv[...] = jnp.full_like(bv, NEG)
    bi[...] = jnp.zeros_like(bi)
    heat = jnp.full((1, 128), temp_ref[0, 0], jnp.float32)
    fold = jnp.where(heat > 2.0**64, 2.0**-64, 1.0)
    c1 = (SOFT_CAP * fold)[:, :1]
    c2 = (1.0 / (heat * fold))[:, :1]

    def score(i, rows, nz_refs):
        slot = lax.rem(i + WEIGHT_GROUPS, RING_GROUPS)
        group = group_of(i)
        for j in range(NSUB):
            e_copy(i, j).wait()
        lhs = f_two[pl.ds(0, rows)]
        for start, size, turn in CUTS:
            block = ring[pl.ds(pl.multiple_of(slot * GROUP + start, 256), size), :]
            if turn:
                for k in range(0, width, 256):
                    turned[pl.ds(k, 256)] = block[:, k : k + 256].T
                z = jnp.dot(lhs, turned[...], preferred_element_type=jnp.float32)
            else:
                z = lax.dot_general(lhs, block, (((1,), (1,)), ((), ())), preferred_element_type=jnp.float32)
            s = jnp.tanh(z * (1.0 / SOFT_CAP)) * c1 * c2
            for part, nz in enumerate(nz_refs):
                take_rows = pl.ds(part * batch, batch)
                for q in range(size // 256):
                    v = s[part * batch : (part + 1) * batch, q * 256 : (q + 1) * 256]
                    v = v + nz[:, start + q * 256 : start + (q + 1) * 256]
                    old = bv[take_rows]
                    better = v > old
                    bv[take_rows] = jnp.where(better, v, old)
                    bi[take_rows] = jnp.where(better, group * (GROUP // 256) + (start // 256 + q), bi[take_rows])

        @pl.when(i + RING_GROUPS < n_iter)
        def _():
            e_start(i + RING_GROUPS)

    def own(i):
        no_copy(i).wait()
        score(i, batch, [nz_own.at[i]])

    def shared(i):
        no_copy(i).wait()
        nr_copy(i - HEAD).wait_recv()
        score(i, 2 * batch, [nz_own.at[i], nz_oth.at[i - HEAD]])

    def settle(part):
        val = bv[pl.ds(part * batch, batch)]
        tile = bi[pl.ds(part * batch, batch)]
        top = jnp.max(val, axis=1, keepdims=True)
        ids = (tile * 256 + lax.broadcasted_iota(jnp.int32, tile.shape, 1)).astype(jnp.float32)
        row = jnp.min(jnp.where(val == top, ids, 3.0e7), axis=1, keepdims=True)
        return jnp.broadcast_to(top, (batch, 128)), jnp.broadcast_to(row, (batch, 128))

    by = remote(best_oth, best_in, sem_by, pair)

    @pl.loop(0, 2)
    def _(phase):
        pl.loop(jnp.where(phase == 0, 0, HEAD + half), jnp.where(phase == 0, HEAD, n_iter))(own)

        @pl.when(phase == 0)
        def _():
            for copy in g_copies:
                copy.wait()
            f_two[pl.ds(batch, batch)] = in_order(f_pair, g_all)
            pl.loop(HEAD, HEAD + half)(shared)
            o_val, o_row = settle(1)
            best_oth[0] = o_val
            best_oth[1] = o_row
            by.start()

    pl.loop(0, half)(lambda j: nr_copy(j).wait_send())
    m_val, m_row = settle(0)
    by.wait()
    keep = m_val >= best_in[0]
    top = jnp.where(keep, m_val, best_in[0])
    row = jnp.where(keep, m_row, best_in[1])
    offset = (tp * (n_group * GROUP)).astype(jnp.float32)
    hb = batch // 2
    for part in range(2):
        best_ref[part, 0] = top[part * hb : (part + 1) * hb]
        best_ref[part, 1] = row[part * hb : (part + 1) * hb] + offset
    line_ref[...] = as_line(row.astype(jnp.int32))


def lookup_kernel(line_ref, emb_ref, out_ref, tiles, sem):
    half, batch = out_ref.shape[1], 2 * out_ref.shape[1]
    for r in range(batch):
        base = pl.multiple_of(lax.div(line_ref[0, r], 8) * 8, 8)
        pltpu.make_async_copy(emb_ref.at[pl.ds(base, 8)], tiles.at[pl.ds(8 * r, 8)], sem).start()
    shape = (batch, 8 * batch)
    place = lax.broadcasted_iota(jnp.int32, (batch, 1), 0)
    want = 8 * place
    for r in range(batch):
        want = want + jnp.where(place == r, lax.rem(line_ref[0, r], 8), 0)
    pick = (lax.broadcasted_iota(jnp.int32, shape, 1) == want).astype(jnp.bfloat16)
    pltpu.make_async_copy(emb_ref.at[pl.ds(0, 8 * batch)], tiles, sem).wait()
    rows = jnp.dot(pick, tiles[...], preferred_element_type=jnp.float32).astype(jnp.bfloat16)
    out_ref[0] = rows[:half]
    out_ref[1] = rows[half:]


def lookup(line, batch, embedding):
    width = embedding.shape[1]
    return pl.pallas_call(
        lookup_kernel,
        out_shape=jax.ShapeDtypeStruct((2, batch // 2, width), jnp.bfloat16),
        in_specs=[pl.BlockSpec(memory_space=pltpu.SMEM), pl.BlockSpec(memory_space=pl.ANY)],
        out_specs=pl.BlockSpec(memory_space=pltpu.VMEM),
        scratch_shapes=[pltpu.VMEM((8 * batch, width), jnp.bfloat16), pltpu.SemaphoreType.DMA(())],
        compiler_params=pltpu.CompilerParams(vmem_limit_bytes=66_000_000),
        name="lookup",
    )(line, embedding)


def call_step(step, steps, batch, width, inner, vocab_local, embed_scale, operands):
    first, last = step == 0, step == steps
    f32, bf16, i32 = jnp.float32, jnp.bfloat16, jnp.int32
    vmem, hbm = pl.BlockSpec(memory_space=pltpu.VMEM), pl.BlockSpec(memory_space=pl.ANY)
    dma = pltpu.SemaphoreType.DMA
    n_group = vocab_local // GROUP
    half = (n_group - OWN) // 2
    n_iter = OWN + half
    hb, quarter = batch // 2, batch // 4
    in_specs = [vmem] * (1 if first else 2 + (step - 1) * last)
    if not last:
        in_specs += [vmem] * 3 + [pl.BlockSpec(memory_space=pltpu.SMEM)] + [hbm] * 5
    outs, scratch = [], []
    if not first:
        outs += [jax.ShapeDtypeStruct((steps, batch) if last else (1, 128), i32), jax.ShapeDtypeStruct((batch, width), bf16)]
        rows, meta = pltpu.VMEM((hb, width), bf16), pltpu.VMEM((2, hb, 128), f32)
        scratch += [rows, meta] * 5 + [dma((3, 2)), dma((3, 2))]
    if not last:
        outs += [
            jax.ShapeDtypeStruct((2, 2, hb, 128), f32),
            jax.ShapeDtypeStruct((1, 128), i32),
        ]
        scratch += [
            pltpu.VMEM((RING_GROUPS * GROUP, width), bf16),
            pltpu.VMEM((n_iter, batch, GROUP), f32),
            pltpu.VMEM((half, batch, GROUP), f32),
            pltpu.VMEM((4, quarter, width), f32),
            pltpu.VMEM((2, quarter, width), f32),
            pltpu.VMEM((2, quarter, width), f32),
            pltpu.VMEM((quarter, width), f32),
            pltpu.VMEM((quarter, width), bf16),
            pltpu.VMEM((3, quarter, width), bf16),
            pltpu.VMEM((quarter, width), bf16),
            pltpu.VMEM((3, quarter, width), bf16),
            pltpu.VMEM((2 * batch, width), bf16),
            pltpu.VMEM((4, quarter, width), f32),
            pltpu.VMEM((batch, inner), bf16),
            pltpu.VMEM((width, max(c[1] for c in CUTS if c[2])), bf16),
            pltpu.VMEM((2 * batch, 256), f32),
            pltpu.VMEM((2 * batch, 256), i32),
            pltpu.VMEM((2, batch, 128), f32),
            pltpu.VMEM((2, batch, 128), f32),
            dma((3,)),
            dma((RING_GROUPS, NSUB)),
            dma((n_iter,)),
            dma((half,)),
            dma((half,)),
            dma((2,)),
            dma((2,)),
            dma((3, 2)),
            dma((2,)),
            dma((3, 2)),
            dma((2,)),
        ]
    return pl.pallas_call(
        functools.partial(step_kernel, (step, first, last, n_group, embed_scale)),
        out_shape=outs,
        in_specs=in_specs,
        out_specs=[vmem] * len(outs),
        scratch_shapes=scratch,
        compiler_params=pltpu.CompilerParams(
            collective_id=step, has_side_effects=True, vmem_limit_bytes=66_000_000
        ),
        name=f"step{step}",
    )(*operands)


def solution(mesh):
    def local_steps(start_hidden, embedding, pre_norm, w_gate, w_up, w_down, post_norm, final_norm, temperature, step_noise):
        vocab_local, width = embedding.shape
        batch, steps = start_hidden.shape[0], step_noise.shape[0]
        inner = w_gate.shape[1]
        embed_scale = float(np.float64(math.sqrt(width)).astype(jnp.bfloat16))
        common = [pre_norm, post_norm, final_norm, temperature.reshape(1, 1), w_gate, w_up, w_down, embedding, step_noise]
        sizes = (steps, batch, width, inner, vocab_local, embed_scale)
        best, line = call_step(0, *sizes, [start_hidden, *common])
        lines = []
        for step in range(1, steps):
            outs = call_step(step, *sizes, [lookup(line, batch, embedding), best, *common])
            lines.append(outs[0])
            best, line = outs[2:]
        tokens, hidden = call_step(steps, *sizes, [lookup(line, batch, embedding), best, *lines])
        return tokens, hidden

    return jax.shard_map(
        local_steps,
        mesh=mesh,
        in_specs=(P("dp", None), P("tp", None), P(), P(None, "tp"), P(None, "tp"), P("tp", None), P(), P(), P(), P(None, "dp", "tp")),
        out_specs=(P(None, "dp"), P("dp", None)),
        check_vma=False,
    )
```

```python
import functools
import math

import jax
import jax.numpy as jnp
import numpy as np
from jax import lax
from jax.experimental import pallas as pl
from jax.experimental.pallas import tpu as pltpu
from jax.sharding import PartitionSpec as P

SOFT_CAP = 30.0
EPSILON = 1e-6
MESH = pl.DeviceIdType.MESH

SUB = 640
NSUB = 2
GROUP = SUB * NSUB
RING_GROUPS = 8
WEIGHT_GROUPS = 6
CUTS = ((0, 512, False), (512, 768, True))
HEAD = 14
TAIL = 2
OWN = HEAD + TAIL
NEG = -3.0e38


def gain(ref):
    return ref[...].astype(jnp.float32).reshape(1, ref.shape[0])


def rms_scale(x_f32, gain_row):
    mean_sq = jnp.mean(x_f32 * x_f32, axis=-1, keepdims=True)
    return x_f32 * lax.rsqrt(mean_sq + EPSILON) * (1.0 + gain_row)


def remote(src, dst, sem, peer):
    return pltpu.make_async_remote_copy(
        src_ref=src, dst_ref=dst, send_sem=sem.at[0], recv_sem=sem.at[1], device_id=peer, device_id_type=MESH
    )


def as_line(wide):
    eye = lax.broadcasted_iota(jnp.int32, wide.shape, 0) == lax.broadcasted_iota(jnp.int32, wide.shape, 1)
    return jnp.sum(jnp.where(eye, wide, 0), axis=0, keepdims=True)


def step_kernel(cfg, *refs):
    step, first, last, n_group, embed_scale = cfg
    refs = list(refs)
    take = lambda n: [refs.pop(0) for _ in range(n)]
    if first:
        (hid_ref,) = take(1)
    else:
        rows_ref, meta_ref = take(2)
        if last:
            old_refs = take(step - 1)
    if not last:
        pre_ref, post_ref, fin_ref, temp_ref, wg_ref, wu_ref, wd_ref, emb_ref, noise_ref = take(9)
    if not first:
        tok_ref, hout_ref = take(2)
    if not last:
        best_ref, line_ref = take(2)
    if not first:
        rows_a, meta_a, rows_m, meta_m, rows_b, meta_b, rows_f, meta_f, rows_c, meta_c, sem_rows, sem_meta = take(12)
    if not last:
        (ring, nz_own, nz_oth, part_s, part_a, half_s, part_b, f_send, f_all, f_pair, g_all, f_two,
         hid32, gate_s, turned, bv, bi, best_oth, best_in,
         sem_w, sem_e, sem_no, sem_ns, sem_nr, sem_ra, sem_rb, sem_f, sem_fo, sem_g, sem_by) = take(30)

    dp, tp = lax.axis_index("dp"), lax.axis_index("tp")
    core, chip = lax.rem(tp, 2), lax.div(tp, 2)
    tp_sib = chip * 2 + (1 - core)
    tp_x = (1 - chip) * 2 + core
    tp_diag = (1 - chip) * 2 + (1 - core)
    sib, over, diag, pair = (dp, tp_sib), (dp, tp_x), (dp, tp_diag), (1 - dp, tp)

    if not last:
        half = (n_group - OWN) // 2
        n_iter = OWN + half
        width = ring.shape[1]
        inner = wg_ref.shape[1]
        weights = [(wg_ref, 0, width), (wu_ref, width, width), (wd_ref, 2 * width, inner)]
        w_copies = [
            pltpu.make_async_copy(ref, ring.at[pl.ds(base, rows)], sem_w.at[k])
            for k, (ref, base, rows) in enumerate(weights)
        ]

        def w_start(k):
            ref, base, rows = weights[k]
            piece = rows // 9
            for p in range(0, rows, piece):
                pltpu.make_async_copy(ref.at[pl.ds(p, piece)], ring.at[pl.ds(base + p, piece)], sem_w.at[k]).start()

        def group_of(i):
            moved = jnp.where(i < HEAD + half, dp * half, half)
            return i + jnp.where(i < HEAD, 0, moved)

        def e_copy(i, j):
            group = group_of(i)
            slot = lax.rem(i + WEIGHT_GROUPS, RING_GROUPS)
            return pltpu.make_async_copy(
                emb_ref.at[pl.ds(group * GROUP + j * SUB, SUB)],
                ring.at[pl.ds(slot * GROUP + j * SUB, SUB)],
                sem_e.at[slot, j],
            )

        def e_start(i):
            for j in range(NSUB):
                e_copy(i, j).start()

        def no_copy(i):
            group = group_of(i)
            return pltpu.make_async_copy(
                noise_ref.at[step, :, pl.ds(group * GROUP, GROUP)], nz_own.at[i], sem_no.at[i]
            )

        def nr_copy(j):
            group = HEAD + (1 - dp) * half + j
            return pltpu.make_async_remote_copy(
                src_ref=noise_ref.at[step, :, pl.ds(group * GROUP, GROUP)],
                dst_ref=nz_oth.at[j],
                send_sem=sem_ns.at[j],
                recv_sem=sem_nr.at[j],
                device_id=pair,
                device_id_type=MESH,
            )

        w_start(0)
        w_start(1)

    barrier = pltpu.get_barrier_semaphore()
    peers = (sib, over) if last else (sib, over, diag, pair)
    for peer in peers:
        pl.semaphore_signal(barrier, inc=1, device_id=peer, device_id_type=MESH)
    pl.semaphore_wait(barrier, len(peers))

    def fetch_head():
        e_start(0)
        e_start(1)
        pl.loop(0, n_iter)(lambda i: no_copy(i).start())

    if not last:
        early = 6
        pl.loop(0, early)(lambda j: nr_copy(j).start())

    if first:
        hid = hid_ref[...].astype(jnp.float32)
        w_start(2)
        w_copies[0].wait()
        fetch_head()
    else:
        a_rows = remote(rows_ref.at[1 - core], rows_a, sem_rows.at[0], sib)
        a_meta = remote(meta_ref.at[1 - core], meta_a, sem_meta.at[0], sib)
        a_rows.start()
        a_meta.start()
        a_rows.wait()
        a_meta.wait()
        if not last:
            w_start(2)
        mine = meta_ref[core]
        seen = meta_a[...]
        keep = mine[0] >= seen[0]
        meta_m[...] = jnp.where(keep[None], mine, seen)
        rows_m[...] = jnp.where(
            keep[:, :1], rows_ref[core].astype(jnp.float32), rows_a[...].astype(jnp.float32)
        ).astype(jnp.bfloat16)
        b_rows = remote(rows_m, rows_b, sem_rows.at[1], over)
        b_meta = remote(meta_m, meta_b, sem_meta.at[1], over)
        b_rows.start()
        b_meta.start()
        b_rows.wait()
        b_meta.wait()
        mine = meta_m[...]
        seen = meta_b[...]
        keep = mine[0] >= seen[0]
        meta_f[...] = jnp.where(keep[None], mine, seen)
        rows_f[...] = jnp.where(
            keep[:, :1], rows_m[...].astype(jnp.float32), rows_b[...].astype(jnp.float32)
        ).astype(jnp.bfloat16)
        c_rows = remote(rows_f, rows_c, sem_rows.at[2], sib)
        c_meta = remote(meta_f, meta_c, sem_meta.at[2], sib)
        c_rows.start()
        c_meta.start()
        c_rows.wait()
        c_meta.wait()
        if not last:
            w_copies[0].wait()
            fetch_head()
        low = core == 0
        r_f, r_c = rows_f[...].astype(jnp.float32), rows_c[...].astype(jnp.float32)
        t_f, t_c = meta_f[1], meta_c[1]
        picked = jnp.concatenate([jnp.where(low, r_f, r_c), jnp.where(low, r_c, r_f)], axis=0)
        token = jnp.concatenate([jnp.where(low, t_f, t_c), jnp.where(low, t_c, t_f)], axis=0).astype(jnp.int32)
        if last:
            for k, line in enumerate([ref[...] for ref in old_refs] + [as_line(token)]):
                tok_ref[k : k + 1] = line[:, : token.shape[0]]
        else:
            tok_ref[...] = as_line(token)
        hid_bf = (picked * embed_scale).astype(jnp.bfloat16)
        hout_ref[...] = hid_bf
        hid = hid_bf.astype(jnp.float32)

    if last:
        return

    batch = hid.shape[0]
    quarter = batch // 4
    hid32[...] = hid.reshape(4, quarter, width)
    normed = rms_scale(hid, gain(pre_ref)).astype(jnp.bfloat16)
    f_two[pl.ds(0, batch)] = normed
    w_copies[1].wait()
    col = 768

    @pl.loop(0, inner // col)
    def _(n):
        cols = pl.ds(pl.multiple_of(n * col, col), col)
        lhs = f_two[pl.ds(0, batch)]
        gate = jnp.dot(lhs, ring[pl.ds(0, width), cols], preferred_element_type=jnp.float32)
        up = jnp.dot(lhs, ring[pl.ds(width, width), cols], preferred_element_type=jnp.float32)
        gate_s[:, cols] = (jax.nn.gelu(gate, approximate=True) * up).astype(jnp.bfloat16)

    for i in range(2, 2 + (2 * width) // GROUP):
        e_start(i)
    w_copies[2].wait()

    @pl.loop(0, width // col)
    def _(n):
        cols = pl.ds(pl.multiple_of(n * col, col), col)
        part_s[:, :, cols] = jnp.dot(
            gate_s[...], ring[pl.ds(2 * width, inner), cols], preferred_element_type=jnp.float32
        ).reshape(4, quarter, col)

    for i in range(2 + (2 * width) // GROUP, RING_GROUPS):
        e_start(i)

    ra = remote(part_s.at[pl.ds(2 * (1 - core), 2)], part_a, sem_ra, sib)
    ra.start()
    ra.wait()
    half_s[...] = part_s[pl.ds(2 * core, 2)] + part_a[...]
    rb = remote(half_s.at[1 - chip], part_b, sem_rb, over)
    rb.start()
    rb.wait()
    down_sum = half_s[chip] + part_b[...]
    place = 2 * core + chip
    post_out = rms_scale(down_sum, gain(post_ref)).astype(jnp.bfloat16)
    resid = (hid32[place] + post_out.astype(jnp.float32)).astype(jnp.bfloat16)
    final_in = rms_scale(resid.astype(jnp.float32), gain(fin_ref)).astype(jnp.bfloat16)
    f_send[...] = final_in
    f_copies = [remote(f_send, f_all.at[k], sem_f.at[k], peer) for k, peer in enumerate((sib, over, diag))]
    f_pair_copy = remote(f_send, f_pair, sem_fo, pair)
    for copy in [*f_copies, f_pair_copy]:
        copy.start()
    pl.loop(early, half)(lambda j: nr_copy(j).start())
    for copy in f_copies:
        copy.wait()
    low_core, low_chip = core == 0, chip == 0

    def in_order(mine_ref, others_ref):
        me_f, sib_f, over_f, diag_f = (v.astype(jnp.float32) for v in (mine_ref[...], *(others_ref[k] for k in range(3))))
        core0 = [jnp.where(low_core, a, b) for a, b in ((me_f, sib_f), (over_f, diag_f))]
        core1 = [jnp.where(low_core, b, a) for a, b in ((me_f, sib_f), (over_f, diag_f))]
        order = [
            jnp.where(low_chip, core0[0], core0[1]),
            jnp.where(low_chip, core0[1], core0[0]),
            jnp.where(low_chip, core1[0], core1[1]),
            jnp.where(low_chip, core1[1], core1[0]),
        ]
        return jnp.concatenate(order, axis=0).astype(jnp.bfloat16)

    f_two[pl.ds(0, batch)] = in_order(f_send, f_all)
    f_pair_copy.wait()
    g_copies = [remote(f_pair, g_all.at[k], sem_g.at[k], peer) for k, peer in enumerate((sib, over, diag))]
    for copy in g_copies:
        copy.start()

    bv[...] = jnp.full_like(bv, NEG)
    bi[...] = jnp.zeros_like(bi)
    heat = jnp.full((1, 128), temp_ref[0, 0], jnp.float32)
    fold = jnp.where(heat > 2.0**64, 2.0**-64, 1.0)
    c1 = (SOFT_CAP * fold)[:, :1]
    c2 = (1.0 / (heat * fold))[:, :1]

    def score(i, rows, nz_refs):
        slot = lax.rem(i + WEIGHT_GROUPS, RING_GROUPS)
        group = group_of(i)
        for j in range(NSUB):
            e_copy(i, j).wait()
        lhs = f_two[pl.ds(0, rows)]
        for start, size, turn in CUTS:
            block = ring[pl.ds(pl.multiple_of(slot * GROUP + start, 256), size), :]
            if turn:
                for k in range(0, width, 256):
                    turned[pl.ds(k, 256)] = block[:, k : k + 256].T
                z = jnp.dot(lhs, turned[...], preferred_element_type=jnp.float32)
            else:
                z = lax.dot_general(lhs, block, (((1,), (1,)), ((), ())), preferred_element_type=jnp.float32)
            s = jnp.tanh(z * (1.0 / SOFT_CAP)) * c1 * c2
            for part, nz in enumerate(nz_refs):
                take_rows = pl.ds(part * batch, batch)
                for q in range(size // 256):
                    v = s[part * batch : (part + 1) * batch, q * 256 : (q + 1) * 256]
                    v = v + nz[:, start + q * 256 : start + (q + 1) * 256]
                    old = bv[take_rows]
                    better = v > old
                    bv[take_rows] = jnp.where(better, v, old)
                    bi[take_rows] = jnp.where(better, group * (GROUP // 256) + (start // 256 + q), bi[take_rows])

        @pl.when(i + RING_GROUPS < n_iter)
        def _():
            e_start(i + RING_GROUPS)

    def own(i):
        no_copy(i).wait()
        score(i, batch, [nz_own.at[i]])

    def shared(i):
        no_copy(i).wait()
        nr_copy(i - HEAD).wait_recv()
        score(i, 2 * batch, [nz_own.at[i], nz_oth.at[i - HEAD]])

    def settle(part):
        val = bv[pl.ds(part * batch, batch)]
        tile = bi[pl.ds(part * batch, batch)]
        top = jnp.max(val, axis=1, keepdims=True)
        ids = (tile * 256 + lax.broadcasted_iota(jnp.int32, tile.shape, 1)).astype(jnp.float32)
        row = jnp.min(jnp.where(val == top, ids, 3.0e7), axis=1, keepdims=True)
        return jnp.broadcast_to(top, (batch, 128)), jnp.broadcast_to(row, (batch, 128))

    by = remote(best_oth, best_in, sem_by, pair)

    @pl.loop(0, 2)
    def _(phase):
        pl.loop(jnp.where(phase == 0, 0, HEAD + half), jnp.where(phase == 0, HEAD, n_iter))(own)

        @pl.when(phase == 0)
        def _():
            for copy in g_copies:
                copy.wait()
            f_two[pl.ds(batch, batch)] = in_order(f_pair, g_all)
            pl.loop(HEAD, HEAD + half)(shared)
            o_val, o_row = settle(1)
            best_oth[0] = o_val
            best_oth[1] = o_row
            by.start()

    pl.loop(0, half)(lambda j: nr_copy(j).wait_send())
    m_val, m_row = settle(0)
    by.wait()
    keep = m_val >= best_in[0]
    top = jnp.where(keep, m_val, best_in[0])
    row = jnp.where(keep, m_row, best_in[1])
    offset = (tp * (n_group * GROUP)).astype(jnp.float32)
    hb = batch // 2
    for part in range(2):
        best_ref[part, 0] = top[part * hb : (part + 1) * hb]
        best_ref[part, 1] = row[part * hb : (part + 1) * hb] + offset
    line_ref[...] = as_line(row.astype(jnp.int32))


def lookup_kernel(line_ref, emb_ref, out_ref, tiles, sem):
    half, batch = out_ref.shape[1], 2 * out_ref.shape[1]
    for r in range(batch):
        base = pl.multiple_of(lax.div(line_ref[0, r], 8) * 8, 8)
        pltpu.make_async_copy(emb_ref.at[pl.ds(base, 8)], tiles.at[pl.ds(8 * r, 8)], sem).start()
    shape = (batch, 8 * batch)
    place = lax.broadcasted_iota(jnp.int32, (batch, 1), 0)
    want = 8 * place
    for r in range(batch):
        want = want + jnp.where(place == r, lax.rem(line_ref[0, r], 8), 0)
    pick = (lax.broadcasted_iota(jnp.int32, shape, 1) == want).astype(jnp.bfloat16)
    pltpu.make_async_copy(emb_ref.at[pl.ds(0, 8 * batch)], tiles, sem).wait()
    rows = jnp.dot(pick, tiles[...], preferred_element_type=jnp.float32).astype(jnp.bfloat16)
    out_ref[0] = rows[:half]
    out_ref[1] = rows[half:]


def lookup(line, batch, embedding):
    width = embedding.shape[1]
    return pl.pallas_call(
        lookup_kernel,
        out_shape=jax.ShapeDtypeStruct((2, batch // 2, width), jnp.bfloat16),
        in_specs=[pl.BlockSpec(memory_space=pltpu.SMEM), pl.BlockSpec(memory_space=pl.ANY)],
        out_specs=pl.BlockSpec(memory_space=pltpu.VMEM),
        scratch_shapes=[pltpu.VMEM((8 * batch, width), jnp.bfloat16), pltpu.SemaphoreType.DMA(())],
        compiler_params=pltpu.CompilerParams(vmem_limit_bytes=66_000_000),
        name="lookup",
    )(line, embedding)


def call_step(step, steps, batch, width, inner, vocab_local, embed_scale, operands):
    first, last = step == 0, step == steps
    f32, bf16, i32 = jnp.float32, jnp.bfloat16, jnp.int32
    vmem, hbm = pl.BlockSpec(memory_space=pltpu.VMEM), pl.BlockSpec(memory_space=pl.ANY)
    dma = pltpu.SemaphoreType.DMA
    n_group = vocab_local // GROUP
    half = (n_group - OWN) // 2
    n_iter = OWN + half
    hb, quarter = batch // 2, batch // 4
    in_specs = [vmem] * (1 if first else 2 + (step - 1) * last)
    if not last:
        in_specs += [vmem] * 3 + [pl.BlockSpec(memory_space=pltpu.SMEM)] + [hbm] * 5
    outs, scratch = [], []
    if not first:
        outs += [jax.ShapeDtypeStruct((steps, batch) if last else (1, 128), i32), jax.ShapeDtypeStruct((batch, width), bf16)]
        rows, meta = pltpu.VMEM((hb, width), bf16), pltpu.VMEM((2, hb, 128), f32)
        scratch += [rows, meta] * 5 + [dma((3, 2)), dma((3, 2))]
    if not last:
        outs += [
            jax.ShapeDtypeStruct((2, 2, hb, 128), f32),
            jax.ShapeDtypeStruct((1, 128), i32),
        ]
        scratch += [
            pltpu.VMEM((RING_GROUPS * GROUP, width), bf16),
            pltpu.VMEM((n_iter, batch, GROUP), f32),
            pltpu.VMEM((half, batch, GROUP), f32),
            pltpu.VMEM((4, quarter, width), f32),
            pltpu.VMEM((2, quarter, width), f32),
            pltpu.VMEM((2, quarter, width), f32),
            pltpu.VMEM((quarter, width), f32),
            pltpu.VMEM((quarter, width), bf16),
            pltpu.VMEM((3, quarter, width), bf16),
            pltpu.VMEM((quarter, width), bf16),
            pltpu.VMEM((3, quarter, width), bf16),
            pltpu.VMEM((2 * batch, width), bf16),
            pltpu.VMEM((4, quarter, width), f32),
            pltpu.VMEM((batch, inner), bf16),
            pltpu.VMEM((width, max(c[1] for c in CUTS if c[2])), bf16),
            pltpu.VMEM((2 * batch, 256), f32),
            pltpu.VMEM((2 * batch, 256), i32),
            pltpu.VMEM((2, batch, 128), f32),
            pltpu.VMEM((2, batch, 128), f32),
            dma((3,)),
            dma((RING_GROUPS, NSUB)),
            dma((n_iter,)),
            dma((half,)),
            dma((half,)),
            dma((2,)),
            dma((2,)),
            dma((3, 2)),
            dma((2,)),
            dma((3, 2)),
            dma((2,)),
        ]
    return pl.pallas_call(
        functools.partial(step_kernel, (step, first, last, n_group, embed_scale)),
        out_shape=outs,
        in_specs=in_specs,
        out_specs=[vmem] * len(outs),
        scratch_shapes=scratch,
        compiler_params=pltpu.CompilerParams(
            collective_id=step, has_side_effects=True, vmem_limit_bytes=66_000_000
        ),
        name=f"step{step}",
    )(*operands)


def solution(mesh):
    def local_steps(start_hidden, embedding, pre_norm, w_gate, w_up, w_down, post_norm, final_norm, temperature, step_noise):
        vocab_local, width = embedding.shape
        batch, steps = start_hidden.shape[0], step_noise.shape[0]
        inner = w_gate.shape[1]
        embed_scale = float(np.float64(math.sqrt(width)).astype(jnp.bfloat16))
        common = [pre_norm, post_norm, final_norm, temperature.reshape(1, 1), w_gate, w_up, w_down, embedding, step_noise]
        sizes = (steps, batch, width, inner, vocab_local, embed_scale)
        best, line = call_step(0, *sizes, [start_hidden, *common])
        lines = []
        for step in range(1, steps):
            outs = call_step(step, *sizes, [lookup(line, batch, embedding), best, *common])
            lines.append(outs[0])
            best, line = outs[2:]
        tokens, hidden = call_step(steps, *sizes, [lookup(line, batch, embedding), best, *lines])
        return tokens, hidden

    return jax.shard_map(
        local_steps,
        mesh=mesh,
        in_specs=(P("dp", None), P("tp", None), P(), P(None, "tp"), P(None, "tp"), P("tp", None), P(), P(), P(), P(None, "dp", "tp")),
        out_specs=(P(None, "dp"), P("dp", None)),
        check_vma=False,
    )
```

```python
import functools
import math

import jax
import jax.numpy as jnp
import numpy as np
from jax import lax
from jax.experimental import pallas as pl
from jax.experimental.pallas import tpu as pltpu
from jax.sharding import PartitionSpec as P

SOFT_CAP = 30.0
EPSILON = 1e-6
MESH = pl.DeviceIdType.MESH

SUB = 640
NSUB = 2
GROUP = SUB * NSUB
RING_GROUPS = 8
WEIGHT_GROUPS = 6
CUTS = ((0, 512, False), (512, 768, True))
HEAD = 10
TAIL = 2
OWN = HEAD + TAIL
NEG = -3.0e38


def gain(ref):
    return ref[...].astype(jnp.float32).reshape(1, ref.shape[0])


def rms_scale(x_f32, gain_row):
    mean_sq = jnp.mean(x_f32 * x_f32, axis=-1, keepdims=True)
    return x_f32 * lax.rsqrt(mean_sq + EPSILON) * (1.0 + gain_row)


def remote(src, dst, sem, peer):
    return pltpu.make_async_remote_copy(
        src_ref=src, dst_ref=dst, send_sem=sem.at[0], recv_sem=sem.at[1], device_id=peer, device_id_type=MESH
    )


def as_line(wide):
    eye = lax.broadcasted_iota(jnp.int32, wide.shape, 0) == lax.broadcasted_iota(jnp.int32, wide.shape, 1)
    return jnp.sum(jnp.where(eye, wide, 0), axis=0, keepdims=True)


def step_kernel(cfg, *refs):
    step, first, last, n_group, embed_scale = cfg
    refs = list(refs)
    take = lambda n: [refs.pop(0) for _ in range(n)]
    if first:
        (hid_hbm,) = take(1)
    else:
        rows_hbm, meta_hbm = take(2)
        if last:
            old_refs = take(step - 1)
    if not last:
        pre_hbm, post_hbm, fin_hbm, temp_ref, wg_ref, wu_ref, wd_ref, emb_ref, noise_ref = take(9)
    if not first:
        tok_ref, hout_ref = take(2)
    if not last:
        best_ref, line_ref = take(2)
    if first:
        hid_ref, sem_in = take(2)
        inputs = [(hid_hbm, hid_ref)]
    else:
        rows_ref, meta_ref, sem_in = take(3)
        inputs = [(rows_hbm, rows_ref), (meta_hbm, meta_ref)]
    if not last:
        pre_ref, post_ref, fin_ref, sem_gain = take(4)
        gains = [(pre_hbm, pre_ref), (post_hbm, post_ref), (fin_hbm, fin_ref)]
    in_copies = [pltpu.make_async_copy(src, dst, sem_in.at[k]) for k, (src, dst) in enumerate(inputs)]
    for copy in in_copies:
        copy.start()
    if not first:
        rows_a, meta_a, rows_m, meta_m, rows_b, meta_b, rows_f, meta_f, rows_c, meta_c, sem_rows, sem_meta = take(12)
    if not last:
        (ring, nz_own, nz_oth, part_s, part_a, half_s, part_b, f_send, f_all, f_pair, g_all, f_two,
         hid32, gate_s, turned, bv, bi, best_oth, best_in,
         sem_w, sem_e, sem_no, sem_ns, sem_nr, sem_ra, sem_rb, sem_f, sem_fo, sem_g, sem_by) = take(30)

    dp, tp = lax.axis_index("dp"), lax.axis_index("tp")
    core, chip = lax.rem(tp, 2), lax.div(tp, 2)
    tp_sib = chip * 2 + (1 - core)
    tp_x = (1 - chip) * 2 + core
    tp_diag = (1 - chip) * 2 + (1 - core)
    sib, over, diag, pair = (dp, tp_sib), (dp, tp_x), (dp, tp_diag), (1 - dp, tp)

    if not last:
        half = (n_group - OWN) // 2
        n_iter = OWN + half
        width = ring.shape[1]
        inner = wg_ref.shape[1]
        weights = [(wg_ref, 0, width), (wu_ref, width, width), (wd_ref, 2 * width, inner)]
        w_copies = [
            pltpu.make_async_copy(ref, ring.at[pl.ds(base, rows)], sem_w.at[k])
            for k, (ref, base, rows) in enumerate(weights)
        ]

        def w_start(k):
            ref, base, rows = weights[k]
            piece = rows // 9
            for p in range(0, rows, piece):
                pltpu.make_async_copy(ref.at[pl.ds(p, piece)], ring.at[pl.ds(base + p, piece)], sem_w.at[k]).start()

        def group_of(i):
            moved = jnp.where(i < HEAD + half, dp * half, half)
            return i + jnp.where(i < HEAD, 0, moved)

        def e_copy(i, j):
            group = group_of(i)
            slot = lax.rem(i + WEIGHT_GROUPS, RING_GROUPS)
            return pltpu.make_async_copy(
                emb_ref.at[pl.ds(group * GROUP + j * SUB, SUB)],
                ring.at[pl.ds(slot * GROUP + j * SUB, SUB)],
                sem_e.at[slot, j],
            )

        def e_start(i):
            for j in range(NSUB):
                e_copy(i, j).start()

        def no_copy(i):
            group = group_of(i)
            return pltpu.make_async_copy(
                noise_ref.at[step, :, pl.ds(group * GROUP, GROUP)], nz_own.at[i], sem_no.at[i]
            )

        def nr_copy(j):
            group = HEAD + (1 - dp) * half + j
            return pltpu.make_async_remote_copy(
                src_ref=noise_ref.at[step, :, pl.ds(group * GROUP, GROUP)],
                dst_ref=nz_oth.at[j],
                send_sem=sem_ns.at[j],
                recv_sem=sem_nr.at[j],
                device_id=pair,
                device_id_type=MESH,
            )

        gain_copies = [pltpu.make_async_copy(src, dst, sem_gain.at[k]) for k, (src, dst) in enumerate(gains)]
        for copy in gain_copies:
            copy.start()
        w_start(0)
        w_start(1)

    barrier = pltpu.get_barrier_semaphore()
    peers = (sib, over) if last else (sib, over, diag, pair)
    for peer in peers:
        pl.semaphore_signal(barrier, inc=1, device_id=peer, device_id_type=MESH)
    pl.semaphore_wait(barrier, len(peers))

    def fetch_head():
        e_start(0)
        e_start(1)
        pl.loop(0, n_iter)(lambda i: no_copy(i).start())

    if not last:
        early = 6
        pl.loop(0, early)(lambda j: nr_copy(j).start())

    for copy in in_copies:
        copy.wait()
    if first:
        hid = hid_ref[...].astype(jnp.float32)
        w_start(2)
        w_copies[0].wait()
        fetch_head()
    else:
        a_rows = remote(rows_ref.at[1 - core], rows_a, sem_rows.at[0], sib)
        a_meta = remote(meta_ref.at[1 - core], meta_a, sem_meta.at[0], sib)
        a_rows.start()
        a_meta.start()
        a_rows.wait()
        a_meta.wait()
        if not last:
            w_start(2)
        mine = meta_ref[core]
        seen = meta_a[...]
        keep = mine[0] >= seen[0]
        meta_m[...] = jnp.where(keep[None], mine, seen)
        rows_m[...] = jnp.where(
            keep[:, :1], rows_ref[core].astype(jnp.float32), rows_a[...].astype(jnp.float32)
        ).astype(jnp.bfloat16)
        b_rows = remote(rows_m, rows_b, sem_rows.at[1], over)
        b_meta = remote(meta_m, meta_b, sem_meta.at[1], over)
        b_rows.start()
        b_meta.start()
        b_rows.wait()
        b_meta.wait()
        mine = meta_m[...]
        seen = meta_b[...]
        keep = mine[0] >= seen[0]
        meta_f[...] = jnp.where(keep[None], mine, seen)
        rows_f[...] = jnp.where(
            keep[:, :1], rows_m[...].astype(jnp.float32), rows_b[...].astype(jnp.float32)
        ).astype(jnp.bfloat16)
        c_rows = remote(rows_f, rows_c, sem_rows.at[2], sib)
        c_meta = remote(meta_f, meta_c, sem_meta.at[2], sib)
        c_rows.start()
        c_meta.start()
        c_rows.wait()
        c_meta.wait()
        if not last:
            w_copies[0].wait()
            fetch_head()
        low = core == 0
        r_f, r_c = rows_f[...].astype(jnp.float32), rows_c[...].astype(jnp.float32)
        t_f, t_c = meta_f[1], meta_c[1]
        picked = jnp.concatenate([jnp.where(low, r_f, r_c), jnp.where(low, r_c, r_f)], axis=0)
        token = jnp.concatenate([jnp.where(low, t_f, t_c), jnp.where(low, t_c, t_f)], axis=0).astype(jnp.int32)
        if last:
            for k, line in enumerate([ref[...] for ref in old_refs] + [as_line(token)]):
                tok_ref[k : k + 1] = line[:, : token.shape[0]]
        else:
            tok_ref[...] = as_line(token)
        hid_bf = (picked * embed_scale).astype(jnp.bfloat16)
        hout_ref[...] = hid_bf
        hid = hid_bf.astype(jnp.float32)

    if last:
        return

    batch = hid.shape[0]
    quarter = batch // 4
    hid32[...] = hid.reshape(4, quarter, width)
    for copy in gain_copies:
        copy.wait()
    normed = rms_scale(hid, gain(pre_ref)).astype(jnp.bfloat16)
    f_two[pl.ds(0, batch)] = normed
    w_copies[1].wait()
    col = 768

    @pl.loop(0, inner // col)
    def _(n):
        cols = pl.ds(pl.multiple_of(n * col, col), col)
        lhs = f_two[pl.ds(0, batch)]
        gate = jnp.dot(lhs, ring[pl.ds(0, width), cols], preferred_element_type=jnp.float32)
        up = jnp.dot(lhs, ring[pl.ds(width, width), cols], preferred_element_type=jnp.float32)
        gate_s[:, cols] = (jax.nn.gelu(gate, approximate=True) * up).astype(jnp.bfloat16)

    for i in range(2, 2 + (2 * width) // GROUP):
        e_start(i)
    w_copies[2].wait()

    @pl.loop(0, width // col)
    def _(n):
        cols = pl.ds(pl.multiple_of(n * col, col), col)
        part_s[:, :, cols] = jnp.dot(
            gate_s[...], ring[pl.ds(2 * width, inner), cols], preferred_element_type=jnp.float32
        ).reshape(4, quarter, col)

    for i in range(2 + (2 * width) // GROUP, RING_GROUPS):
        e_start(i)

    ra = remote(part_s.at[pl.ds(2 * (1 - core), 2)], part_a, sem_ra, sib)
    ra.start()
    ra.wait()
    half_s[...] = part_s[pl.ds(2 * core, 2)] + part_a[...]
    rb = remote(half_s.at[1 - chip], part_b, sem_rb, over)
    rb.start()
    rb.wait()
    down_sum = half_s[chip] + part_b[...]
    place = 2 * core + chip
    post_out = rms_scale(down_sum, gain(post_ref)).astype(jnp.bfloat16)
    resid = (hid32[place] + post_out.astype(jnp.float32)).astype(jnp.bfloat16)
    final_in = rms_scale(resid.astype(jnp.float32), gain(fin_ref)).astype(jnp.bfloat16)
    f_send[...] = final_in
    f_copies = [remote(f_send, f_all.at[k], sem_f.at[k], peer) for k, peer in enumerate((sib, over, diag))]
    f_pair_copy = remote(f_send, f_pair, sem_fo, pair)
    for copy in [*f_copies, f_pair_copy]:
        copy.start()
    pl.loop(early, half)(lambda j: nr_copy(j).start())
    for copy in f_copies:
        copy.wait()
    low_core, low_chip = core == 0, chip == 0

    def in_order(mine_ref, others_ref):
        me_f, sib_f, over_f, diag_f = (v.astype(jnp.float32) for v in (mine_ref[...], *(others_ref[k] for k in range(3))))
        core0 = [jnp.where(low_core, a, b) for a, b in ((me_f, sib_f), (over_f, diag_f))]
        core1 = [jnp.where(low_core, b, a) for a, b in ((me_f, sib_f), (over_f, diag_f))]
        order = [
            jnp.where(low_chip, core0[0], core0[1]),
            jnp.where(low_chip, core0[1], core0[0]),
            jnp.where(low_chip, core1[0], core1[1]),
            jnp.where(low_chip, core1[1], core1[0]),
        ]
        return jnp.concatenate(order, axis=0).astype(jnp.bfloat16)

    f_two[pl.ds(0, batch)] = in_order(f_send, f_all)
    f_pair_copy.wait()
    g_copies = [remote(f_pair, g_all.at[k], sem_g.at[k], peer) for k, peer in enumerate((sib, over, diag))]
    for copy in g_copies:
        copy.start()

    bv[...] = jnp.full_like(bv, NEG)
    bi[...] = jnp.zeros_like(bi)
    heat = jnp.full((1, 128), temp_ref[0, 0], jnp.float32)
    fold = jnp.where(heat > 2.0**64, 2.0**-64, 1.0)
    c1 = (SOFT_CAP * fold)[:, :1]
    c2 = (1.0 / (heat * fold))[:, :1]

    def score(i, rows, nz_refs):
        slot = lax.rem(i + WEIGHT_GROUPS, RING_GROUPS)
        group = group_of(i)
        for j in range(NSUB):
            e_copy(i, j).wait()
        lhs = f_two[pl.ds(0, rows)]
        for start, size, turn in CUTS:
            block = ring[pl.ds(pl.multiple_of(slot * GROUP + start, 256), size), :]
            if turn:
                for k in range(0, width, 256):
                    turned[pl.ds(k, 256)] = block[:, k : k + 256].T
                z = jnp.dot(lhs, turned[...], preferred_element_type=jnp.float32)
            else:
                z = lax.dot_general(lhs, block, (((1,), (1,)), ((), ())), preferred_element_type=jnp.float32)
            s = jnp.tanh(z * (1.0 / SOFT_CAP)) * c1 * c2
            for part, nz in enumerate(nz_refs):
                take_rows = pl.ds(part * batch, batch)
                for q in range(size // 256):
                    v = s[part * batch : (part + 1) * batch, q * 256 : (q + 1) * 256]
                    v = v + nz[:, start + q * 256 : start + (q + 1) * 256]
                    old = bv[take_rows]
                    better = v > old
                    bv[take_rows] = jnp.where(better, v, old)
                    bi[take_rows] = jnp.where(better, group * (GROUP // 256) + (start // 256 + q), bi[take_rows])

        @pl.when(i + RING_GROUPS < n_iter)
        def _():
            e_start(i + RING_GROUPS)

    def own(i):
        no_copy(i).wait()
        score(i, batch, [nz_own.at[i]])

    def shared(i):
        no_copy(i).wait()
        nr_copy(i - HEAD).wait_recv()
        score(i, 2 * batch, [nz_own.at[i], nz_oth.at[i - HEAD]])

    def settle(part):
        val = bv[pl.ds(part * batch, batch)]
        tile = bi[pl.ds(part * batch, batch)]
        top = jnp.max(val, axis=1, keepdims=True)
        ids = (tile * 256 + lax.broadcasted_iota(jnp.int32, tile.shape, 1)).astype(jnp.float32)
        row = jnp.min(jnp.where(val == top, ids, 3.0e7), axis=1, keepdims=True)
        return jnp.broadcast_to(top, (batch, 128)), jnp.broadcast_to(row, (batch, 128))

    by = remote(best_oth, best_in, sem_by, pair)

    @pl.loop(0, 2)
    def _(phase):
        pl.loop(jnp.where(phase == 0, 0, HEAD + half), jnp.where(phase == 0, HEAD, n_iter))(own)

        @pl.when(phase == 0)
        def _():
            for copy in g_copies:
                copy.wait()
            f_two[pl.ds(batch, batch)] = in_order(f_pair, g_all)
            pl.loop(HEAD, HEAD + half)(shared)
            o_val, o_row = settle(1)
            best_oth[0] = o_val
            best_oth[1] = o_row
            by.start()

    pl.loop(0, half)(lambda j: nr_copy(j).wait_send())
    m_val, m_row = settle(0)
    by.wait()
    keep = m_val >= best_in[0]
    top = jnp.where(keep, m_val, best_in[0])
    row = jnp.where(keep, m_row, best_in[1])
    offset = (tp * (n_group * GROUP)).astype(jnp.float32)
    hb = batch // 2
    for part in range(2):
        best_ref[part, 0] = top[part * hb : (part + 1) * hb]
        best_ref[part, 1] = row[part * hb : (part + 1) * hb] + offset
    line_ref[...] = as_line(row.astype(jnp.int32))


def lookup_kernel(line_ref, emb_ref, out_ref, tiles, sem):
    half, batch = out_ref.shape[1], 2 * out_ref.shape[1]
    for r in range(batch):
        base = pl.multiple_of(lax.div(line_ref[0, r], 8) * 8, 8)
        pltpu.make_async_copy(emb_ref.at[pl.ds(base, 8)], tiles.at[pl.ds(8 * r, 8)], sem).start()
    shape = (batch, 8 * batch)
    place = lax.broadcasted_iota(jnp.int32, (batch, 1), 0)
    want = 8 * place
    for r in range(batch):
        want = want + jnp.where(place == r, lax.rem(line_ref[0, r], 8), 0)
    pick = (lax.broadcasted_iota(jnp.int32, shape, 1) == want).astype(jnp.bfloat16)
    pltpu.make_async_copy(emb_ref.at[pl.ds(0, 8 * batch)], tiles, sem).wait()
    rows = jnp.dot(pick, tiles[...], preferred_element_type=jnp.float32).astype(jnp.bfloat16)
    out_ref[0] = rows[:half]
    out_ref[1] = rows[half:]


def lookup(line, batch, embedding):
    width = embedding.shape[1]
    return pl.pallas_call(
        lookup_kernel,
        out_shape=jax.ShapeDtypeStruct((2, batch // 2, width), jnp.bfloat16),
        in_specs=[pl.BlockSpec(memory_space=pltpu.SMEM), pl.BlockSpec(memory_space=pl.ANY)],
        out_specs=pl.BlockSpec(memory_space=pltpu.VMEM),
        scratch_shapes=[pltpu.VMEM((8 * batch, width), jnp.bfloat16), pltpu.SemaphoreType.DMA(())],
        compiler_params=pltpu.CompilerParams(vmem_limit_bytes=66_000_000),
        name="lookup",
    )(line, embedding)


def call_step(step, steps, batch, width, inner, vocab_local, embed_scale, operands):
    first, last = step == 0, step == steps
    f32, bf16, i32 = jnp.float32, jnp.bfloat16, jnp.int32
    vmem, hbm = pl.BlockSpec(memory_space=pltpu.VMEM), pl.BlockSpec(memory_space=pl.ANY)
    dma = pltpu.SemaphoreType.DMA
    n_group = vocab_local // GROUP
    half = (n_group - OWN) // 2
    n_iter = OWN + half
    hb, quarter = batch // 2, batch // 4
    in_specs = [hbm] * (1 if first else 2) + [vmem] * ((step - 1) * last)
    if not last:
        in_specs += [hbm] * 3 + [pl.BlockSpec(memory_space=pltpu.SMEM)] + [hbm] * 5
    outs, scratch = [], []
    if first:
        scratch += [pltpu.VMEM((batch, width), bf16), dma((1,))]
    else:
        scratch += [pltpu.VMEM((2, hb, width), bf16), pltpu.VMEM((2, 2, hb, 128), f32), dma((2,))]
    if not last:
        scratch += [pltpu.VMEM((width,), bf16)] * 3 + [dma((3,))]
    if not first:
        outs += [jax.ShapeDtypeStruct((steps, batch) if last else (1, 128), i32), jax.ShapeDtypeStruct((batch, width), bf16)]
        rows, meta = pltpu.VMEM((hb, width), bf16), pltpu.VMEM((2, hb, 128), f32)
        scratch += [rows, meta] * 5 + [dma((3, 2)), dma((3, 2))]
    if not last:
        outs += [
            jax.ShapeDtypeStruct((2, 2, hb, 128), f32),
            jax.ShapeDtypeStruct((1, 128), i32),
        ]
        scratch += [
            pltpu.VMEM((RING_GROUPS * GROUP, width), bf16),
            pltpu.VMEM((n_iter, batch, GROUP), f32),
            pltpu.VMEM((half, batch, GROUP), f32),
            pltpu.VMEM((4, quarter, width), f32),
            pltpu.VMEM((2, quarter, width), f32),
            pltpu.VMEM((2, quarter, width), f32),
            pltpu.VMEM((quarter, width), f32),
            pltpu.VMEM((quarter, width), bf16),
            pltpu.VMEM((3, quarter, width), bf16),
            pltpu.VMEM((quarter, width), bf16),
            pltpu.VMEM((3, quarter, width), bf16),
            pltpu.VMEM((2 * batch, width), bf16),
            pltpu.VMEM((4, quarter, width), f32),
            pltpu.VMEM((batch, inner), bf16),
            pltpu.VMEM((width, max(c[1] for c in CUTS if c[2])), bf16),
            pltpu.VMEM((2 * batch, 256), f32),
            pltpu.VMEM((2 * batch, 256), i32),
            pltpu.VMEM((2, batch, 128), f32),
            pltpu.VMEM((2, batch, 128), f32),
            dma((3,)),
            dma((RING_GROUPS, NSUB)),
            dma((n_iter,)),
            dma((half,)),
            dma((half,)),
            dma((2,)),
            dma((2,)),
            dma((3, 2)),
            dma((2,)),
            dma((3, 2)),
            dma((2,)),
        ]
    return pl.pallas_call(
        functools.partial(step_kernel, (step, first, last, n_group, embed_scale)),
        out_shape=outs,
        in_specs=in_specs,
        out_specs=[vmem] * len(outs),
        scratch_shapes=scratch,
        compiler_params=pltpu.CompilerParams(
            collective_id=step, has_side_effects=True, vmem_limit_bytes=66_000_000
        ),
        name=f"step{step}",
    )(*operands)


def solution(mesh):
    def local_steps(start_hidden, embedding, pre_norm, w_gate, w_up, w_down, post_norm, final_norm, temperature, step_noise):
        vocab_local, width = embedding.shape
        batch, steps = start_hidden.shape[0], step_noise.shape[0]
        inner = w_gate.shape[1]
        embed_scale = float(np.float64(math.sqrt(width)).astype(jnp.bfloat16))
        common = [pre_norm, post_norm, final_norm, temperature.reshape(1, 1), w_gate, w_up, w_down, embedding, step_noise]
        sizes = (steps, batch, width, inner, vocab_local, embed_scale)
        best, line = call_step(0, *sizes, [start_hidden, *common])
        lines = []
        for step in range(1, steps):
            outs = call_step(step, *sizes, [lookup(line, batch, embedding), best, *common])
            lines.append(outs[0])
            best, line = outs[2:]
        tokens, hidden = call_step(steps, *sizes, [lookup(line, batch, embedding), best, *lines])
        return tokens, hidden

    return jax.shard_map(
        local_steps,
        mesh=mesh,
        in_specs=(P("dp", None), P("tp", None), P(), P(None, "tp"), P(None, "tp"), P("tp", None), P(), P(), P(), P(None, "dp", "tp")),
        out_specs=(P(None, "dp"), P("dp", None)),
        check_vma=False,
    )
```

```python
import functools
import math

import jax
import jax.numpy as jnp
import numpy as np
from jax import lax
from jax.experimental import pallas as pl
from jax.experimental.pallas import tpu as pltpu
from jax.sharding import PartitionSpec as P

SOFT_CAP = 30.0
EPSILON = 1e-6
MESH = pl.DeviceIdType.MESH

SUB = 640
NSUB = 2
GROUP = SUB * NSUB
RING_GROUPS = 8
SPREAD = 3
WEIGHT_GROUPS = 6
CUTS = ((0, 512, False), (512, 768, True))
HEAD = 12
TAIL = 2
OWN = HEAD + TAIL
NEG = -3.0e38


def gain(ref):
    return ref[...].astype(jnp.float32).reshape(1, ref.shape[0])


def rms_scale(x_f32, gain_row):
    mean_sq = jnp.mean(x_f32 * x_f32, axis=-1, keepdims=True)
    return x_f32 * lax.rsqrt(mean_sq + EPSILON) * (1.0 + gain_row)


def remote(src, dst, sem, peer):
    return pltpu.make_async_remote_copy(
        src_ref=src, dst_ref=dst, send_sem=sem.at[0], recv_sem=sem.at[1], device_id=peer, device_id_type=MESH
    )


def as_line(wide):
    eye = lax.broadcasted_iota(jnp.int32, wide.shape, 0) == lax.broadcasted_iota(jnp.int32, wide.shape, 1)
    return jnp.sum(jnp.where(eye, wide, 0), axis=0, keepdims=True)


def step_kernel(cfg, *refs):
    step, first, last, n_group, embed_scale = cfg
    refs = list(refs)
    take = lambda n: [refs.pop(0) for _ in range(n)]
    if first:
        (hid_hbm,) = take(1)
    else:
        rows_hbm, meta_hbm = take(2)
        if last:
            old_refs = take(step - 1)
    if not last:
        pre_hbm, post_hbm, fin_hbm, temp_ref, wg_ref, wu_ref, wd_ref, emb_ref, noise_ref = take(9)
    if not first:
        tok_ref, hout_ref = take(2)
    if not last:
        best_ref, line_ref = take(2)
    if first:
        hid_ref, sem_in = take(2)
        inputs = [(hid_hbm, hid_ref)]
    else:
        rows_ref, meta_ref, sem_in = take(3)
        inputs = [(rows_hbm, rows_ref), (meta_hbm, meta_ref)]
    if not last:
        pre_ref, post_ref, fin_ref, sem_gain = take(4)
        gains = [(pre_hbm, pre_ref), (post_hbm, post_ref), (fin_hbm, fin_ref)]
    in_copies = [pltpu.make_async_copy(src, dst, sem_in.at[k]) for k, (src, dst) in enumerate(inputs)]
    for copy in in_copies:
        copy.start()
    if not first:
        rows_a, meta_a, rows_m, meta_m, rows_b, meta_b, rows_f, meta_f, rows_c, meta_c, sem_rows, sem_meta = take(12)
    if not last:
        (ring, nz_own, nz_oth, part_s, part_a, half_s, part_b, f_send, f_all, f_pair, g_all, f_two,
         hid32, gate_s, turned, bv, bi, best_oth, best_in,
         sem_w, sem_e, sem_no, sem_ns, sem_nr, sem_ra, sem_rb, sem_f, sem_fo, sem_g, sem_by) = take(30)

    dp, tp = lax.axis_index("dp"), lax.axis_index("tp")
    core, chip = lax.rem(tp, 2), lax.div(tp, 2)
    tp_sib = chip * 2 + (1 - core)
    tp_x = (1 - chip) * 2 + core
    tp_diag = (1 - chip) * 2 + (1 - core)
    sib, over, diag, pair = (dp, tp_sib), (dp, tp_x), (dp, tp_diag), (1 - dp, tp)

    if not last:
        half = (n_group - OWN) // 2
        n_iter = OWN + half
        width = ring.shape[1]
        inner = wg_ref.shape[1]
        weights = [(wg_ref, 0, width), (wu_ref, width, width), (wd_ref, 2 * width, inner)]
        w_copies = [
            pltpu.make_async_copy(ref, ring.at[pl.ds(base, rows)], sem_w.at[k])
            for k, (ref, base, rows) in enumerate(weights)
        ]

        def w_start(k):
            ref, base, rows = weights[k]
            piece = rows // 9
            for p in range(0, rows, piece):
                pltpu.make_async_copy(ref.at[pl.ds(p, piece)], ring.at[pl.ds(base + p, piece)], sem_w.at[k]).start()

        def group_of(i):
            moved = jnp.where(i < HEAD + half, dp * half, half)
            return i + jnp.where(i < HEAD, 0, moved)

        def e_copy(i, j):
            group = group_of(i)
            slot = lax.rem(i + WEIGHT_GROUPS, RING_GROUPS)
            return pltpu.make_async_copy(
                emb_ref.at[pl.ds(group * GROUP + j * SUB, SUB)],
                ring.at[pl.ds(slot * GROUP + j * SUB, SUB)],
                sem_e.at[slot, j],
            )

        def e_start(i):
            for j in range(NSUB):
                e_copy(i, j).start()

        def no_copy(i):
            group = group_of(i)
            return pltpu.make_async_copy(
                noise_ref.at[step, :, pl.ds(group * GROUP, GROUP)], nz_own.at[i], sem_no.at[i]
            )

        def nr_copy(j):
            group = HEAD + (1 - dp) * half + j
            return pltpu.make_async_remote_copy(
                src_ref=noise_ref.at[step, :, pl.ds(group * GROUP, GROUP)],
                dst_ref=nz_oth.at[j],
                send_sem=sem_ns.at[j],
                recv_sem=sem_nr.at[j],
                device_id=pair,
                device_id_type=MESH,
            )

        gain_copies = [pltpu.make_async_copy(src, dst, sem_gain.at[k]) for k, (src, dst) in enumerate(gains)]
        for copy in gain_copies:
            copy.start()
        w_start(0)
        w_start(1)

    barrier = pltpu.get_barrier_semaphore()
    peers = (sib, over) if last else (sib, over, diag, pair)
    for peer in peers:
        pl.semaphore_signal(barrier, inc=1, device_id=peer, device_id_type=MESH)
    pl.semaphore_wait(barrier, len(peers))

    def fetch_head():
        e_start(0)
        e_start(1)
        pl.loop(0, n_iter)(lambda i: no_copy(i).start())

    if not last:
        early = 6
        pl.loop(0, early)(lambda j: nr_copy(j).start())

    for copy in in_copies:
        copy.wait()
    if first:
        hid = hid_ref[...].astype(jnp.float32)
        w_start(2)
        w_copies[0].wait()
        fetch_head()
    else:
        a_rows = remote(rows_ref.at[1 - core], rows_a, sem_rows.at[0], sib)
        a_meta = remote(meta_ref.at[1 - core], meta_a, sem_meta.at[0], sib)
        a_rows.start()
        a_meta.start()
        a_rows.wait()
        a_meta.wait()
        if not last:
            w_start(2)
        mine = meta_ref[core]
        seen = meta_a[...]
        keep = mine[0] >= seen[0]
        meta_m[...] = jnp.where(keep[None], mine, seen)
        rows_m[...] = jnp.where(
            keep[:, :1], rows_ref[core].astype(jnp.float32), rows_a[...].astype(jnp.float32)
        ).astype(jnp.bfloat16)
        b_rows = remote(rows_m, rows_b, sem_rows.at[1], over)
        b_meta = remote(meta_m, meta_b, sem_meta.at[1], over)
        b_rows.start()
        b_meta.start()
        b_rows.wait()
        b_meta.wait()
        mine = meta_m[...]
        seen = meta_b[...]
        keep = mine[0] >= seen[0]
        meta_f[...] = jnp.where(keep[None], mine, seen)
        rows_f[...] = jnp.where(
            keep[:, :1], rows_m[...].astype(jnp.float32), rows_b[...].astype(jnp.float32)
        ).astype(jnp.bfloat16)
        c_rows = remote(rows_f, rows_c, sem_rows.at[2], sib)
        c_meta = remote(meta_f, meta_c, sem_meta.at[2], sib)
        c_rows.start()
        c_meta.start()
        c_rows.wait()
        c_meta.wait()
        if not last:
            w_copies[0].wait()
            fetch_head()
        low = core == 0
        r_f, r_c = rows_f[...].astype(jnp.float32), rows_c[...].astype(jnp.float32)
        t_f, t_c = meta_f[1], meta_c[1]
        picked = jnp.concatenate([jnp.where(low, r_f, r_c), jnp.where(low, r_c, r_f)], axis=0)
        token = jnp.concatenate([jnp.where(low, t_f, t_c), jnp.where(low, t_c, t_f)], axis=0).astype(jnp.int32)
        if last:
            for k, line in enumerate([ref[...] for ref in old_refs] + [as_line(token)]):
                tok_ref[k : k + 1] = line[:, : token.shape[0]]
        else:
            tok_ref[...] = as_line(token)
        hid_bf = (picked * embed_scale).astype(jnp.bfloat16)
        hout_ref[...] = hid_bf
        hid = hid_bf.astype(jnp.float32)

    if last:
        return

    batch = hid.shape[0]
    quarter = batch // 4
    hid32[...] = hid.reshape(4, quarter, width)
    for copy in gain_copies:
        copy.wait()
    normed = rms_scale(hid, gain(pre_ref)).astype(jnp.bfloat16)
    f_two[pl.ds(0, batch)] = normed
    w_copies[1].wait()
    col = 768

    @pl.loop(0, inner // col)
    def _(n):
        cols = pl.ds(pl.multiple_of(n * col, col), col)
        lhs = f_two[pl.ds(0, batch)]
        gate = jnp.dot(lhs, ring[pl.ds(0, width), cols], preferred_element_type=jnp.float32)
        up = jnp.dot(lhs, ring[pl.ds(width, width), cols], preferred_element_type=jnp.float32)
        gate_s[:, cols] = (jax.nn.gelu(gate, approximate=True) * up).astype(jnp.bfloat16)

    for i in range(2, 2 + (2 * width) // GROUP):
        e_start(i)
    w_copies[2].wait()

    @pl.loop(0, width // col)
    def _(n):
        cols = pl.ds(pl.multiple_of(n * col, col), col)
        part_s[:, :, cols] = jnp.dot(
            gate_s[...], ring[pl.ds(2 * width, inner), cols], preferred_element_type=jnp.float32
        ).reshape(4, quarter, col)

    for i in range(2 + (2 * width) // GROUP, RING_GROUPS):
        e_start(i)

    ra = remote(part_s.at[pl.ds(2 * (1 - core), 2)], part_a, sem_ra, sib)
    ra.start()
    ra.wait()
    half_s[...] = part_s[pl.ds(2 * core, 2)] + part_a[...]
    rb = remote(half_s.at[1 - chip], part_b, sem_rb, over)
    rb.start()
    rb.wait()
    down_sum = half_s[chip] + part_b[...]
    place = 2 * core + chip
    post_out = rms_scale(down_sum, gain(post_ref)).astype(jnp.bfloat16)
    resid = (hid32[place] + post_out.astype(jnp.float32)).astype(jnp.bfloat16)
    final_in = rms_scale(resid.astype(jnp.float32), gain(fin_ref)).astype(jnp.bfloat16)
    f_send[...] = final_in
    f_copies = [remote(f_send, f_all.at[k], sem_f.at[k], peer) for k, peer in enumerate((sib, over, diag))]
    f_pair_copy = remote(f_send, f_pair, sem_fo, pair)
    for copy in [*f_copies, f_pair_copy]:
        copy.start()
    pl.loop(early, half)(lambda j: nr_copy(j).start())
    for copy in f_copies:
        copy.wait()
    low_core, low_chip = core == 0, chip == 0

    def in_order(mine_ref, others_ref):
        me_f, sib_f, over_f, diag_f = (v.astype(jnp.float32) for v in (mine_ref[...], *(others_ref[k] for k in range(3))))
        core0 = [jnp.where(low_core, a, b) for a, b in ((me_f, sib_f), (over_f, diag_f))]
        core1 = [jnp.where(low_core, b, a) for a, b in ((me_f, sib_f), (over_f, diag_f))]
        order = [
            jnp.where(low_chip, core0[0], core0[1]),
            jnp.where(low_chip, core0[1], core0[0]),
            jnp.where(low_chip, core1[0], core1[1]),
            jnp.where(low_chip, core1[1], core1[0]),
        ]
        return jnp.concatenate(order, axis=0).astype(jnp.bfloat16)

    f_two[pl.ds(0, batch)] = in_order(f_send, f_all)
    g_copies = [remote(f_pair, g_all.at[k], sem_g.at[k], peer) for k, peer in enumerate((sib, over, diag))]

    bv[...] = jnp.full_like(bv, NEG)
    bi[...] = jnp.zeros_like(bi)
    heat = jnp.full((1, 128), temp_ref[0, 0], jnp.float32)
    fold = jnp.where(heat > 2.0**64, 2.0**-64, 1.0)
    c1 = (SOFT_CAP * fold)[:, :1]
    c2 = (1.0 / (heat * fold))[:, :1]

    def score(i, rows, nz_refs):
        slot = lax.rem(i + WEIGHT_GROUPS, RING_GROUPS)
        group = group_of(i)
        for j in range(NSUB):
            e_copy(i, j).wait()
        lhs = f_two[pl.ds(0, rows)]
        for start, size, turn in CUTS:
            block = ring[pl.ds(pl.multiple_of(slot * GROUP + start, 256), size), :]
            if turn:
                for k in range(0, width, 256):
                    turned[pl.ds(k, 256)] = block[:, k : k + 256].T
                z = jnp.dot(lhs, turned[...], preferred_element_type=jnp.float32)
            else:
                z = lax.dot_general(lhs, block, (((1,), (1,)), ((), ())), preferred_element_type=jnp.float32)
            s = jnp.tanh(z * (1.0 / SOFT_CAP)) * c1 * c2
            for part, nz in enumerate(nz_refs):
                take_rows = pl.ds(part * batch, batch)
                for q in range(size // 256):
                    v = s[part * batch : (part + 1) * batch, q * 256 : (q + 1) * 256]
                    v = v + nz[:, start + q * 256 : start + (q + 1) * 256]
                    old = bv[take_rows]
                    better = v > old
                    bv[take_rows] = jnp.where(better, v, old)
                    bi[take_rows] = jnp.where(better, group * (GROUP // 256) + (start // 256 + q), bi[take_rows])

        @pl.when(i + RING_GROUPS < n_iter)
        def _():
            e_start(i + RING_GROUPS)

    def own(i):
        no_copy(i).wait()
        score(i, batch, [nz_own.at[i]])

        @pl.when(i == SPREAD)
        def _():
            f_pair_copy.wait()
            for copy in g_copies:
                copy.start()

    def shared(i):
        no_copy(i).wait()
        nr_copy(i - HEAD).wait_recv()
        score(i, 2 * batch, [nz_own.at[i], nz_oth.at[i - HEAD]])

    def settle(part):
        val = bv[pl.ds(part * batch, batch)]
        tile = bi[pl.ds(part * batch, batch)]
        top = jnp.max(val, axis=1, keepdims=True)
        ids = (tile * 256 + lax.broadcasted_iota(jnp.int32, tile.shape, 1)).astype(jnp.float32)
        row = jnp.min(jnp.where(val == top, ids, 3.0e7), axis=1, keepdims=True)
        return jnp.broadcast_to(top, (batch, 128)), jnp.broadcast_to(row, (batch, 128))

    by = remote(best_oth, best_in, sem_by, pair)

    @pl.loop(0, 2)
    def _(phase):
        pl.loop(jnp.where(phase == 0, 0, HEAD + half), jnp.where(phase == 0, HEAD, n_iter))(own)

        @pl.when(phase == 0)
        def _():
            for copy in g_copies:
                copy.wait()
            f_two[pl.ds(batch, batch)] = in_order(f_pair, g_all)
            pl.loop(HEAD, HEAD + half)(shared)
            o_val, o_row = settle(1)
            best_oth[0] = o_val
            best_oth[1] = o_row
            by.start()

    pl.loop(0, half)(lambda j: nr_copy(j).wait_send())
    m_val, m_row = settle(0)
    by.wait()
    keep = m_val >= best_in[0]
    top = jnp.where(keep, m_val, best_in[0])
    row = jnp.where(keep, m_row, best_in[1])
    offset = (tp * (n_group * GROUP)).astype(jnp.float32)
    hb = batch // 2
    for part in range(2):
        best_ref[part, 0] = top[part * hb : (part + 1) * hb]
        best_ref[part, 1] = row[part * hb : (part + 1) * hb] + offset
    line_ref[...] = as_line(row.astype(jnp.int32))


def lookup_kernel(line_ref, emb_ref, out_ref, tiles, sem):
    half, batch = out_ref.shape[1], 2 * out_ref.shape[1]
    for r in range(batch):
        base = pl.multiple_of(lax.div(line_ref[0, r], 8) * 8, 8)
        pltpu.make_async_copy(emb_ref.at[pl.ds(base, 8)], tiles.at[pl.ds(8 * r, 8)], sem).start()
    shape = (batch, 8 * batch)
    place = lax.broadcasted_iota(jnp.int32, (batch, 1), 0)
    want = 8 * place
    for r in range(batch):
        want = want + jnp.where(place == r, lax.rem(line_ref[0, r], 8), 0)
    pick = (lax.broadcasted_iota(jnp.int32, shape, 1) == want).astype(jnp.bfloat16)
    pltpu.make_async_copy(emb_ref.at[pl.ds(0, 8 * batch)], tiles, sem).wait()
    rows = jnp.dot(pick, tiles[...], preferred_element_type=jnp.float32).astype(jnp.bfloat16)
    out_ref[0] = rows[:half]
    out_ref[1] = rows[half:]


def lookup(line, batch, embedding):
    width = embedding.shape[1]
    return pl.pallas_call(
        lookup_kernel,
        out_shape=jax.ShapeDtypeStruct((2, batch // 2, width), jnp.bfloat16),
        in_specs=[pl.BlockSpec(memory_space=pltpu.SMEM), pl.BlockSpec(memory_space=pl.ANY)],
        out_specs=pl.BlockSpec(memory_space=pltpu.VMEM),
        scratch_shapes=[pltpu.VMEM((8 * batch, width), jnp.bfloat16), pltpu.SemaphoreType.DMA(())],
        compiler_params=pltpu.CompilerParams(vmem_limit_bytes=66_000_000),
        name="lookup",
    )(line, embedding)


def call_step(step, steps, batch, width, inner, vocab_local, embed_scale, operands):
    first, last = step == 0, step == steps
    f32, bf16, i32 = jnp.float32, jnp.bfloat16, jnp.int32
    vmem, hbm = pl.BlockSpec(memory_space=pltpu.VMEM), pl.BlockSpec(memory_space=pl.ANY)
    dma = pltpu.SemaphoreType.DMA
    n_group = vocab_local // GROUP
    half = (n_group - OWN) // 2
    n_iter = OWN + half
    hb, quarter = batch // 2, batch // 4
    in_specs = [hbm] * (1 if first else 2) + [vmem] * ((step - 1) * last)
    if not last:
        in_specs += [hbm] * 3 + [pl.BlockSpec(memory_space=pltpu.SMEM)] + [hbm] * 5
    outs, scratch = [], []
    if first:
        scratch += [pltpu.VMEM((batch, width), bf16), dma((1,))]
    else:
        scratch += [pltpu.VMEM((2, hb, width), bf16), pltpu.VMEM((2, 2, hb, 128), f32), dma((2,))]
    if not last:
        scratch += [pltpu.VMEM((width,), bf16)] * 3 + [dma((3,))]
    if not first:
        outs += [jax.ShapeDtypeStruct((steps, batch) if last else (1, 128), i32), jax.ShapeDtypeStruct((batch, width), bf16)]
        rows, meta = pltpu.VMEM((hb, width), bf16), pltpu.VMEM((2, hb, 128), f32)
        scratch += [rows, meta] * 5 + [dma((3, 2)), dma((3, 2))]
    if not last:
        outs += [
            jax.ShapeDtypeStruct((2, 2, hb, 128), f32),
            jax.ShapeDtypeStruct((1, 128), i32),
        ]
        scratch += [
            pltpu.VMEM((RING_GROUPS * GROUP, width), bf16),
            pltpu.VMEM((n_iter, batch, GROUP), f32),
            pltpu.VMEM((half, batch, GROUP), f32),
            pltpu.VMEM((4, quarter, width), f32),
            pltpu.VMEM((2, quarter, width), f32),
            pltpu.VMEM((2, quarter, width), f32),
            pltpu.VMEM((quarter, width), f32),
            pltpu.VMEM((quarter, width), bf16),
            pltpu.VMEM((3, quarter, width), bf16),
            pltpu.VMEM((quarter, width), bf16),
            pltpu.VMEM((3, quarter, width), bf16),
            pltpu.VMEM((2 * batch, width), bf16),
            pltpu.VMEM((4, quarter, width), f32),
            pltpu.VMEM((batch, inner), bf16),
            pltpu.VMEM((width, max(c[1] for c in CUTS if c[2])), bf16),
            pltpu.VMEM((2 * batch, 256), f32),
            pltpu.VMEM((2 * batch, 256), i32),
            pltpu.VMEM((2, batch, 128), f32),
            pltpu.VMEM((2, batch, 128), f32),
            dma((3,)),
            dma((RING_GROUPS, NSUB)),
            dma((n_iter,)),
            dma((half,)),
            dma((half,)),
            dma((2,)),
            dma((2,)),
            dma((3, 2)),
            dma((2,)),
            dma((3, 2)),
            dma((2,)),
        ]
    return pl.pallas_call(
        functools.partial(step_kernel, (step, first, last, n_group, embed_scale)),
        out_shape=outs,
        in_specs=in_specs,
        out_specs=[vmem] * len(outs),
        scratch_shapes=scratch,
        compiler_params=pltpu.CompilerParams(
            collective_id=step, has_side_effects=True, vmem_limit_bytes=66_000_000
        ),
        name=f"step{step}",
    )(*operands)


def solution(mesh):
    def local_steps(start_hidden, embedding, pre_norm, w_gate, w_up, w_down, post_norm, final_norm, temperature, step_noise):
        vocab_local, width = embedding.shape
        batch, steps = start_hidden.shape[0], step_noise.shape[0]
        inner = w_gate.shape[1]
        embed_scale = float(np.float64(math.sqrt(width)).astype(jnp.bfloat16))
        common = [pre_norm, post_norm, final_norm, temperature.reshape(1, 1), w_gate, w_up, w_down, embedding, step_noise]
        sizes = (steps, batch, width, inner, vocab_local, embed_scale)
        best, line = call_step(0, *sizes, [start_hidden, *common])
        lines = []
        for step in range(1, steps):
            outs = call_step(step, *sizes, [lookup(line, batch, embedding), best, *common])
            lines.append(outs[0])
            best, line = outs[2:]
        tokens, hidden = call_step(steps, *sizes, [lookup(line, batch, embedding), best, *lines])
        return tokens, hidden

    return jax.shard_map(
        local_steps,
        mesh=mesh,
        in_specs=(P("dp", None), P("tp", None), P(), P(None, "tp"), P(None, "tp"), P("tp", None), P(), P(), P(), P(None, "dp", "tp")),
        out_specs=(P(None, "dp"), P("dp", None)),
        check_vma=False,
    )
```

```python
import functools
import math

import jax
import jax.numpy as jnp
import numpy as np
from jax import lax
from jax.experimental import pallas as pl
from jax.experimental.pallas import tpu as pltpu
from jax.sharding import PartitionSpec as P

SOFT_CAP = 30.0
EPSILON = 1e-6
MESH = pl.DeviceIdType.MESH

SUB = 640
NSUB = 2
GROUP = SUB * NSUB
RING_GROUPS = 9
SPREAD = 3
WEIGHT_GROUPS = 6
CUTS = ((0, 512, False), (512, 768, True))
HEAD = 12
TAIL = 2
OWN = HEAD + TAIL
NEG = -3.0e38


def gain(ref):
    return ref[...].astype(jnp.float32).reshape(1, ref.shape[0])


def rms_scale(x_f32, gain_row):
    mean_sq = jnp.mean(x_f32 * x_f32, axis=-1, keepdims=True)
    return x_f32 * lax.rsqrt(mean_sq + EPSILON) * (1.0 + gain_row)


def remote(src, dst, sem, peer):
    return pltpu.make_async_remote_copy(
        src_ref=src, dst_ref=dst, send_sem=sem.at[0], recv_sem=sem.at[1], device_id=peer, device_id_type=MESH
    )


def as_line(wide):
    eye = lax.broadcasted_iota(jnp.int32, wide.shape, 0) == lax.broadcasted_iota(jnp.int32, wide.shape, 1)
    return jnp.sum(jnp.where(eye, wide, 0), axis=0, keepdims=True)


def step_kernel(cfg, *refs):
    step, first, last, n_group, embed_scale = cfg
    refs = list(refs)
    take = lambda n: [refs.pop(0) for _ in range(n)]
    if first:
        (hid_hbm,) = take(1)
    else:
        rows_hbm, meta_hbm = take(2)
        if last:
            old_refs = take(step - 1)
    if not last:
        pre_hbm, post_hbm, fin_hbm, temp_ref, wg_ref, wu_ref, wd_ref, emb_ref, noise_ref = take(9)
    if not first:
        tok_ref, hout_ref = take(2)
    if not last:
        best_ref, line_ref = take(2)
    if first:
        hid_ref, sem_in = take(2)
        inputs = [(hid_hbm, hid_ref)]
    else:
        rows_ref, meta_ref, sem_in = take(3)
        inputs = [(rows_hbm, rows_ref), (meta_hbm, meta_ref)]
    if not last:
        pre_ref, post_ref, fin_ref, sem_gain = take(4)
        gains = [(pre_hbm, pre_ref), (post_hbm, post_ref), (fin_hbm, fin_ref)]
    in_copies = [pltpu.make_async_copy(src, dst, sem_in.at[k]) for k, (src, dst) in enumerate(inputs)]
    for copy in in_copies:
        copy.start()
    if not first:
        rows_a, meta_a, rows_m, meta_m, rows_b, meta_b, rows_f, meta_f, rows_c, meta_c, sem_rows, sem_meta = take(12)
    if not last:
        (ring, nz_own, nz_oth, part_s, part_a, half_s, part_b, f_send, f_all, f_pair, g_all, f_two,
         hid32, gate_s, turned, bv, bi, best_oth, best_in,
         sem_w, sem_e, sem_no, sem_ns, sem_nr, sem_ra, sem_rb, sem_f, sem_fo, sem_g, sem_by) = take(30)

    dp, tp = lax.axis_index("dp"), lax.axis_index("tp")
    core, chip = lax.rem(tp, 2), lax.div(tp, 2)
    tp_sib = chip * 2 + (1 - core)
    tp_x = (1 - chip) * 2 + core
    tp_diag = (1 - chip) * 2 + (1 - core)
    sib, over, diag, pair = (dp, tp_sib), (dp, tp_x), (dp, tp_diag), (1 - dp, tp)

    if not last:
        half = (n_group - OWN) // 2
        n_iter = OWN + half
        width = ring.shape[1]
        inner = wg_ref.shape[1]
        weights = [(wg_ref, 0, width), (wu_ref, width, width), (wd_ref, 2 * width, inner)]
        w_copies = [
            pltpu.make_async_copy(ref, ring.at[pl.ds(base, rows)], sem_w.at[k])
            for k, (ref, base, rows) in enumerate(weights)
        ]

        def w_start(k):
            ref, base, rows = weights[k]
            piece = rows // 9
            for p in range(0, rows, piece):
                pltpu.make_async_copy(ref.at[pl.ds(p, piece)], ring.at[pl.ds(base + p, piece)], sem_w.at[k]).start()

        def group_of(i):
            moved = jnp.where(i < HEAD + half, dp * half, half)
            return i + jnp.where(i < HEAD, 0, moved)

        def e_copy(i, j):
            group = group_of(i)
            slot = lax.rem(i + WEIGHT_GROUPS, RING_GROUPS)
            return pltpu.make_async_copy(
                emb_ref.at[pl.ds(group * GROUP + j * SUB, SUB)],
                ring.at[pl.ds(slot * GROUP + j * SUB, SUB)],
                sem_e.at[slot, j],
            )

        def e_start(i):
            for j in range(NSUB):
                e_copy(i, j).start()
            no_copy(i).start()

        def no_copy(i):
            group = group_of(i)
            return pltpu.make_async_copy(
                noise_ref.at[step, :, pl.ds(group * GROUP, GROUP)], nz_own.at[lax.rem(i, RING_GROUPS)], sem_no.at[lax.rem(i, RING_GROUPS)]
            )

        def nr_copy(j):
            group = HEAD + (1 - dp) * half + j
            return pltpu.make_async_remote_copy(
                src_ref=noise_ref.at[step, :, pl.ds(group * GROUP, GROUP)],
                dst_ref=nz_oth.at[j],
                send_sem=sem_ns.at[j],
                recv_sem=sem_nr.at[j],
                device_id=pair,
                device_id_type=MESH,
            )

        gain_copies = [pltpu.make_async_copy(src, dst, sem_gain.at[k]) for k, (src, dst) in enumerate(gains)]
        for copy in gain_copies:
            copy.start()
        w_start(0)
        w_start(1)

    barrier = pltpu.get_barrier_semaphore()
    peers = (sib, over) if last else (sib, over, diag, pair)
    for peer in peers:
        pl.semaphore_signal(barrier, inc=1, device_id=peer, device_id_type=MESH)
    pl.semaphore_wait(barrier, len(peers))

    def fetch_head():
        for i in range(RING_GROUPS - WEIGHT_GROUPS):
            e_start(i)

    if not last:
        early = 6
        pl.loop(0, early)(lambda j: nr_copy(j).start())

    for copy in in_copies:
        copy.wait()
    if first:
        hid = hid_ref[...].astype(jnp.float32)
        w_copies[0].wait()
        w_start(2)
        fetch_head()
    else:
        a_rows = remote(rows_ref.at[1 - core], rows_a, sem_rows.at[0], sib)
        a_meta = remote(meta_ref.at[1 - core], meta_a, sem_meta.at[0], sib)
        a_rows.start()
        a_meta.start()
        a_rows.wait()
        a_meta.wait()
        mine = meta_ref[core]
        seen = meta_a[...]
        keep = mine[0] >= seen[0]
        meta_m[...] = jnp.where(keep[None], mine, seen)
        rows_m[...] = jnp.where(
            keep[:, :1], rows_ref[core].astype(jnp.float32), rows_a[...].astype(jnp.float32)
        ).astype(jnp.bfloat16)
        b_rows = remote(rows_m, rows_b, sem_rows.at[1], over)
        b_meta = remote(meta_m, meta_b, sem_meta.at[1], over)
        b_rows.start()
        b_meta.start()
        b_rows.wait()
        b_meta.wait()
        if not last:
            w_start(2)
        mine = meta_m[...]
        seen = meta_b[...]
        keep = mine[0] >= seen[0]
        meta_f[...] = jnp.where(keep[None], mine, seen)
        rows_f[...] = jnp.where(
            keep[:, :1], rows_m[...].astype(jnp.float32), rows_b[...].astype(jnp.float32)
        ).astype(jnp.bfloat16)
        c_rows = remote(rows_f, rows_c, sem_rows.at[2], sib)
        c_meta = remote(meta_f, meta_c, sem_meta.at[2], sib)
        c_rows.start()
        c_meta.start()
        c_rows.wait()
        c_meta.wait()
        if not last:
            w_copies[0].wait()
            fetch_head()
        low = core == 0
        r_f, r_c = rows_f[...].astype(jnp.float32), rows_c[...].astype(jnp.float32)
        t_f, t_c = meta_f[1], meta_c[1]
        picked = jnp.concatenate([jnp.where(low, r_f, r_c), jnp.where(low, r_c, r_f)], axis=0)
        token = jnp.concatenate([jnp.where(low, t_f, t_c), jnp.where(low, t_c, t_f)], axis=0).astype(jnp.int32)
        if last:
            for k, line in enumerate([ref[...] for ref in old_refs] + [as_line(token)]):
                tok_ref[k : k + 1] = line[:, : token.shape[0]]
        else:
            tok_ref[...] = as_line(token)
        hid_bf = (picked * embed_scale).astype(jnp.bfloat16)
        hout_ref[...] = hid_bf
        hid = hid_bf.astype(jnp.float32)

    if last:
        return

    batch = hid.shape[0]
    quarter = batch // 4
    hid32[...] = hid.reshape(4, quarter, width)
    for copy in gain_copies:
        copy.wait()
    normed = rms_scale(hid, gain(pre_ref)).astype(jnp.bfloat16)
    f_two[pl.ds(0, batch)] = normed
    w_copies[1].wait()
    col = 768

    @pl.loop(0, inner // col)
    def _(n):
        cols = pl.ds(pl.multiple_of(n * col, col), col)
        lhs = f_two[pl.ds(0, batch)]
        gate = jnp.dot(lhs, ring[pl.ds(0, width), cols], preferred_element_type=jnp.float32)
        up = jnp.dot(lhs, ring[pl.ds(width, width), cols], preferred_element_type=jnp.float32)
        gate_s[:, cols] = (jax.nn.gelu(gate, approximate=True) * up).astype(jnp.bfloat16)

    free = RING_GROUPS - WEIGHT_GROUPS + (2 * width) // GROUP
    for i in range(RING_GROUPS - WEIGHT_GROUPS, free):
        e_start(i)
    w_copies[2].wait()

    @pl.loop(0, width // col)
    def _(n):
        cols = pl.ds(pl.multiple_of(n * col, col), col)
        part_s[:, :, cols] = jnp.dot(
            gate_s[...], ring[pl.ds(2 * width, inner), cols], preferred_element_type=jnp.float32
        ).reshape(4, quarter, col)

    for i in range(free, RING_GROUPS):
        e_start(i)

    ra = remote(part_s.at[pl.ds(2 * (1 - core), 2)], part_a, sem_ra, sib)
    ra.start()
    ra.wait()
    half_s[...] = part_s[pl.ds(2 * core, 2)] + part_a[...]
    rb = remote(half_s.at[1 - chip], part_b, sem_rb, over)
    rb.start()
    rb.wait()
    down_sum = half_s[chip] + part_b[...]
    place = 2 * core + chip
    post_out = rms_scale(down_sum, gain(post_ref)).astype(jnp.bfloat16)
    resid = (hid32[place] + post_out.astype(jnp.float32)).astype(jnp.bfloat16)
    final_in = rms_scale(resid.astype(jnp.float32), gain(fin_ref)).astype(jnp.bfloat16)
    f_send[...] = final_in
    f_copies = [remote(f_send, f_all.at[k], sem_f.at[k], peer) for k, peer in enumerate((sib, over, diag))]
    f_pair_copy = remote(f_send, f_pair, sem_fo, pair)
    for copy in [*f_copies, f_pair_copy]:
        copy.start()
    pl.loop(early, half)(lambda j: nr_copy(j).start())
    for copy in f_copies:
        copy.wait()
    low_core, low_chip = core == 0, chip == 0

    def in_order(mine_ref, others_ref):
        me_f, sib_f, over_f, diag_f = (v.astype(jnp.float32) for v in (mine_ref[...], *(others_ref[k] for k in range(3))))
        core0 = [jnp.where(low_core, a, b) for a, b in ((me_f, sib_f), (over_f, diag_f))]
        core1 = [jnp.where(low_core, b, a) for a, b in ((me_f, sib_f), (over_f, diag_f))]
        order = [
            jnp.where(low_chip, core0[0], core0[1]),
            jnp.where(low_chip, core0[1], core0[0]),
            jnp.where(low_chip, core1[0], core1[1]),
            jnp.where(low_chip, core1[1], core1[0]),
        ]
        return jnp.concatenate(order, axis=0).astype(jnp.bfloat16)

    f_two[pl.ds(0, batch)] = in_order(f_send, f_all)
    g_copies = [remote(f_pair, g_all.at[k], sem_g.at[k], peer) for k, peer in enumerate((sib, over, diag))]

    bv[...] = jnp.full_like(bv, NEG)
    bi[...] = jnp.zeros_like(bi)
    heat = jnp.full((1, 128), temp_ref[0, 0], jnp.float32)
    fold = jnp.where(heat > 2.0**64, 2.0**-64, 1.0)
    c1 = (SOFT_CAP * fold)[:, :1]
    c2 = (1.0 / (heat * fold))[:, :1]

    def score(i, rows, nz_refs):
        slot = lax.rem(i + WEIGHT_GROUPS, RING_GROUPS)
        group = group_of(i)
        for j in range(NSUB):
            e_copy(i, j).wait()
        lhs = f_two[pl.ds(0, rows)]
        for start, size, turn in CUTS:
            block = ring[pl.ds(pl.multiple_of(slot * GROUP + start, 256), size), :]
            if turn:
                for k in range(0, width, 256):
                    turned[pl.ds(k, 256)] = block[:, k : k + 256].T
                z = jnp.dot(lhs, turned[...], preferred_element_type=jnp.float32)
            else:
                z = lax.dot_general(lhs, block, (((1,), (1,)), ((), ())), preferred_element_type=jnp.float32)
            s = jnp.tanh(z * (1.0 / SOFT_CAP)) * c1 * c2
            for part, nz in enumerate(nz_refs):
                take_rows = pl.ds(part * batch, batch)
                for q in range(size // 256):
                    v = s[part * batch : (part + 1) * batch, q * 256 : (q + 1) * 256]
                    v = v + nz[:, start + q * 256 : start + (q + 1) * 256]
                    old = bv[take_rows]
                    better = v > old
                    bv[take_rows] = jnp.where(better, v, old)
                    bi[take_rows] = jnp.where(better, group * (GROUP // 256) + (start // 256 + q), bi[take_rows])

        @pl.when(i + RING_GROUPS < n_iter)
        def _():
            e_start(i + RING_GROUPS)

    def own(i):
        no_copy(i).wait()
        score(i, batch, [nz_own.at[lax.rem(i, RING_GROUPS)]])

        @pl.when(i == SPREAD)
        def _():
            f_pair_copy.wait()
            for copy in g_copies:
                copy.start()

    def shared(i):
        no_copy(i).wait()
        nr_copy(i - HEAD).wait_recv()
        score(i, 2 * batch, [nz_own.at[lax.rem(i, RING_GROUPS)], nz_oth.at[i - HEAD]])

    def settle(part):
        val = bv[pl.ds(part * batch, batch)]
        tile = bi[pl.ds(part * batch, batch)]
        top = jnp.max(val, axis=1, keepdims=True)
        ids = (tile * 256 + lax.broadcasted_iota(jnp.int32, tile.shape, 1)).astype(jnp.float32)
        row = jnp.min(jnp.where(val == top, ids, 3.0e7), axis=1, keepdims=True)
        return jnp.broadcast_to(top, (batch, 128)), jnp.broadcast_to(row, (batch, 128))

    by = remote(best_oth, best_in, sem_by, pair)

    @pl.loop(0, 2)
    def _(phase):
        pl.loop(jnp.where(phase == 0, 0, HEAD + half), jnp.where(phase == 0, HEAD, n_iter))(own)

        @pl.when(phase == 0)
        def _():
            for copy in g_copies:
                copy.wait()
            f_two[pl.ds(batch, batch)] = in_order(f_pair, g_all)
            pl.loop(HEAD, HEAD + half)(shared)
            o_val, o_row = settle(1)
            best_oth[0] = o_val
            best_oth[1] = o_row
            by.start()

    pl.loop(0, half)(lambda j: nr_copy(j).wait_send())
    m_val, m_row = settle(0)
    by.wait()
    keep = m_val >= best_in[0]
    top = jnp.where(keep, m_val, best_in[0])
    row = jnp.where(keep, m_row, best_in[1])
    offset = (tp * (n_group * GROUP)).astype(jnp.float32)
    hb = batch // 2
    for part in range(2):
        best_ref[part, 0] = top[part * hb : (part + 1) * hb]
        best_ref[part, 1] = row[part * hb : (part + 1) * hb] + offset
    line_ref[...] = as_line(row.astype(jnp.int32))


def lookup_kernel(line_ref, emb_ref, out_ref, tiles, sem):
    half, batch = out_ref.shape[1], 2 * out_ref.shape[1]
    for r in range(batch):
        base = pl.multiple_of(lax.div(line_ref[0, r], 8) * 8, 8)
        pltpu.make_async_copy(emb_ref.at[pl.ds(base, 8)], tiles.at[pl.ds(8 * r, 8)], sem).start()
    shape = (batch, 8 * batch)
    place = lax.broadcasted_iota(jnp.int32, (batch, 1), 0)
    want = 8 * place
    for r in range(batch):
        want = want + jnp.where(place == r, lax.rem(line_ref[0, r], 8), 0)
    pick = (lax.broadcasted_iota(jnp.int32, shape, 1) == want).astype(jnp.bfloat16)
    pltpu.make_async_copy(emb_ref.at[pl.ds(0, 8 * batch)], tiles, sem).wait()
    rows = jnp.dot(pick, tiles[...], preferred_element_type=jnp.float32).astype(jnp.bfloat16)
    out_ref[0] = rows[:half]
    out_ref[1] = rows[half:]


def lookup(line, batch, embedding):
    width = embedding.shape[1]
    return pl.pallas_call(
        lookup_kernel,
        out_shape=jax.ShapeDtypeStruct((2, batch // 2, width), jnp.bfloat16),
        in_specs=[pl.BlockSpec(memory_space=pltpu.SMEM), pl.BlockSpec(memory_space=pl.ANY)],
        out_specs=pl.BlockSpec(memory_space=pltpu.VMEM),
        scratch_shapes=[pltpu.VMEM((8 * batch, width), jnp.bfloat16), pltpu.SemaphoreType.DMA(())],
        compiler_params=pltpu.CompilerParams(vmem_limit_bytes=66_000_000),
        name="lookup",
    )(line, embedding)


def call_step(step, steps, batch, width, inner, vocab_local, embed_scale, operands):
    first, last = step == 0, step == steps
    f32, bf16, i32 = jnp.float32, jnp.bfloat16, jnp.int32
    vmem, hbm = pl.BlockSpec(memory_space=pltpu.VMEM), pl.BlockSpec(memory_space=pl.ANY)
    dma = pltpu.SemaphoreType.DMA
    n_group = vocab_local // GROUP
    half = (n_group - OWN) // 2
    n_iter = OWN + half
    hb, quarter = batch // 2, batch // 4
    in_specs = [hbm] * (1 if first else 2) + [vmem] * ((step - 1) * last)
    if not last:
        in_specs += [hbm] * 3 + [pl.BlockSpec(memory_space=pltpu.SMEM)] + [hbm] * 5
    outs, scratch = [], []
    if first:
        scratch += [pltpu.VMEM((batch, width), bf16), dma((1,))]
    else:
        scratch += [pltpu.VMEM((2, hb, width), bf16), pltpu.VMEM((2, 2, hb, 128), f32), dma((2,))]
    if not last:
        scratch += [pltpu.VMEM((width,), bf16)] * 3 + [dma((3,))]
    if not first:
        outs += [jax.ShapeDtypeStruct((steps, batch) if last else (1, 128), i32), jax.ShapeDtypeStruct((batch, width), bf16)]
        rows, meta = pltpu.VMEM((hb, width), bf16), pltpu.VMEM((2, hb, 128), f32)
        scratch += [rows, meta] * 5 + [dma((3, 2)), dma((3, 2))]
    if not last:
        outs += [
            jax.ShapeDtypeStruct((2, 2, hb, 128), f32),
            jax.ShapeDtypeStruct((1, 128), i32),
        ]
        scratch += [
            pltpu.VMEM((RING_GROUPS * GROUP, width), bf16),
            pltpu.VMEM((RING_GROUPS, batch, GROUP), f32),
            pltpu.VMEM((half, batch, GROUP), f32),
            pltpu.VMEM((4, quarter, width), f32),
            pltpu.VMEM((2, quarter, width), f32),
            pltpu.VMEM((2, quarter, width), f32),
            pltpu.VMEM((quarter, width), f32),
            pltpu.VMEM((quarter, width), bf16),
            pltpu.VMEM((3, quarter, width), bf16),
            pltpu.VMEM((quarter, width), bf16),
            pltpu.VMEM((3, quarter, width), bf16),
            pltpu.VMEM((2 * batch, width), bf16),
            pltpu.VMEM((4, quarter, width), f32),
            pltpu.VMEM((batch, inner), bf16),
            pltpu.VMEM((width, max(c[1] for c in CUTS if c[2])), bf16),
            pltpu.VMEM((2 * batch, 256), f32),
            pltpu.VMEM((2 * batch, 256), i32),
            pltpu.VMEM((2, batch, 128), f32),
            pltpu.VMEM((2, batch, 128), f32),
            dma((3,)),
            dma((RING_GROUPS, NSUB)),
            dma((RING_GROUPS,)),
            dma((half,)),
            dma((half,)),
            dma((2,)),
            dma((2,)),
            dma((3, 2)),
            dma((2,)),
            dma((3, 2)),
            dma((2,)),
        ]
    return pl.pallas_call(
        functools.partial(step_kernel, (step, first, last, n_group, embed_scale)),
        out_shape=outs,
        in_specs=in_specs,
        out_specs=[vmem] * len(outs),
        scratch_shapes=scratch,
        compiler_params=pltpu.CompilerParams(
            collective_id=step, has_side_effects=True, vmem_limit_bytes=66_000_000
        ),
        name=f"step{step}",
    )(*operands)


def solution(mesh):
    def local_steps(start_hidden, embedding, pre_norm, w_gate, w_up, w_down, post_norm, final_norm, temperature, step_noise):
        vocab_local, width = embedding.shape
        batch, steps = start_hidden.shape[0], step_noise.shape[0]
        inner = w_gate.shape[1]
        embed_scale = float(np.float64(math.sqrt(width)).astype(jnp.bfloat16))
        common = [pre_norm, post_norm, final_norm, temperature.reshape(1, 1), w_gate, w_up, w_down, embedding, step_noise]
        sizes = (steps, batch, width, inner, vocab_local, embed_scale)
        best, line = call_step(0, *sizes, [start_hidden, *common])
        lines = []
        for step in range(1, steps):
            outs = call_step(step, *sizes, [lookup(line, batch, embedding), best, *common])
            lines.append(outs[0])
            best, line = outs[2:]
        tokens, hidden = call_step(steps, *sizes, [lookup(line, batch, embedding), best, *lines])
        return tokens, hidden

    return jax.shard_map(
        local_steps,
        mesh=mesh,
        in_specs=(P("dp", None), P("tp", None), P(), P(None, "tp"), P(None, "tp"), P("tp", None), P(), P(), P(), P(None, "dp", "tp")),
        out_specs=(P(None, "dp"), P("dp", None)),
        check_vma=False,
    )
```

```python
import functools
import math

import jax
import jax.numpy as jnp
import numpy as np
from jax import lax
from jax.experimental import pallas as pl
from jax.experimental.pallas import tpu as pltpu
from jax.sharding import PartitionSpec as P

SOFT_CAP = 30.0
EPSILON = 1e-6
MESH = pl.DeviceIdType.MESH

SUB = 640
NSUB = 2
GROUP = SUB * NSUB
RING_GROUPS = 9
SPREAD = 3
WEIGHT_GROUPS = 6
CUTS = ((0, 512, False), (512, 768, True))
HEAD = 15
TAIL = 1
OWN = HEAD + TAIL
NEG = -3.0e38


def gain(ref):
    return ref[...].astype(jnp.float32).reshape(1, ref.shape[0])


def rms_scale(x_f32, gain_row):
    mean_sq = jnp.mean(x_f32 * x_f32, axis=-1, keepdims=True)
    return x_f32 * lax.rsqrt(mean_sq + EPSILON) * (1.0 + gain_row)


def remote(src, dst, sem, peer):
    return pltpu.make_async_remote_copy(
        src_ref=src, dst_ref=dst, send_sem=sem.at[0], recv_sem=sem.at[1], device_id=peer, device_id_type=MESH
    )


def as_line(wide):
    eye = lax.broadcasted_iota(jnp.int32, wide.shape, 0) == lax.broadcasted_iota(jnp.int32, wide.shape, 1)
    return jnp.sum(jnp.where(eye, wide, 0), axis=0, keepdims=True)


def step_kernel(cfg, *refs):
    step, first, last, n_group, embed_scale = cfg
    refs = list(refs)
    take = lambda n: [refs.pop(0) for _ in range(n)]
    if first:
        (hid_hbm,) = take(1)
    else:
        rows_hbm, meta_hbm = take(2)
        if last:
            old_refs = take(step - 1)
    if not last:
        pre_hbm, post_hbm, fin_hbm, temp_ref, wg_ref, wu_ref, wd_ref, emb_ref, noise_ref = take(9)
    if not first:
        tok_ref, hout_ref = take(2)
    if not last:
        best_ref, line_ref = take(2)
    if first:
        hid_ref, sem_in = take(2)
        inputs = [(hid_hbm, hid_ref)]
    else:
        rows_ref, meta_ref, sem_in = take(3)
        inputs = [(rows_hbm, rows_ref), (meta_hbm, meta_ref)]
    if not last:
        pre_ref, post_ref, fin_ref, sem_gain = take(4)
        gains = [(pre_hbm, pre_ref), (post_hbm, post_ref), (fin_hbm, fin_ref)]
    in_copies = [pltpu.make_async_copy(src, dst, sem_in.at[k]) for k, (src, dst) in enumerate(inputs)]
    for copy in in_copies:
        copy.start()
    if not first:
        rows_a, meta_a, rows_m, meta_m, rows_b, meta_b, rows_f, meta_f, rows_c, meta_c, sem_rows, sem_meta = take(12)
    if not last:
        (ring, nz_own, nz_oth, part_s, part_a, half_s, part_b, f_send, f_all, f_pair, g_all, f_two,
         hid32, gate_s, turned, bv, bi, best_oth, best_in,
         sem_w, sem_e, sem_no, sem_ns, sem_nr, sem_ra, sem_rb, sem_f, sem_fo, sem_g, sem_by) = take(30)

    dp, tp = lax.axis_index("dp"), lax.axis_index("tp")
    core, chip = lax.rem(tp, 2), lax.div(tp, 2)
    tp_sib = chip * 2 + (1 - core)
    tp_x = (1 - chip) * 2 + core
    tp_diag = (1 - chip) * 2 + (1 - core)
    sib, over, diag, pair = (dp, tp_sib), (dp, tp_x), (dp, tp_diag), (1 - dp, tp)

    if not last:
        half = (n_group - OWN) // 2
        n_iter = OWN + half
        width = ring.shape[1]
        inner = wg_ref.shape[1]
        weights = [(wg_ref, 0, width), (wu_ref, width, width), (wd_ref, 2 * width, inner)]
        w_copies = [
            pltpu.make_async_copy(ref, ring.at[pl.ds(base, rows)], sem_w.at[k])
            for k, (ref, base, rows) in enumerate(weights)
        ]

        def w_start(k):
            ref, base, rows = weights[k]
            piece = rows // 9
            for p in range(0, rows, piece):
                pltpu.make_async_copy(ref.at[pl.ds(p, piece)], ring.at[pl.ds(base + p, piece)], sem_w.at[k]).start()

        def group_of(i):
            moved = jnp.where(i < HEAD + half, dp * half, half)
            return i + jnp.where(i < HEAD, 0, moved)

        def e_copy(i, j):
            group = group_of(i)
            slot = lax.rem(i + WEIGHT_GROUPS, RING_GROUPS)
            return pltpu.make_async_copy(
                emb_ref.at[pl.ds(group * GROUP + j * SUB, SUB)],
                ring.at[pl.ds(slot * GROUP + j * SUB, SUB)],
                sem_e.at[slot, j],
            )

        def e_start(i):
            for j in range(NSUB):
                e_copy(i, j).start()
            no_copy(i).start()

        def no_copy(i):
            group = group_of(i)
            return pltpu.make_async_copy(
                noise_ref.at[step, :, pl.ds(group * GROUP, GROUP)], nz_own.at[lax.rem(i, RING_GROUPS)], sem_no.at[lax.rem(i, RING_GROUPS)]
            )

        def nr_copy(j):
            group = HEAD + (1 - dp) * half + j
            return pltpu.make_async_remote_copy(
                src_ref=noise_ref.at[step, :, pl.ds(group * GROUP, GROUP)],
                dst_ref=nz_oth.at[j],
                send_sem=sem_ns.at[j],
                recv_sem=sem_nr.at[j],
                device_id=pair,
                device_id_type=MESH,
            )

        gain_copies = [pltpu.make_async_copy(src, dst, sem_gain.at[k]) for k, (src, dst) in enumerate(gains)]
        for copy in gain_copies:
            copy.start()
        w_start(0)
        w_start(1)

    barrier = pltpu.get_barrier_semaphore()
    peers = (sib, over) if last else (sib, over, diag, pair)
    for peer in peers:
        pl.semaphore_signal(barrier, inc=1, device_id=peer, device_id_type=MESH)
    pl.semaphore_wait(barrier, len(peers))

    def fetch_head():
        for i in range(RING_GROUPS - WEIGHT_GROUPS):
            e_start(i)

    if not last:
        early = 6
        pl.loop(0, early)(lambda j: nr_copy(j).start())

    for copy in in_copies:
        copy.wait()
    if first:
        hid = hid_ref[...].astype(jnp.float32)
        w_copies[0].wait()
        w_start(2)
        fetch_head()
    else:
        a_rows = remote(rows_ref.at[1 - core], rows_a, sem_rows.at[0], sib)
        a_meta = remote(meta_ref.at[1 - core], meta_a, sem_meta.at[0], sib)
        a_rows.start()
        a_meta.start()
        a_rows.wait()
        a_meta.wait()
        mine = meta_ref[core]
        seen = meta_a[...]
        keep = mine[0] >= seen[0]
        meta_m[...] = jnp.where(keep[None], mine, seen)
        rows_m[...] = jnp.where(
            keep[:, :1], rows_ref[core].astype(jnp.float32), rows_a[...].astype(jnp.float32)
        ).astype(jnp.bfloat16)
        b_rows = remote(rows_m, rows_b, sem_rows.at[1], over)
        b_meta = remote(meta_m, meta_b, sem_meta.at[1], over)
        b_rows.start()
        b_meta.start()
        b_rows.wait()
        b_meta.wait()
        if not last:
            w_start(2)
        mine = meta_m[...]
        seen = meta_b[...]
        keep = mine[0] >= seen[0]
        meta_f[...] = jnp.where(keep[None], mine, seen)
        rows_f[...] = jnp.where(
            keep[:, :1], rows_m[...].astype(jnp.float32), rows_b[...].astype(jnp.float32)
        ).astype(jnp.bfloat16)
        c_rows = remote(rows_f, rows_c, sem_rows.at[2], sib)
        c_meta = remote(meta_f, meta_c, sem_meta.at[2], sib)
        c_rows.start()
        c_meta.start()
        c_rows.wait()
        c_meta.wait()
        if not last:
            w_copies[0].wait()
            fetch_head()
        low = core == 0
        r_f, r_c = rows_f[...].astype(jnp.float32), rows_c[...].astype(jnp.float32)
        t_f, t_c = meta_f[1], meta_c[1]
        picked = jnp.concatenate([jnp.where(low, r_f, r_c), jnp.where(low, r_c, r_f)], axis=0)
        token = jnp.concatenate([jnp.where(low, t_f, t_c), jnp.where(low, t_c, t_f)], axis=0).astype(jnp.int32)
        if last:
            for k, line in enumerate([ref[...] for ref in old_refs] + [as_line(token)]):
                tok_ref[k : k + 1] = line[:, : token.shape[0]]
        else:
            tok_ref[...] = as_line(token)
        hid_bf = (picked * embed_scale).astype(jnp.bfloat16)
        hout_ref[...] = hid_bf
        hid = hid_bf.astype(jnp.float32)

    if last:
        return

    batch = hid.shape[0]
    quarter = batch // 4
    hid32[...] = hid.reshape(4, quarter, width)
    for copy in gain_copies:
        copy.wait()
    normed = rms_scale(hid, gain(pre_ref)).astype(jnp.bfloat16)
    f_two[pl.ds(0, batch)] = normed
    w_copies[1].wait()
    col = 768

    @pl.loop(0, inner // col)
    def _(n):
        cols = pl.ds(pl.multiple_of(n * col, col), col)
        lhs = f_two[pl.ds(0, batch)]
        gate = jnp.dot(lhs, ring[pl.ds(0, width), cols], preferred_element_type=jnp.float32)
        up = jnp.dot(lhs, ring[pl.ds(width, width), cols], preferred_element_type=jnp.float32)
        gate_s[:, cols] = (jax.nn.gelu(gate, approximate=True) * up).astype(jnp.bfloat16)

    free = RING_GROUPS - WEIGHT_GROUPS + (2 * width) // GROUP
    for i in range(RING_GROUPS - WEIGHT_GROUPS, free):
        e_start(i)
    w_copies[2].wait()

    @pl.loop(0, width // col)
    def _(n):
        cols = pl.ds(pl.multiple_of(n * col, col), col)
        part_s[:, :, cols] = jnp.dot(
            gate_s[...], ring[pl.ds(2 * width, inner), cols], preferred_element_type=jnp.float32
        ).reshape(4, quarter, col)

    for i in range(free, RING_GROUPS):
        e_start(i)

    ra = remote(part_s.at[pl.ds(2 * (1 - core), 2)], part_a, sem_ra, sib)
    ra.start()
    ra.wait()
    half_s[...] = part_s[pl.ds(2 * core, 2)] + part_a[...]
    rb = remote(half_s.at[1 - chip], part_b, sem_rb, over)
    rb.start()
    rb.wait()
    down_sum = half_s[chip] + part_b[...]
    place = 2 * core + chip
    post_out = rms_scale(down_sum, gain(post_ref)).astype(jnp.bfloat16)
    resid = (hid32[place] + post_out.astype(jnp.float32)).astype(jnp.bfloat16)
    final_in = rms_scale(resid.astype(jnp.float32), gain(fin_ref)).astype(jnp.bfloat16)
    f_send[...] = final_in
    f_copies = [remote(f_send, f_all.at[k], sem_f.at[k], peer) for k, peer in enumerate((sib, over, diag))]
    f_pair_copy = remote(f_send, f_pair, sem_fo, pair)
    for copy in [*f_copies, f_pair_copy]:
        copy.start()
    pl.loop(early, half)(lambda j: nr_copy(j).start())
    for copy in f_copies:
        copy.wait()
    low_core, low_chip = core == 0, chip == 0

    def in_order(mine_ref, others_ref):
        me_f, sib_f, over_f, diag_f = (v.astype(jnp.float32) for v in (mine_ref[...], *(others_ref[k] for k in range(3))))
        core0 = [jnp.where(low_core, a, b) for a, b in ((me_f, sib_f), (over_f, diag_f))]
        core1 = [jnp.where(low_core, b, a) for a, b in ((me_f, sib_f), (over_f, diag_f))]
        order = [
            jnp.where(low_chip, core0[0], core0[1]),
            jnp.where(low_chip, core0[1], core0[0]),
            jnp.where(low_chip, core1[0], core1[1]),
            jnp.where(low_chip, core1[1], core1[0]),
        ]
        return jnp.concatenate(order, axis=0).astype(jnp.bfloat16)

    f_two[pl.ds(0, batch)] = in_order(f_send, f_all)
    g_copies = [remote(f_pair, g_all.at[k], sem_g.at[k], peer) for k, peer in enumerate((sib, over, diag))]

    bv[...] = jnp.full_like(bv, NEG)
    bi[...] = jnp.zeros_like(bi)
    heat = jnp.full((1, 128), temp_ref[0, 0], jnp.float32)
    fold = jnp.where(heat > 2.0**64, 2.0**-64, 1.0)
    c1 = (SOFT_CAP * fold)[:, :1]
    c2 = (1.0 / (heat * fold))[:, :1]

    def score(i, rows, nz_refs):
        slot = lax.rem(i + WEIGHT_GROUPS, RING_GROUPS)
        group = group_of(i)
        for j in range(NSUB):
            e_copy(i, j).wait()
        lhs = f_two[pl.ds(0, rows)]
        for start, size, turn in CUTS:
            block = ring[pl.ds(pl.multiple_of(slot * GROUP + start, 256), size), :]
            if turn:
                for k in range(0, width, 256):
                    turned[pl.ds(k, 256)] = block[:, k : k + 256].T
                z = jnp.dot(lhs, turned[...], preferred_element_type=jnp.float32)
            else:
                z = lax.dot_general(lhs, block, (((1,), (1,)), ((), ())), preferred_element_type=jnp.float32)
            s = jnp.tanh(z * (1.0 / SOFT_CAP)) * c1 * c2
            for part, nz in enumerate(nz_refs):
                take_rows = pl.ds(part * batch, batch)
                for q in range(size // 256):
                    v = s[part * batch : (part + 1) * batch, q * 256 : (q + 1) * 256]
                    v = v + nz[:, start + q * 256 : start + (q + 1) * 256]
                    old = bv[take_rows]
                    better = v > old
                    bv[take_rows] = jnp.where(better, v, old)
                    bi[take_rows] = jnp.where(better, group * (GROUP // 256) + (start // 256 + q), bi[take_rows])

        @pl.when(i + RING_GROUPS < n_iter)
        def _():
            e_start(i + RING_GROUPS)

    def own(i):
        no_copy(i).wait()
        score(i, batch, [nz_own.at[lax.rem(i, RING_GROUPS)]])

        @pl.when(i == SPREAD)
        def _():
            f_pair_copy.wait()
            for copy in g_copies:
                copy.start()

    def shared(i):
        no_copy(i).wait()
        nr_copy(i - HEAD).wait_recv()
        score(i, 2 * batch, [nz_own.at[lax.rem(i, RING_GROUPS)], nz_oth.at[i - HEAD]])

    def settle(part):
        val = bv[pl.ds(part * batch, batch)]
        tile = bi[pl.ds(part * batch, batch)]
        top = jnp.max(val, axis=1, keepdims=True)
        ids = (tile * 256 + lax.broadcasted_iota(jnp.int32, tile.shape, 1)).astype(jnp.float32)
        row = jnp.min(jnp.where(val == top, ids, 3.0e7), axis=1, keepdims=True)
        return jnp.broadcast_to(top, (batch, 128)), jnp.broadcast_to(row, (batch, 128))

    by = remote(best_oth, best_in, sem_by, pair)

    @pl.loop(0, 2)
    def _(phase):
        pl.loop(jnp.where(phase == 0, 0, HEAD + half), jnp.where(phase == 0, HEAD, n_iter))(own)

        @pl.when(phase == 0)
        def _():
            for copy in g_copies:
                copy.wait()
            f_two[pl.ds(batch, batch)] = in_order(f_pair, g_all)
            pl.loop(HEAD, HEAD + half)(shared)
            o_val, o_row = settle(1)
            best_oth[0] = o_val
            best_oth[1] = o_row
            by.start()

    pl.loop(0, half)(lambda j: nr_copy(j).wait_send())
    m_val, m_row = settle(0)
    by.wait()
    keep = m_val >= best_in[0]
    top = jnp.where(keep, m_val, best_in[0])
    row = jnp.where(keep, m_row, best_in[1])
    offset = (tp * (n_group * GROUP)).astype(jnp.float32)
    hb = batch // 2
    for part in range(2):
        best_ref[part, 0] = top[part * hb : (part + 1) * hb]
        best_ref[part, 1] = row[part * hb : (part + 1) * hb] + offset
    line_ref[...] = as_line(row.astype(jnp.int32))


def lookup_kernel(line_ref, emb_ref, out_ref, tiles, sem):
    half, batch = out_ref.shape[1], 2 * out_ref.shape[1]
    for r in range(batch):
        base = pl.multiple_of(lax.div(line_ref[0, r], 8) * 8, 8)
        pltpu.make_async_copy(emb_ref.at[pl.ds(base, 8)], tiles.at[pl.ds(8 * r, 8)], sem).start()
    shape = (batch, 8 * batch)
    place = lax.broadcasted_iota(jnp.int32, (batch, 1), 0)
    want = 8 * place
    for r in range(batch):
        want = want + jnp.where(place == r, lax.rem(line_ref[0, r], 8), 0)
    pick = (lax.broadcasted_iota(jnp.int32, shape, 1) == want).astype(jnp.bfloat16)
    pltpu.make_async_copy(emb_ref.at[pl.ds(0, 8 * batch)], tiles, sem).wait()
    rows = jnp.dot(pick, tiles[...], preferred_element_type=jnp.float32).astype(jnp.bfloat16)
    out_ref[0] = rows[:half]
    out_ref[1] = rows[half:]


def lookup(line, batch, embedding):
    width = embedding.shape[1]
    return pl.pallas_call(
        lookup_kernel,
        out_shape=jax.ShapeDtypeStruct((2, batch // 2, width), jnp.bfloat16),
        in_specs=[pl.BlockSpec(memory_space=pltpu.SMEM), pl.BlockSpec(memory_space=pl.ANY)],
        out_specs=pl.BlockSpec(memory_space=pltpu.VMEM),
        scratch_shapes=[pltpu.VMEM((8 * batch, width), jnp.bfloat16), pltpu.SemaphoreType.DMA(())],
        compiler_params=pltpu.CompilerParams(vmem_limit_bytes=66_000_000),
        name="lookup",
    )(line, embedding)


def call_step(step, steps, batch, width, inner, vocab_local, embed_scale, operands):
    first, last = step == 0, step == steps
    f32, bf16, i32 = jnp.float32, jnp.bfloat16, jnp.int32
    vmem, hbm = pl.BlockSpec(memory_space=pltpu.VMEM), pl.BlockSpec(memory_space=pl.ANY)
    dma = pltpu.SemaphoreType.DMA
    n_group = vocab_local // GROUP
    half = (n_group - OWN) // 2
    n_iter = OWN + half
    hb, quarter = batch // 2, batch // 4
    in_specs = [hbm] * (1 if first else 2) + [vmem] * ((step - 1) * last)
    if not last:
        in_specs += [hbm] * 3 + [pl.BlockSpec(memory_space=pltpu.SMEM)] + [hbm] * 5
    outs, scratch = [], []
    if first:
        scratch += [pltpu.VMEM((batch, width), bf16), dma((1,))]
    else:
        scratch += [pltpu.VMEM((2, hb, width), bf16), pltpu.VMEM((2, 2, hb, 128), f32), dma((2,))]
    if not last:
        scratch += [pltpu.VMEM((width,), bf16)] * 3 + [dma((3,))]
    if not first:
        outs += [jax.ShapeDtypeStruct((steps, batch) if last else (1, 128), i32), jax.ShapeDtypeStruct((batch, width), bf16)]
        rows, meta = pltpu.VMEM((hb, width), bf16), pltpu.VMEM((2, hb, 128), f32)
        scratch += [rows, meta] * 5 + [dma((3, 2)), dma((3, 2))]
    if not last:
        outs += [
            jax.ShapeDtypeStruct((2, 2, hb, 128), f32),
            jax.ShapeDtypeStruct((1, 128), i32),
        ]
        scratch += [
            pltpu.VMEM((RING_GROUPS * GROUP, width), bf16),
            pltpu.VMEM((RING_GROUPS, batch, GROUP), f32),
            pltpu.VMEM((half, batch, GROUP), f32),
            pltpu.VMEM((4, quarter, width), f32),
            pltpu.VMEM((2, quarter, width), f32),
            pltpu.VMEM((2, quarter, width), f32),
            pltpu.VMEM((quarter, width), f32),
            pltpu.VMEM((quarter, width), bf16),
            pltpu.VMEM((3, quarter, width), bf16),
            pltpu.VMEM((quarter, width), bf16),
            pltpu.VMEM((3, quarter, width), bf16),
            pltpu.VMEM((2 * batch, width), bf16),
            pltpu.VMEM((4, quarter, width), f32),
            pltpu.VMEM((batch, inner), bf16),
            pltpu.VMEM((width, max(c[1] for c in CUTS if c[2])), bf16),
            pltpu.VMEM((2 * batch, 256), f32),
            pltpu.VMEM((2 * batch, 256), i32),
            pltpu.VMEM((2, batch, 128), f32),
            pltpu.VMEM((2, batch, 128), f32),
            dma((3,)),
            dma((RING_GROUPS, NSUB)),
            dma((RING_GROUPS,)),
            dma((half,)),
            dma((half,)),
            dma((2,)),
            dma((2,)),
            dma((3, 2)),
            dma((2,)),
            dma((3, 2)),
            dma((2,)),
        ]
    return pl.pallas_call(
        functools.partial(step_kernel, (step, first, last, n_group, embed_scale)),
        out_shape=outs,
        in_specs=in_specs,
        out_specs=[vmem] * len(outs),
        scratch_shapes=scratch,
        compiler_params=pltpu.CompilerParams(
            collective_id=step, has_side_effects=True, vmem_limit_bytes=66_000_000
        ),
        name=f"step{step}",
    )(*operands)


def solution(mesh):
    def local_steps(start_hidden, embedding, pre_norm, w_gate, w_up, w_down, post_norm, final_norm, temperature, step_noise):
        vocab_local, width = embedding.shape
        batch, steps = start_hidden.shape[0], step_noise.shape[0]
        inner = w_gate.shape[1]
        embed_scale = float(np.float64(math.sqrt(width)).astype(jnp.bfloat16))
        common = [pre_norm, post_norm, final_norm, temperature.reshape(1, 1), w_gate, w_up, w_down, embedding, step_noise]
        sizes = (steps, batch, width, inner, vocab_local, embed_scale)
        best, line = call_step(0, *sizes, [start_hidden, *common])
        lines = []
        for step in range(1, steps):
            outs = call_step(step, *sizes, [lookup(line, batch, embedding), best, *common])
            lines.append(outs[0])
            best, line = outs[2:]
        tokens, hidden = call_step(steps, *sizes, [lookup(line, batch, embedding), best, *lines])
        return tokens, hidden

    return jax.shard_map(
        local_steps,
        mesh=mesh,
        in_specs=(P("dp", None), P("tp", None), P(), P(None, "tp"), P(None, "tp"), P("tp", None), P(), P(), P(), P(None, "dp", "tp")),
        out_specs=(P(None, "dp"), P("dp", None)),
        check_vma=False,
    )
```

```python
import functools
import math

import jax
import jax.numpy as jnp
import numpy as np
from jax import lax
from jax.experimental import pallas as pl
from jax.experimental.pallas import tpu as pltpu
from jax.sharding import PartitionSpec as P

SOFT_CAP = 30.0
EPSILON = 1e-6
MESH = pl.DeviceIdType.MESH

SUB = 640
NSUB = 2
GROUP = SUB * NSUB
RING_GROUPS = 9
SPREAD = 5
WEIGHT_GROUPS = 6
CUTS = ((0, 512, False), (512, 768, True))
HEAD = 12
TAIL = 2
OWN = HEAD + TAIL
NEG = -3.0e38


def gain(ref):
    return ref[...].astype(jnp.float32).reshape(1, ref.shape[0])


def rms_scale(x_f32, gain_row):
    mean_sq = jnp.mean(x_f32 * x_f32, axis=-1, keepdims=True)
    return x_f32 * lax.rsqrt(mean_sq + EPSILON) * (1.0 + gain_row)


def remote(src, dst, sem, peer):
    return pltpu.make_async_remote_copy(
        src_ref=src, dst_ref=dst, send_sem=sem.at[0], recv_sem=sem.at[1], device_id=peer, device_id_type=MESH
    )


def as_line(wide):
    eye = lax.broadcasted_iota(jnp.int32, wide.shape, 0) == lax.broadcasted_iota(jnp.int32, wide.shape, 1)
    return jnp.sum(jnp.where(eye, wide, 0), axis=0, keepdims=True)


def step_kernel(cfg, *refs):
    step, first, last, n_group, embed_scale = cfg
    refs = list(refs)
    take = lambda n: [refs.pop(0) for _ in range(n)]
    if first:
        (hid_hbm,) = take(1)
    else:
        rows_hbm, meta_hbm = take(2)
        if last:
            old_refs = take(step - 1)
    if not last:
        pre_hbm, post_hbm, fin_hbm, temp_ref, wg_ref, wu_ref, wd_ref, emb_ref, noise_ref = take(9)
    if not first:
        tok_ref, hout_ref = take(2)
    if not last:
        best_ref, line_ref = take(2)
    if first:
        hid_ref, sem_in = take(2)
        inputs = [(hid_hbm, hid_ref)]
    else:
        rows_ref, meta_ref, sem_in = take(3)
        inputs = [(rows_hbm, rows_ref), (meta_hbm, meta_ref)]
    if not last:
        pre_ref, post_ref, fin_ref, sem_gain = take(4)
        gains = [(pre_hbm, pre_ref), (post_hbm, post_ref), (fin_hbm, fin_ref)]
    in_copies = [pltpu.make_async_copy(src, dst, sem_in.at[k]) for k, (src, dst) in enumerate(inputs)]
    for copy in in_copies:
        copy.start()
    if not first:
        rows_a, meta_a, rows_m, meta_m, rows_b, meta_b, rows_f, meta_f, rows_c, meta_c, sem_rows, sem_meta = take(12)
    if not last:
        (ring, nz_own, nz_oth, part_s, part_a, half_s, part_b, f_send, f_all, f_pair, g_all, f_two,
         hid32, gate_s, turned, bv, bi, best_oth, best_in,
         sem_w, sem_e, sem_no, sem_ns, sem_nr, sem_ra, sem_rb, sem_f, sem_fo, sem_g, sem_by) = take(30)

    dp, tp = lax.axis_index("dp"), lax.axis_index("tp")
    core, chip = lax.rem(tp, 2), lax.div(tp, 2)
    tp_sib = chip * 2 + (1 - core)
    tp_x = (1 - chip) * 2 + core
    tp_diag = (1 - chip) * 2 + (1 - core)
    sib, over, diag, pair = (dp, tp_sib), (dp, tp_x), (dp, tp_diag), (1 - dp, tp)

    if not last:
        half = (n_group - OWN) // 2
        n_iter = OWN + half
        width = ring.shape[1]
        inner = wg_ref.shape[1]
        weights = [(wg_ref, 0, width), (wu_ref, width, width), (wd_ref, 2 * width, inner)]
        w_copies = [
            pltpu.make_async_copy(ref, ring.at[pl.ds(base, rows)], sem_w.at[k])
            for k, (ref, base, rows) in enumerate(weights)
        ]

        def w_start(k):
            ref, base, rows = weights[k]
            piece = rows // 9
            for p in range(0, rows, piece):
                pltpu.make_async_copy(ref.at[pl.ds(p, piece)], ring.at[pl.ds(base + p, piece)], sem_w.at[k]).start()

        def group_of(i):
            moved = jnp.where(i < HEAD + half, dp * half, half)
            return i + jnp.where(i < HEAD, 0, moved)

        def e_copy(i, j):
            group = group_of(i)
            slot = lax.rem(i + WEIGHT_GROUPS, RING_GROUPS)
            return pltpu.make_async_copy(
                emb_ref.at[pl.ds(group * GROUP + j * SUB, SUB)],
                ring.at[pl.ds(slot * GROUP + j * SUB, SUB)],
                sem_e.at[slot, j],
            )

        def e_start(i):
            for j in range(NSUB):
                e_copy(i, j).start()
            no_copy(i).start()

        def no_copy(i):
            group = group_of(i)
            return pltpu.make_async_copy(
                noise_ref.at[step, :, pl.ds(group * GROUP, GROUP)], nz_own.at[lax.rem(i, RING_GROUPS)], sem_no.at[lax.rem(i, RING_GROUPS)]
            )

        def nr_copy(j):
            group = HEAD + (1 - dp) * half + j
            return pltpu.make_async_remote_copy(
                src_ref=noise_ref.at[step, :, pl.ds(group * GROUP, GROUP)],
                dst_ref=nz_oth.at[j],
                send_sem=sem_ns.at[j],
                recv_sem=sem_nr.at[j],
                device_id=pair,
                device_id_type=MESH,
            )

        gain_copies = [pltpu.make_async_copy(src, dst, sem_gain.at[k]) for k, (src, dst) in enumerate(gains)]
        for copy in gain_copies:
            copy.start()
        w_start(0)
        w_start(1)

    barrier = pltpu.get_barrier_semaphore()
    peers = (sib, over) if last else (sib, over, diag, pair)
    for peer in peers:
        pl.semaphore_signal(barrier, inc=1, device_id=peer, device_id_type=MESH)
    pl.semaphore_wait(barrier, len(peers))

    def fetch_head():
        for i in range(RING_GROUPS - WEIGHT_GROUPS):
            e_start(i)

    if not last:
        early = 7
        pl.loop(0, early)(lambda j: nr_copy(j).start())

    for copy in in_copies:
        copy.wait()
    if first:
        hid = hid_ref[...].astype(jnp.float32)
        w_copies[0].wait()
        w_start(2)
        fetch_head()
    else:
        a_rows = remote(rows_ref.at[1 - core], rows_a, sem_rows.at[0], sib)
        a_meta = remote(meta_ref.at[1 - core], meta_a, sem_meta.at[0], sib)
        a_rows.start()
        a_meta.start()
        a_rows.wait()
        a_meta.wait()
        if not last:
            w_start(2)
        mine = meta_ref[core]
        seen = meta_a[...]
        keep = mine[0] >= seen[0]
        meta_m[...] = jnp.where(keep[None], mine, seen)
        rows_m[...] = jnp.where(
            keep[:, :1], rows_ref[core].astype(jnp.float32), rows_a[...].astype(jnp.float32)
        ).astype(jnp.bfloat16)
        b_rows = remote(rows_m, rows_b, sem_rows.at[1], over)
        b_meta = remote(meta_m, meta_b, sem_meta.at[1], over)
        b_rows.start()
        b_meta.start()
        b_rows.wait()
        b_meta.wait()
        if not last:
            fetch_head()
        mine = meta_m[...]
        seen = meta_b[...]
        keep = mine[0] >= seen[0]
        meta_f[...] = jnp.where(keep[None], mine, seen)
        rows_f[...] = jnp.where(
            keep[:, :1], rows_m[...].astype(jnp.float32), rows_b[...].astype(jnp.float32)
        ).astype(jnp.bfloat16)
        c_rows = remote(rows_f, rows_c, sem_rows.at[2], sib)
        c_meta = remote(meta_f, meta_c, sem_meta.at[2], sib)
        c_rows.start()
        c_meta.start()
        c_rows.wait()
        c_meta.wait()
        if not last:
            w_copies[0].wait()
        low = core == 0
        r_f, r_c = rows_f[...].astype(jnp.float32), rows_c[...].astype(jnp.float32)
        t_f, t_c = meta_f[1], meta_c[1]
        picked = jnp.concatenate([jnp.where(low, r_f, r_c), jnp.where(low, r_c, r_f)], axis=0)
        token = jnp.concatenate([jnp.where(low, t_f, t_c), jnp.where(low, t_c, t_f)], axis=0).astype(jnp.int32)
        if last:
            for k, line in enumerate([ref[...] for ref in old_refs] + [as_line(token)]):
                tok_ref[k : k + 1] = line[:, : token.shape[0]]
        else:
            tok_ref[...] = as_line(token)
        hid_bf = (picked * embed_scale).astype(jnp.bfloat16)
        hout_ref[...] = hid_bf
        hid = hid_bf.astype(jnp.float32)

    if last:
        return

    batch = hid.shape[0]
    quarter = batch // 4
    hid32[...] = hid.reshape(4, quarter, width)
    for copy in gain_copies:
        copy.wait()
    normed = rms_scale(hid, gain(pre_ref)).astype(jnp.bfloat16)
    f_two[pl.ds(0, batch)] = normed
    w_copies[1].wait()
    col = 768

    @pl.loop(0, inner // col)
    def _(n):
        cols = pl.ds(pl.multiple_of(n * col, col), col)
        lhs = f_two[pl.ds(0, batch)]
        gate = jnp.dot(lhs, ring[pl.ds(0, width), cols], preferred_element_type=jnp.float32)
        up = jnp.dot(lhs, ring[pl.ds(width, width), cols], preferred_element_type=jnp.float32)
        gate_s[:, cols] = (jax.nn.gelu(gate, approximate=True) * up).astype(jnp.bfloat16)

    free = RING_GROUPS - WEIGHT_GROUPS + (2 * width) // GROUP
    for i in range(RING_GROUPS - WEIGHT_GROUPS, free):
        e_start(i)
    w_copies[2].wait()

    @pl.loop(0, width // col)
    def _(n):
        cols = pl.ds(pl.multiple_of(n * col, col), col)
        part_s[:, :, cols] = jnp.dot(
            gate_s[...], ring[pl.ds(2 * width, inner), cols], preferred_element_type=jnp.float32
        ).reshape(4, quarter, col)

    for i in range(free, RING_GROUPS):
        e_start(i)

    ra = remote(part_s.at[pl.ds(2 * (1 - core), 2)], part_a, sem_ra, sib)
    ra.start()
    ra.wait()
    half_s[...] = part_s[pl.ds(2 * core, 2)] + part_a[...]
    rb = remote(half_s.at[1 - chip], part_b, sem_rb, over)
    rb.start()
    rb.wait()
    down_sum = half_s[chip] + part_b[...]
    place = 2 * core + chip
    post_out = rms_scale(down_sum, gain(post_ref)).astype(jnp.bfloat16)
    resid = (hid32[place] + post_out.astype(jnp.float32)).astype(jnp.bfloat16)
    final_in = rms_scale(resid.astype(jnp.float32), gain(fin_ref)).astype(jnp.bfloat16)
    f_send[...] = final_in
    f_copies = [remote(f_send, f_all.at[k], sem_f.at[k], peer) for k, peer in enumerate((sib, over, diag))]
    f_pair_copy = remote(f_send, f_pair, sem_fo, pair)
    for copy in [*f_copies, f_pair_copy]:
        copy.start()
    pl.loop(early, half)(lambda j: nr_copy(j).start())
    for copy in f_copies:
        copy.wait()
    low_core, low_chip = core == 0, chip == 0

    def in_order(mine_ref, others_ref):
        me_f, sib_f, over_f, diag_f = (v.astype(jnp.float32) for v in (mine_ref[...], *(others_ref[k] for k in range(3))))
        core0 = [jnp.where(low_core, a, b) for a, b in ((me_f, sib_f), (over_f, diag_f))]
        core1 = [jnp.where(low_core, b, a) for a, b in ((me_f, sib_f), (over_f, diag_f))]
        order = [
            jnp.where(low_chip, core0[0], core0[1]),
            jnp.where(low_chip, core0[1], core0[0]),
            jnp.where(low_chip, core1[0], core1[1]),
            jnp.where(low_chip, core1[1], core1[0]),
        ]
        return jnp.concatenate(order, axis=0).astype(jnp.bfloat16)

    f_two[pl.ds(0, batch)] = in_order(f_send, f_all)
    g_copies = [remote(f_pair, g_all.at[k], sem_g.at[k], peer) for k, peer in enumerate((sib, over, diag))]

    bv[...] = jnp.full_like(bv, NEG)
    bi[...] = jnp.zeros_like(bi)
    heat = jnp.full((1, 128), temp_ref[0, 0], jnp.float32)
    fold = jnp.where(heat > 2.0**64, 2.0**-64, 1.0)
    c1 = (SOFT_CAP * fold)[:, :1]
    c2 = (1.0 / (heat * fold))[:, :1]

    def score(i, rows, nz_refs):
        slot = lax.rem(i + WEIGHT_GROUPS, RING_GROUPS)
        group = group_of(i)
        for j in range(NSUB):
            e_copy(i, j).wait()
        lhs = f_two[pl.ds(0, rows)]
        for start, size, turn in CUTS:
            block = ring[pl.ds(pl.multiple_of(slot * GROUP + start, 256), size), :]
            if turn:
                for k in range(0, width, 256):
                    turned[pl.ds(k, 256)] = block[:, k : k + 256].T
                z = jnp.dot(lhs, turned[...], preferred_element_type=jnp.float32)
            else:
                z = lax.dot_general(lhs, block, (((1,), (1,)), ((), ())), preferred_element_type=jnp.float32)
            s = jnp.tanh(z * (1.0 / SOFT_CAP)) * c1 * c2
            for part, nz in enumerate(nz_refs):
                take_rows = pl.ds(part * batch, batch)
                for q in range(size // 256):
                    v = s[part * batch : (part + 1) * batch, q * 256 : (q + 1) * 256]
                    v = v + nz[:, start + q * 256 : start + (q + 1) * 256]
                    old = bv[take_rows]
                    better = v > old
                    bv[take_rows] = jnp.where(better, v, old)
                    bi[take_rows] = jnp.where(better, group * (GROUP // 256) + (start // 256 + q), bi[take_rows])

        @pl.when(i + RING_GROUPS < n_iter)
        def _():
            e_start(i + RING_GROUPS)

    def own(i):
        no_copy(i).wait()
        score(i, batch, [nz_own.at[lax.rem(i, RING_GROUPS)]])

        @pl.when(i == SPREAD)
        def _():
            f_pair_copy.wait()
            for copy in g_copies:
                copy.start()

    def shared(i):
        no_copy(i).wait()
        nr_copy(i - HEAD).wait_recv()
        score(i, 2 * batch, [nz_own.at[lax.rem(i, RING_GROUPS)], nz_oth.at[i - HEAD]])

    def settle(part):
        val = bv[pl.ds(part * batch, batch)]
        tile = bi[pl.ds(part * batch, batch)]
        top = jnp.max(val, axis=1, keepdims=True)
        ids = (tile * 256 + lax.broadcasted_iota(jnp.int32, tile.shape, 1)).astype(jnp.float32)
        row = jnp.min(jnp.where(val == top, ids, 3.0e7), axis=1, keepdims=True)
        return jnp.broadcast_to(top, (batch, 128)), jnp.broadcast_to(row, (batch, 128))

    by = remote(best_oth, best_in, sem_by, pair)

    @pl.loop(0, 2)
    def _(phase):
        pl.loop(jnp.where(phase == 0, 0, HEAD + half), jnp.where(phase == 0, HEAD, n_iter))(own)

        @pl.when(phase == 0)
        def _():
            for copy in g_copies:
                copy.wait()
            f_two[pl.ds(batch, batch)] = in_order(f_pair, g_all)
            pl.loop(HEAD, HEAD + half)(shared)
            o_val, o_row = settle(1)
            best_oth[0] = o_val
            best_oth[1] = o_row
            by.start()

    pl.loop(0, half)(lambda j: nr_copy(j).wait_send())
    m_val, m_row = settle(0)
    by.wait()
    keep = m_val >= best_in[0]
    top = jnp.where(keep, m_val, best_in[0])
    row = jnp.where(keep, m_row, best_in[1])
    offset = (tp * (n_group * GROUP)).astype(jnp.float32)
    hb = batch // 2
    for part in range(2):
        best_ref[part, 0] = top[part * hb : (part + 1) * hb]
        best_ref[part, 1] = row[part * hb : (part + 1) * hb] + offset
    line_ref[...] = as_line(row.astype(jnp.int32))


def lookup_kernel(line_ref, emb_ref, out_ref, tiles, sem):
    half, batch = out_ref.shape[1], 2 * out_ref.shape[1]
    for r in range(batch):
        base = pl.multiple_of(lax.div(line_ref[0, r], 8) * 8, 8)
        pltpu.make_async_copy(emb_ref.at[pl.ds(base, 8)], tiles.at[pl.ds(8 * r, 8)], sem).start()
    shape = (batch, 8 * batch)
    place = lax.broadcasted_iota(jnp.int32, (batch, 1), 0)
    want = 8 * place
    for r in range(batch):
        want = want + jnp.where(place == r, lax.rem(line_ref[0, r], 8), 0)
    pick = (lax.broadcasted_iota(jnp.int32, shape, 1) == want).astype(jnp.bfloat16)
    pltpu.make_async_copy(emb_ref.at[pl.ds(0, 8 * batch)], tiles, sem).wait()
    rows = jnp.dot(pick, tiles[...], preferred_element_type=jnp.float32).astype(jnp.bfloat16)
    out_ref[0] = rows[:half]
    out_ref[1] = rows[half:]


def lookup(line, batch, embedding):
    width = embedding.shape[1]
    return pl.pallas_call(
        lookup_kernel,
        out_shape=jax.ShapeDtypeStruct((2, batch // 2, width), jnp.bfloat16),
        in_specs=[pl.BlockSpec(memory_space=pltpu.SMEM), pl.BlockSpec(memory_space=pl.ANY)],
        out_specs=pl.BlockSpec(memory_space=pltpu.VMEM),
        scratch_shapes=[pltpu.VMEM((8 * batch, width), jnp.bfloat16), pltpu.SemaphoreType.DMA(())],
        compiler_params=pltpu.CompilerParams(vmem_limit_bytes=66_000_000),
        name="lookup",
    )(line, embedding)


def call_step(step, steps, batch, width, inner, vocab_local, embed_scale, operands):
    first, last = step == 0, step == steps
    f32, bf16, i32 = jnp.float32, jnp.bfloat16, jnp.int32
    vmem, hbm = pl.BlockSpec(memory_space=pltpu.VMEM), pl.BlockSpec(memory_space=pl.ANY)
    dma = pltpu.SemaphoreType.DMA
    n_group = vocab_local // GROUP
    half = (n_group - OWN) // 2
    n_iter = OWN + half
    hb, quarter = batch // 2, batch // 4
    in_specs = [hbm] * (1 if first else 2) + [vmem] * ((step - 1) * last)
    if not last:
        in_specs += [hbm] * 3 + [pl.BlockSpec(memory_space=pltpu.SMEM)] + [hbm] * 5
    outs, scratch = [], []
    if first:
        scratch += [pltpu.VMEM((batch, width), bf16), dma((1,))]
    else:
        scratch += [pltpu.VMEM((2, hb, width), bf16), pltpu.VMEM((2, 2, hb, 128), f32), dma((2,))]
    if not last:
        scratch += [pltpu.VMEM((width,), bf16)] * 3 + [dma((3,))]
    if not first:
        outs += [jax.ShapeDtypeStruct((steps, batch) if last else (1, 128), i32), jax.ShapeDtypeStruct((batch, width), bf16)]
        rows, meta = pltpu.VMEM((hb, width), bf16), pltpu.VMEM((2, hb, 128), f32)
        scratch += [rows, meta] * 5 + [dma((3, 2)), dma((3, 2))]
    if not last:
        outs += [
            jax.ShapeDtypeStruct((2, 2, hb, 128), f32),
            jax.ShapeDtypeStruct((1, 128), i32),
        ]
        scratch += [
            pltpu.VMEM((RING_GROUPS * GROUP, width), bf16),
            pltpu.VMEM((RING_GROUPS, batch, GROUP), f32),
            pltpu.VMEM((half, batch, GROUP), f32),
            pltpu.VMEM((4, quarter, width), f32),
            pltpu.VMEM((2, quarter, width), f32),
            pltpu.VMEM((2, quarter, width), f32),
            pltpu.VMEM((quarter, width), f32),
            pltpu.VMEM((quarter, width), bf16),
            pltpu.VMEM((3, quarter, width), bf16),
            pltpu.VMEM((quarter, width), bf16),
            pltpu.VMEM((3, quarter, width), bf16),
            pltpu.VMEM((2 * batch, width), bf16),
            pltpu.VMEM((4, quarter, width), f32),
            pltpu.VMEM((batch, inner), bf16),
            pltpu.VMEM((width, max(c[1] for c in CUTS if c[2])), bf16),
            pltpu.VMEM((2 * batch, 256), f32),
            pltpu.VMEM((2 * batch, 256), i32),
            pltpu.VMEM((2, batch, 128), f32),
            pltpu.VMEM((2, batch, 128), f32),
            dma((3,)),
            dma((RING_GROUPS, NSUB)),
            dma((RING_GROUPS,)),
            dma((half,)),
            dma((half,)),
            dma((2,)),
            dma((2,)),
            dma((3, 2)),
            dma((2,)),
            dma((3, 2)),
            dma((2,)),
        ]
    return pl.pallas_call(
        functools.partial(step_kernel, (step, first, last, n_group, embed_scale)),
        out_shape=outs,
        in_specs=in_specs,
        out_specs=[vmem] * len(outs),
        scratch_shapes=scratch,
        compiler_params=pltpu.CompilerParams(
            collective_id=step, has_side_effects=True, vmem_limit_bytes=66_000_000
        ),
        name=f"step{step}",
    )(*operands)


def solution(mesh):
    def local_steps(start_hidden, embedding, pre_norm, w_gate, w_up, w_down, post_norm, final_norm, temperature, step_noise):
        vocab_local, width = embedding.shape
        batch, steps = start_hidden.shape[0], step_noise.shape[0]
        inner = w_gate.shape[1]
        embed_scale = float(np.float64(math.sqrt(width)).astype(jnp.bfloat16))
        common = [pre_norm, post_norm, final_norm, temperature.reshape(1, 1), w_gate, w_up, w_down, embedding, step_noise]
        sizes = (steps, batch, width, inner, vocab_local, embed_scale)
        best, line = call_step(0, *sizes, [start_hidden, *common])
        lines = []
        for step in range(1, steps):
            outs = call_step(step, *sizes, [lookup(line, batch, embedding), best, *common])
            lines.append(outs[0])
            best, line = outs[2:]
        tokens, hidden = call_step(steps, *sizes, [lookup(line, batch, embedding), best, *lines])
        return tokens, hidden

    return jax.shard_map(
        local_steps,
        mesh=mesh,
        in_specs=(P("dp", None), P("tp", None), P(), P(None, "tp"), P(None, "tp"), P("tp", None), P(), P(), P(), P(None, "dp", "tp")),
        out_specs=(P(None, "dp"), P("dp", None)),
        check_vma=False,
    )
```
